8 devices in a mesh: tp: 2 (over z, y), cp: 4 (over x, core).
Axes of the slice: x: 2, y: 2, z: 1, core: 2. Of those that a mesh axis runs over, the one named last changes fastest.
Arguments:
- hidden: bfloat16 [2048, 4608], P('cp')
- g_pre: float32 [4608], replicated
- w_q: bfloat16 [4608, 32, 128], P(None, 'tp')
- w_k: bfloat16 [4608, 16, 128], P(None, 'tp')
- w_v: bfloat16 [4608, 16, 128], P(None, 'tp')
- w_o: bfloat16 [32, 128, 4608], P('tp')
- g_post: float32 [4608], replicated
- d_out: bfloat16 [2048, 4608], P('cp')
Outputs:
- output 1: bfloat16 [2048, 4608], P('cp')
- output 2: bfloat16 [2048, 4608], P('cp')
- output 3: float32 [4608], replicated
- output 4: float32 [4608, 32, 128], P(None, 'tp')
- output 5: float32 [4608, 16, 128], P(None, 'tp')
- output 6: float32 [4608, 16, 128], P(None, 'tp')
- output 7: float32 [32, 128, 4608], P('tp')
- output 8: float32 [4608], replicated
All inputs are finite; a program needn't handle non-finite values.
Results may differ from the reference program's by a relative error of at most 0.0176177.
Values are sent between devices in bfloat16 or wider.
A program may use at most 1 GiB of HBM per device.

```python
import jax
import jax.numpy as jnp
from jax import lax

D = 4608
HEADS = 32
KV_HEADS = 16
HEAD = 128
SEQ = 2048
Q_BLOCK = 256
SOFT_CAP = 30
GROUPS = HEADS // KV_HEADS
N_BLOCKS = SEQ // Q_BLOCK
ATTN_SCALE = HEAD ** -0.5
NORM_EPS = 1e-5
ROPE_THETA = 10000.0
MASK_FILL = -1e30


def setup_inputs(seed: int = 0) -> dict:
    rng_keys = jax.random.split(jax.random.key(seed), 8)
    qk_gain = (0.5 * SOFT_CAP) ** 0.5 * D ** -0.5
    hidden = jax.random.normal(rng_keys[0], (SEQ, D), jnp.float32)
    g_pre = jax.random.uniform(rng_keys[1], (D,), jnp.float32, 0.5, 1.5)
    w_q = jax.random.normal(rng_keys[2], (D, HEADS, HEAD), jnp.float32) * qk_gain
    w_k = jax.random.normal(rng_keys[3], (D, KV_HEADS, HEAD), jnp.float32) * qk_gain
    w_v = jax.random.normal(rng_keys[4], (D, KV_HEADS, HEAD), jnp.float32) * D ** -0.5
    w_o = jax.random.normal(rng_keys[5], (HEADS, HEAD, D), jnp.float32) * (HEADS * HEAD) ** -0.5
    g_post = jax.random.uniform(rng_keys[6], (D,), jnp.float32, 0.5, 1.5)
    d_out = jax.random.normal(rng_keys[7], (SEQ, D), jnp.float32)
    return {'hidden': hidden.astype(jnp.bfloat16), 'g_pre': g_pre, 'w_q': w_q.astype(jnp.bfloat16), 'w_k': w_k.astype(jnp.bfloat16), 'w_v': w_v.astype(jnp.bfloat16), 'w_o': w_o.astype(jnp.bfloat16), 'g_post': g_post, 'd_out': d_out.astype(jnp.bfloat16)}


def rms_norm(x_val):
    return x_val * lax.rsqrt(jnp.mean(x_val * x_val, axis=-1, keepdims=True) + NORM_EPS)


def rope_tables():
    half_dim = HEAD // 2
    inv_freq = ROPE_THETA ** (-jnp.arange(half_dim, dtype=jnp.float32) * 2.0 / HEAD)
    rot_angle = jnp.arange(SEQ, dtype=jnp.float32)[:, None] * inv_freq[None, :]
    return jnp.cos(rot_angle)[:, None, :], jnp.sin(rot_angle)[:, None, :]


def rope_apply(x_val, cos_t, sin_t):
    half_dim = x_val.shape[-1] // 2
    x_lo = x_val[..., :half_dim]
    x_hi = x_val[..., half_dim:]
    return jnp.concatenate([x_lo * cos_t - x_hi * sin_t, x_hi * cos_t + x_lo * sin_t], axis=-1)


def causal_attention(q_all, k_all, v_all):
    q_grp = q_all.reshape(N_BLOCKS, Q_BLOCK, KV_HEADS, GROUPS, HEAD).transpose(2, 0, 1, 3, 4).reshape(KV_HEADS * N_BLOCKS, Q_BLOCK, GROUPS, HEAD)
    head_ids = jnp.repeat(jnp.arange(KV_HEADS), N_BLOCKS)
    block_ids = jnp.tile(jnp.arange(N_BLOCKS), KV_HEADS)
    key_pos = jnp.arange(SEQ)

    def one_block(block_in):
        q_blk, head_id, block_id = block_in
        k_head = lax.dynamic_index_in_dim(k_all, head_id, axis=1, keepdims=False)
        v_head = lax.dynamic_index_in_dim(v_all, head_id, axis=1, keepdims=False)
        logits = jnp.einsum('qge,ke->gqk', q_blk, k_head) * ATTN_SCALE
        capped = SOFT_CAP * jnp.tanh(logits / SOFT_CAP)
        query_pos = block_id * Q_BLOCK + jnp.arange(Q_BLOCK)
        visible = query_pos[:, None] >= key_pos[None, :]
        capped = jnp.where(visible[None], capped, MASK_FILL)
        attn_prob = jax.nn.softmax(capped, axis=-1)
        return jnp.einsum('gqk,ke->qge', attn_prob, v_head)

    ctx_blocks = lax.map(jax.checkpoint(one_block), (q_grp, head_ids, block_ids))
    return ctx_blocks.reshape(KV_HEADS, N_BLOCKS, Q_BLOCK, GROUPS, HEAD).transpose(1, 2, 0, 3, 4).reshape(SEQ, HEADS, HEAD)


def block_forward(hidden, g_pre, w_q, w_k, w_v, w_o, g_post):
    a_act = (rms_norm(hidden) * g_pre).astype(jnp.bfloat16).astype(jnp.float32)
    cos_t, sin_t = rope_tables()
    q_all = rope_apply(jnp.einsum('sd,dhe->she', a_act, w_q), cos_t, sin_t).astype(jnp.bfloat16).astype(jnp.float32)
    k_all = rope_apply(jnp.einsum('sd,dhe->she', a_act, w_k), cos_t, sin_t).astype(jnp.bfloat16).astype(jnp.float32)
    v_all = jnp.einsum('sd,dhe->she', a_act, w_v).astype(jnp.bfloat16).astype(jnp.float32)
    ctx = causal_attention(q_all, k_all, v_all).astype(jnp.bfloat16).astype(jnp.float32)
    o_sum = jnp.einsum('she,hed->sd', ctx, w_o)
    return hidden + rms_norm(o_sum) * g_post


def reference(hidden, g_pre, w_q, w_k, w_v, w_o, g_post, d_out):
    y_full, pullback = jax.vjp(block_forward, hidden.astype(jnp.float32), g_pre, w_q.astype(jnp.float32), w_k.astype(jnp.float32), w_v.astype(jnp.float32), w_o.astype(jnp.float32), g_post)
    grad_h, grad_gpre, grad_wq, grad_wk, grad_wv, grad_wo, grad_gpost = pullback(d_out.astype(jnp.float32))
    return (y_full.astype(jnp.bfloat16), grad_h.astype(jnp.bfloat16), grad_gpre, grad_wq, grad_wk, grad_wv, grad_wo, grad_gpost)
```

```python
import functools

import jax
import jax.numpy as jnp
from jax import lax
from jax.experimental import pallas as pl
from jax.experimental.pallas import tpu as pltpu
from jax.sharding import PartitionSpec as P

SOFT_CAP = 30.0
NORM_EPS = 1e-5
ROPE_THETA = 10000.0
HEAD = 128
LOG2E = 1.4426950408889634
NEG = -1e30
F32 = jnp.float32
BF16 = jnp.bfloat16

NT = (((1,), (1,)), ((), ()))
NN = (((1,), (0,)), ((), ()))
TN = (((0,), (0,)), ((), ()))


def dotf(a, b, dims):
    return lax.dot_general(a, b, dims, preferred_element_type=F32)


def rope_tables(length):
    half = HEAD // 2
    inv_freq = ROPE_THETA ** (-jnp.arange(half, dtype=F32) * 2.0 / HEAD)
    ang = jnp.arange(length).astype(F32)[:, None] * inv_freq[None, :]
    cos, sin = jnp.cos(ang), jnp.sin(ang)
    return jnp.concatenate([cos, cos], axis=-1), jnp.concatenate([-sin, sin], axis=-1)


QB = 256
KB = 256


def attn_fwd_kernel(q_ref, k_ref, v_ref, ctx_ref, lse_ref, acc_ref, sum_ref, *, k1, k2):
    i = pl.program_id(1)
    q = jnp.concatenate([q_ref[:, :HEAD], q_ref[:, HEAD:]], axis=0)
    acc_ref[...] = jnp.zeros_like(acc_ref)
    sum_ref[...] = jnp.zeros_like(sum_ref)

    def chunk(row0, mask):
        k = k_ref[pl.ds(row0, KB), :]
        v = v_ref[pl.ds(row0, KB), :]
        s = dotf(q, k, NT)
        p = jnp.exp2(jnp.tanh(s * k1) * k2)
        if mask is not None:
            p = jnp.where(mask, p, 0.0)
        part = p[:, :128]
        for c in range(1, KB // 128):
            part = part + p[:, c * 128:(c + 1) * 128]
        return part, dotf(p.astype(BF16), v, NN)

    def pair(j, carry):
        s0, a0 = chunk(pl.multiple_of(j * (2 * KB), 2 * KB), None)
        s1, a1 = chunk(pl.multiple_of(j * (2 * KB) + KB, KB), None)
        acc_ref[...] += a0 + a1
        sum_ref[...] += s0 + s1
        return carry

    lax.fori_loop(0, i // 2, pair, 0)

    @pl.when(i % 2 == 1)
    def _():
        s0, a0 = chunk(pl.multiple_of((i - 1) * KB, KB), None)
        acc_ref[...] += a0
        sum_ref[...] += s0

    rows = lax.broadcasted_iota(jnp.int32, (2 * QB, KB), 0) % QB
    cols = lax.broadcasted_iota(jnp.int32, (2 * QB, KB), 1)
    s0, a0 = chunk(pl.multiple_of(i * KB, KB), rows >= cols)
    total = jnp.sum(sum_ref[...] + s0, axis=1, keepdims=True)
    ctx = ((acc_ref[...] + a0) / total).astype(BF16)
    ctx_ref[:, :HEAD] = ctx[:QB]
    ctx_ref[:, HEAD:] = ctx[QB:]
    lse = jnp.broadcast_to(jnp.log2(total), (2 * QB, 128)).T
    lse_ref[0, 0:1, :] = lse[0:1, :QB]
    lse_ref[0, 1:2, :] = lse[0:1, QB:]


def attn_fwd(q, k, v):
    T, kvh = q.shape[0], k.shape[1] // HEAD
    scale = HEAD ** -0.5
    return pl.pallas_call(
        functools.partial(attn_fwd_kernel, k1=scale / SOFT_CAP, k2=SOFT_CAP * LOG2E),
        grid=(kvh, T // QB),
        in_specs=[
            pl.BlockSpec((QB, 2 * HEAD), lambda h, i: (i, h)),
            pl.BlockSpec((T, HEAD), lambda h, i: (0, h)),
            pl.BlockSpec((T, HEAD), lambda h, i: (0, h)),
        ],
        out_specs=[
            pl.BlockSpec((QB, 2 * HEAD), lambda h, i: (i, h)),
            pl.BlockSpec((1, 2, QB), lambda h, i: (h, 0, i)),
        ],
        out_shape=[
            jax.ShapeDtypeStruct(q.shape, BF16),
            jax.ShapeDtypeStruct((kvh, 2, T), F32),
        ],
        scratch_shapes=[pltpu.VMEM((2 * QB, HEAD), F32), pltpu.VMEM((2 * QB, 128), F32)],
        compiler_params=pltpu.CompilerParams(dimension_semantics=("arbitrary", "arbitrary")),
        cost_estimate=pl.CostEstimate(flops=int(2 * 2 * T * T * HEAD * kvh * 2), bytes_accessed=4 * q.size * 2, transcendentals=0),
        name="attn_fwd",
    )(q, k, v)


BQ = 256
BK = 512


def attn_bwd_kernel(q_ref, k_ref, v_ref, do_ref, ctx_ref, lse_ref, cos_ref, sin_ref, dq_ref, dk_ref, dv_ref,
                    dqa_ref, dka_ref, dva_ref, dd_ref, *, k1, k2, scale):
    J = pl.program_id(1)
    nq = q_ref.shape[0] // BQ
    r = BK // BQ

    @pl.when(J == 0)
    def _():
        dqa_ref[...] = jnp.zeros_like(dqa_ref)
        for g in range(2):
            for i in range(nq):
                sl = slice(i * BQ, (i + 1) * BQ)
                prod = do_ref[sl, g * HEAD:(g + 1) * HEAD].astype(F32) * ctx_ref[sl, g * HEAD:(g + 1) * HEAD].astype(F32)
                dd_ref[g, 0:1, sl] = jnp.sum(prod.T, axis=0, keepdims=True)

    dka_ref[...] = jnp.zeros_like(dka_ref)
    dva_ref[...] = jnp.zeros_like(dva_ref)
    k = k_ref[...]
    v = v_ref[...]

    def tile(i, mask):
        row0 = pl.multiple_of(i * BQ, BQ)
        rs = pl.ds(row0, BQ)
        dks, dvs = [], []
        for g in range(2):
            q = q_ref[rs, g * HEAD:(g + 1) * HEAD]
            do = do_ref[rs, g * HEAD:(g + 1) * HEAD]
            lse = lse_ref[0, g:g + 1, rs]
            dd = dd_ref[g, 0:1, rs]
            s = dotf(k, q, NT)
            u = jnp.tanh(s * k1)
            p = jnp.exp2(u * k2 - lse)
            if mask is not None:
                p = jnp.where(mask, p, 0.0)
            dp = dotf(v, do, NT)
            ds = (p * (dp - dd) * (1.0 - u * u)).astype(BF16)
            dvs.append(dotf(p.astype(BF16), do, NN))
            dks.append(dotf(ds, q, NN))
            dqa_ref[g, rs, :] += dotf(ds, k, TN)
        dva_ref[...] += dvs[0] + dvs[1]
        dka_ref[...] += dks[0] + dks[1]

    kpos = lax.broadcasted_iota(jnp.int32, (BK, BQ), 0)
    qpos = lax.broadcasted_iota(jnp.int32, (BK, BQ), 1)
    for m in range(r):
        tile(J * r + m, qpos + m * BQ >= kpos)

    def body(i, carry):
        tile(i, None)
        return carry

    lax.fori_loop(J * r + r, nq, body, 0)

    krow = pl.ds(pl.multiple_of(J * BK, BK), BK)

    def unrope(g, cos, sin):
        return (g * cos - pltpu.roll(g, HEAD // 2, 1) * sin) * scale

    dk_ref[...] = unrope(dka_ref[...], cos_ref[krow, :], sin_ref[krow, :]).astype(BF16)
    dv_ref[...] = dva_ref[...].astype(BF16)
    for g in range(2):
        dq_ref[:, g * HEAD:(g + 1) * HEAD] = unrope(dqa_ref[g, krow, :], cos_ref[krow, :], sin_ref[krow, :]).astype(BF16)


def attn_bwd(q, k, v, do, ctx, lse, cos, sin):
    T, kvh = q.shape[0], k.shape[1] // HEAD
    scale = HEAD ** -0.5
    full2 = pl.BlockSpec((T, 2 * HEAD), lambda h, j: (0, h))
    kblk = pl.BlockSpec((BK, HEAD), lambda h, j: (j, h))
    tab = pl.BlockSpec((T, HEAD), lambda h, j: (0, 0))
    return pl.pallas_call(
        functools.partial(attn_bwd_kernel, k1=scale / SOFT_CAP, k2=SOFT_CAP * LOG2E, scale=scale),
        grid=(kvh, T // BK),
        in_specs=[full2, kblk, kblk, full2, full2, pl.BlockSpec((1, 2, T), lambda h, j: (h, 0, 0)), tab, tab],
        out_specs=[pl.BlockSpec((BK, 2 * HEAD), lambda h, j: (j, h)), kblk, kblk],
        out_shape=[
            jax.ShapeDtypeStruct(q.shape, BF16),
            jax.ShapeDtypeStruct(k.shape, BF16),
            jax.ShapeDtypeStruct(v.shape, BF16),
        ],
        scratch_shapes=[
            pltpu.VMEM((2, T, HEAD), F32),
            pltpu.VMEM((BK, HEAD), F32),
            pltpu.VMEM((BK, HEAD), F32),
            pltpu.VMEM((2, 1, T), F32),
        ],
        compiler_params=pltpu.CompilerParams(dimension_semantics=("arbitrary", "arbitrary")),
        cost_estimate=pl.CostEstimate(flops=int(5 * 2 * T * T * HEAD * kvh), bytes_accessed=6 * q.size * 2, transcendentals=0),
        name="attn_bwd",
    )(q, k, v, do, ctx, lse, cos, sin)


def dw_kernel(a_ref, g0_ref, g1_ref, out_ref, *, nh):
    db = a_ref.shape[1]
    half = nh // 2
    at = a_ref[...].T
    for c, g_ref in enumerate((g0_ref, g1_ref)):
        res = dotf(at, g_ref[...], NN)
        for h in range(half):
            out_ref[pl.ds(c * half + h, db, stride=nh), :] = res[:, h * HEAD:(h + 1) * HEAD]


def dw_proj(a, g0, g1, db):
    T, D = a.shape
    cols = g0.shape[1]
    nh = 2 * cols // HEAD
    out = pl.pallas_call(
        functools.partial(dw_kernel, nh=nh),
        grid=(D // db,),
        in_specs=[
            pl.BlockSpec((T, db), lambda i: (0, i)),
            pl.BlockSpec((T, cols), lambda i: (0, 0)),
            pl.BlockSpec((T, cols), lambda i: (0, 0)),
        ],
        out_specs=pl.BlockSpec((db * nh, HEAD), lambda i: (i, 0)),
        out_shape=jax.ShapeDtypeStruct((D * nh, HEAD), F32),
        compiler_params=pltpu.CompilerParams(dimension_semantics=("arbitrary",)),
        cost_estimate=pl.CostEstimate(flops=int(2 * T * D * nh * HEAD), bytes_accessed=D * nh * HEAD * 4 + 2 * a.size, transcendentals=0),
        name="dw_proj",
    )(a, g0, g1)
    return out.reshape(D, nh, HEAD)


def solution(mesh):
    core_perm = [(0, 1), (1, 0), (2, 3), (3, 2)]
    x_perm = [(0, 2), (2, 0), (1, 3), (3, 1)]
    tp_perm = [(0, 1), (1, 0)]

    def gather(blk, me):
        b1 = lax.ppermute(blk, 'cp', core_perm)
        b2 = lax.ppermute(blk, 'cp', x_perm)
        b3 = lax.ppermute(b2, 'cp', core_perm)
        n = blk.shape[0]
        out = jnp.zeros((4 * n,) + blk.shape[1:], blk.dtype)
        for rel, b in enumerate((blk, b1, b2, b3)):
            out = lax.dynamic_update_slice_in_dim(out, b, (me ^ rel) * n, 0)
        return out

    def device_fn(hidden, g_pre, w_q, w_k, w_v, w_o, g_post, d_out):
        tokens, D = hidden.shape
        T = 4 * tokens
        me = lax.axis_index('cp')
        core = me % 2
        HL = w_q.shape[1] // 2
        KL = w_k.shape[1] // 2
        cos, sin = rope_tables(T)
        row0 = me * tokens

        h_f32 = hidden.astype(F32)
        inv_pre = lax.rsqrt(jnp.mean(h_f32 * h_f32, axis=-1, keepdims=True) + NORM_EPS)
        a_loc = (h_f32 * inv_pre * g_pre).astype(BF16)
        a_all = gather(a_loc, me)

        def split(w, n):
            return [w[:, c * n:(c + 1) * n].reshape(D, n * HEAD) for c in range(2)]

        wq, wk, wv = split(w_q, HL), split(w_k, KL), split(w_v, KL)
        w_cat = [jnp.concatenate([wq[c], wk[c], wv[c]], axis=1) for c in range(2)]
        w_own = jnp.where(core == 0, w_cat[0], w_cat[1])
        qkv = jnp.dot(a_all, w_own, preferred_element_type=F32)

        def rope(x):
            x3 = x.reshape(T, -1, HEAD)
            lo, hi = x3[..., :HEAD // 2], x3[..., HEAD // 2:]
            c, s = cos[:, None, :HEAD // 2], sin[:, None, HEAD // 2:]
            return jnp.concatenate([lo * c - hi * s, hi * c + lo * s], axis=-1).reshape(x.shape).astype(BF16)

        q = rope(qkv[:, :HL * HEAD])
        k = rope(qkv[:, HL * HEAD:(HL + KL) * HEAD])
        v = qkv[:, (HL + KL) * HEAD:].astype(BF16)

        ctx, lse = attn_fwd(q, k, v)
        ctx_p = lax.ppermute(ctx, 'cp', core_perm)
        ctx_c = [jnp.where(core == 0, ctx, ctx_p), jnp.where(core == 0, ctx_p, ctx)]
        ctx_all = jnp.concatenate(ctx_c, axis=1)
        wo2 = w_o.reshape(2 * HL * HEAD, D)
        ctx_rows = lax.dynamic_slice_in_dim(ctx_all, row0, tokens, 0)
        o_part = jnp.dot(ctx_rows, wo2, preferred_element_type=F32).astype(BF16)
        o_peer = lax.ppermute(o_part, 'tp', tp_perm)
        o_sum = o_part.astype(F32) + o_peer.astype(F32)
        inv_post = lax.rsqrt(jnp.mean(o_sum * o_sum, axis=-1, keepdims=True) + NORM_EPS)
        o_hat = o_sum * inv_post
        y_blk = (h_f32 + o_hat * g_post).astype(BF16)

        g_out = d_out.astype(F32)
        dgpost = jnp.sum(g_out * o_hat, axis=0)
        gg = g_out * g_post
        grad_o = (inv_post * (gg - o_hat * jnp.mean(gg * o_hat, axis=-1, keepdims=True))).astype(BF16)
        go_all = gather(grad_o, me)

        wo_own = lax.dynamic_slice_in_dim(wo2, core * HL * HEAD, HL * HEAD, 0)
        dctx = lax.dot_general(go_all, wo_own, NT, preferred_element_type=F32).astype(BF16)
        dq, dk, dv = attn_bwd(q, k, v, dctx, ctx, lse, cos, sin)

        def both(g):
            gp = lax.ppermute(g, 'cp', core_perm)
            return jnp.where(core == 0, g, gp), jnp.where(core == 0, gp, g)

        dqs, dks, dvs = both(dq), both(dk), both(dv)
        rows = [lax.dynamic_slice_in_dim(g, row0, tokens, 0) for c in range(2) for g in (dqs[c], dks[c], dvs[c])]
        drow = jnp.concatenate(rows, axis=1)
        w_all = jnp.concatenate(w_cat, axis=1)
        ga_part = lax.dot_general(drow, w_all, NT, preferred_element_type=F32).astype(BF16)
        ga_peer = lax.ppermute(ga_part, 'tp', tp_perm)

        dwo = lax.dot_general(ctx_all, go_all, TN, preferred_element_type=F32).reshape(w_o.shape)
        dwq = dw_proj(a_all, dqs[0], dqs[1], 256)
        dwk = dw_proj(a_all, dks[0], dks[1], 256)
        dwv = dw_proj(a_all, dvs[0], dvs[1], 256)

        ga = ga_part.astype(F32) + ga_peer.astype(F32)
        a_hat = h_f32 * inv_pre
        dgpre = jnp.sum(ga * a_hat, axis=0)
        gh = ga * g_pre
        grad_h = (g_out + inv_pre * (gh - a_hat * jnp.mean(gh * a_hat, axis=-1, keepdims=True))).astype(BF16)
        dg = jnp.stack([dgpre, dgpost])
        dg = dg + lax.ppermute(dg, 'cp', core_perm)
        dg = dg + lax.ppermute(dg, 'cp', x_perm)
        return y_blk, grad_h, dg[0], dwq, dwk, dwv, dwo, dg[1]

    row_spec = P('cp', None)
    head_spec = P(None, 'tp', None)
    out_head_spec = P('tp', None, None)
    return jax.shard_map(device_fn, mesh=mesh, in_specs=(row_spec, P(), head_spec, head_spec, head_spec, out_head_spec, P(), row_spec), out_specs=(row_spec, row_spec, P(), head_spec, head_spec, head_spec, out_head_spec, P()), check_vma=False)
```

```python
import functools

import jax
import jax.numpy as jnp
from jax import lax
from jax.experimental import pallas as pl
from jax.experimental.pallas import tpu as pltpu
from jax.sharding import PartitionSpec as P


SOFT_CAP = 30.0
NORM_EPS = 1e-5
ROPE_THETA = 10000.0
HEAD = 128
LOG2E = 1.4426950408889634
F32 = jnp.float32
BF16 = jnp.bfloat16

NT = (((1,), (1,)), ((), ()))
NN = (((1,), (0,)), ((), ()))
TN = (((0,), (0,)), ((), ()))


def dotf(a, b, dims):
    return lax.dot_general(a, b, dims, preferred_element_type=F32)


def rope_tables(length):
    half = HEAD // 2
    inv_freq = ROPE_THETA ** (-jnp.arange(half, dtype=F32) * 2.0 / HEAD)
    ang = jnp.arange(length).astype(F32)[:, None] * inv_freq[None, :]
    cos, sin = jnp.cos(ang), jnp.sin(ang)
    return jnp.concatenate([cos, cos], axis=-1), jnp.concatenate([-sin, sin], axis=-1)


QB = 256
KB = 256


def attn_fwd_kernel(q_ref, k_ref, v_ref, ctx_ref, lse_ref, acc_ref, sum_ref, *, k1, k2):
    i = pl.program_id(1)
    q = jnp.concatenate([q_ref[:, :HEAD], q_ref[:, HEAD:]], axis=0)
    acc_ref[...] = jnp.zeros_like(acc_ref)
    sum_ref[...] = jnp.zeros_like(sum_ref)

    def chunk(row0, mask):
        k = k_ref[pl.ds(row0, KB), :]
        v = v_ref[pl.ds(row0, KB), :]
        s = dotf(q, k, NT)
        p = jnp.exp2(jnp.tanh(s * k1) * k2)
        if mask is not None:
            p = jnp.where(mask, p, 0.0)
        part = p[:, :128]
        for c in range(1, KB // 128):
            part = part + p[:, c * 128:(c + 1) * 128]
        return part, dotf(p.astype(BF16), v, NN)

    def pair(j, carry):
        s0, a0 = chunk(pl.multiple_of(j * (2 * KB), 2 * KB), None)
        s1, a1 = chunk(pl.multiple_of(j * (2 * KB) + KB, KB), None)
        acc_ref[...] += a0 + a1
        sum_ref[...] += s0 + s1
        return carry

    lax.fori_loop(0, i // 2, pair, 0)

    @pl.when(i % 2 == 1)
    def _():
        s0, a0 = chunk(pl.multiple_of((i - 1) * KB, KB), None)
        acc_ref[...] += a0
        sum_ref[...] += s0

    rows = lax.broadcasted_iota(jnp.int32, (2 * QB, KB), 0) % QB
    cols = lax.broadcasted_iota(jnp.int32, (2 * QB, KB), 1)
    s0, a0 = chunk(pl.multiple_of(i * KB, KB), rows >= cols)
    total = jnp.sum(sum_ref[...] + s0, axis=1, keepdims=True)
    ctx = ((acc_ref[...] + a0) / total).astype(BF16)
    ctx_ref[:, :HEAD] = ctx[:QB]
    ctx_ref[:, HEAD:] = ctx[QB:]
    lse = jnp.broadcast_to(jnp.log2(total), (2 * QB, 128)).T
    lse_ref[0, 0:1, :] = lse[0:1, :QB]
    lse_ref[0, 1:2, :] = lse[0:1, QB:]


def attn_fwd(qkv, kvh, nq):
    T = qkv.shape[0]
    scale = HEAD ** -0.5
    return pl.pallas_call(
        functools.partial(attn_fwd_kernel, k1=scale / SOFT_CAP, k2=SOFT_CAP * LOG2E),
        grid=(kvh, T // QB),
        in_specs=[
            pl.BlockSpec((QB, 2 * HEAD), lambda h, i: (i, h)),
            pl.BlockSpec((T, HEAD), lambda h, i: (0, nq + h)),
            pl.BlockSpec((T, HEAD), lambda h, i: (0, nq + kvh + h)),
        ],
        out_specs=[
            pl.BlockSpec((QB, 2 * HEAD), lambda h, i: (i, h)),
            pl.BlockSpec((1, 2, QB), lambda h, i: (h, 0, i)),
        ],
        out_shape=[
            jax.ShapeDtypeStruct((T, nq * HEAD), BF16),
            jax.ShapeDtypeStruct((kvh, 2, T), F32),
        ],
        scratch_shapes=[pltpu.VMEM((2 * QB, HEAD), F32), pltpu.VMEM((2 * QB, 128), F32)],
        compiler_params=pltpu.CompilerParams(dimension_semantics=("arbitrary", "arbitrary")),
        cost_estimate=pl.CostEstimate(flops=int(2 * 2 * T * T * HEAD * kvh * 2), bytes_accessed=2 * qkv.size * 2, transcendentals=0),
        name="attn_fwd",
    )(qkv, qkv, qkv)


BQ = 256
BK = 512


def attn_bwd_kernel(q_ref, k_ref, v_ref, do_ref, ctx_ref, lse_ref, cos_ref, sin_ref, dq_ref, dk_ref, dv_ref,
                    dqa_ref, dka_ref, dva_ref, dd_ref, *, k1, k2, scale):
    J = pl.program_id(1)
    nq = q_ref.shape[0] // BQ
    r = BK // BQ

    @pl.when(J == 0)
    def _():
        dqa_ref[...] = jnp.zeros_like(dqa_ref)
        for g in range(2):
            for i in range(nq):
                sl = slice(i * BQ, (i + 1) * BQ)
                prod = do_ref[sl, g * HEAD:(g + 1) * HEAD].astype(F32) * ctx_ref[sl, g * HEAD:(g + 1) * HEAD].astype(F32)
                dd_ref[g, 0:1, sl] = jnp.sum(prod.T, axis=0, keepdims=True)

    dka_ref[...] = jnp.zeros_like(dka_ref)
    dva_ref[...] = jnp.zeros_like(dva_ref)
    k = k_ref[...]
    v = v_ref[...]

    def tile(i, mask):
        row0 = pl.multiple_of(i * BQ, BQ)
        rs = pl.ds(row0, BQ)
        dks, dvs = [], []
        for g in range(2):
            q = q_ref[rs, g * HEAD:(g + 1) * HEAD]
            do = do_ref[rs, g * HEAD:(g + 1) * HEAD]
            lse = lse_ref[0, g:g + 1, rs]
            dd = dd_ref[g, 0:1, rs]
            s = dotf(k, q, NT)
            u = jnp.tanh(s * k1)
            p = jnp.exp2(u * k2 - lse)
            if mask is not None:
                p = jnp.where(mask, p, 0.0)
            dp = dotf(v, do, NT)
            ds = (p * (dp - dd) * (1.0 - u * u)).astype(BF16)
            dvs.append(dotf(p.astype(BF16), do, NN))
            dks.append(dotf(ds, q, NN))
            dqa_ref[g, rs, :] += dotf(ds, k, TN)
        dva_ref[...] += dvs[0] + dvs[1]
        dka_ref[...] += dks[0] + dks[1]

    kpos = lax.broadcasted_iota(jnp.int32, (BK, BQ), 0)
    qpos = lax.broadcasted_iota(jnp.int32, (BK, BQ), 1)
    for m in range(r):
        tile(J * r + m, qpos + m * BQ >= kpos)

    def body(i, carry):
        tile(i, None)
        return carry

    lax.fori_loop(J * r + r, nq, body, 0)

    krow = pl.ds(pl.multiple_of(J * BK, BK), BK)

    def unrope(g, cos, sin):
        return (g * cos - pltpu.roll(g, HEAD // 2, 1) * sin) * scale

    dk_ref[...] = unrope(dka_ref[...], cos_ref[krow, :], sin_ref[krow, :]).astype(BF16)
    dv_ref[...] = dva_ref[...].astype(BF16)
    for g in range(2):
        dq_ref[:, g * HEAD:(g + 1) * HEAD] = unrope(dqa_ref[g, krow, :], cos_ref[krow, :], sin_ref[krow, :]).astype(BF16)


def attn_bwd(qkv, kvh, nq, do, ctx, lse, cos, sin):
    T = qkv.shape[0]
    scale = HEAD ** -0.5
    full2 = pl.BlockSpec((T, 2 * HEAD), lambda h, j: (0, h))
    kblk = pl.BlockSpec((BK, HEAD), lambda h, j: (j, h))
    tab = pl.BlockSpec((T, HEAD), lambda h, j: (0, 0))
    return pl.pallas_call(
        functools.partial(attn_bwd_kernel, k1=scale / SOFT_CAP, k2=SOFT_CAP * LOG2E, scale=scale),
        grid=(kvh, T // BK),
        in_specs=[full2, pl.BlockSpec((BK, HEAD), lambda h, j: (j, nq + h)), pl.BlockSpec((BK, HEAD), lambda h, j: (j, nq + kvh + h)), full2, full2, pl.BlockSpec((1, 2, T), lambda h, j: (h, 0, 0)), tab, tab],
        out_specs=[pl.BlockSpec((BK, 2 * HEAD), lambda h, j: (j, h)), kblk, kblk],
        out_shape=[
            jax.ShapeDtypeStruct((T, nq * HEAD), BF16),
            jax.ShapeDtypeStruct((T, kvh * HEAD), BF16),
            jax.ShapeDtypeStruct((T, kvh * HEAD), BF16),
        ],
        scratch_shapes=[
            pltpu.VMEM((2, T, HEAD), F32),
            pltpu.VMEM((BK, HEAD), F32),
            pltpu.VMEM((BK, HEAD), F32),
            pltpu.VMEM((2, 1, T), F32),
        ],
        compiler_params=pltpu.CompilerParams(dimension_semantics=("arbitrary", "arbitrary")),
        cost_estimate=pl.CostEstimate(flops=int(5 * 2 * T * T * HEAD * kvh), bytes_accessed=3 * qkv.size * 2, transcendentals=0),
        name="attn_bwd",
    )(qkv, qkv, qkv, do, ctx, lse, cos, sin)


VMEM_LIMIT = 64_000_000


def gmm_kernel(sc_ref, *refs, layout, rope_blocks, n_w, w_of, aliased):
    np_ = len(layout)
    pieces = refs[:np_]
    ws = refs[np_:np_ + n_w]
    cos_ref, sin_ref = refs[np_ + n_w:np_ + n_w + 2]
    rest = refs[np_ + n_w + 2:]
    if aliased:
        rest = rest[2:]
    out_ref, all_ref, x_ref, sem_in, sem_out = rest
    n = pl.program_id(0)
    last = pl.num_programs(0) - 1
    half = x_ref.shape[0]
    xt = sc_ref[0]
    dst = pl.multiple_of(xt * half, half)

    def off(i):
        return pl.multiple_of(sc_ref[1 + i], 16)

    def cp_in(i):
        return pltpu.make_async_copy(pieces[i], x_ref.at[pl.ds(off(i), layout[i])], sem_in.at[i])

    def cp_out():
        return pltpu.make_async_copy(x_ref, all_ref.at[pl.ds(dst, half)], sem_out)

    @pl.when(n == 0)
    def _():
        for i in range(np_):
            cp_in(i).start()
        for i in range(np_):
            cp_in(i).wait()
        cp_out().start()

    for b, wi in enumerate(w_of):
        @pl.when(n == b)
        def _(b=b, wi=wi):
            res = dotf(x_ref[...], ws[wi][...], NT)
            if b in rope_blocks:
                c, s = cos_ref[...], sin_ref[...]
                for h in range(res.shape[1] // HEAD):
                    r = res[:, h * HEAD:(h + 1) * HEAD]
                    out_ref[:, h * HEAD:(h + 1) * HEAD] = (r * c + pltpu.roll(r, HEAD // 2, 1) * s).astype(BF16)
            else:
                out_ref[...] = res.astype(BF16)

    @pl.when(n == last)
    def _():
        cp_out().wait()


def gather_matmul(scal, pieces, ws, w_maps, w_of, rope_blocks, cos, sin, T, nb, bufs=None):
    D = pieces[0].shape[1]
    half = T // 2
    nblk = len(w_of)
    layout = tuple(p.shape[0] for p in pieces)
    anyspec = pl.BlockSpec(memory_space=pl.ANY)
    tab = pl.BlockSpec((half, HEAD), lambda n, s: (s[0], 0), pipeline_mode=pl.Buffered(1))
    in_specs = [anyspec] * len(pieces) + [pl.BlockSpec((nb, D), m) for m in w_maps] + [tab, tab]
    args = list(pieces) + list(ws) + [cos, sin]
    aliases = {}
    if bufs is not None:
        aliases = {1 + len(args): 0, 2 + len(args): 1}
        in_specs += [anyspec, anyspec]
        args += list(bufs)
    return pl.pallas_call(
        functools.partial(gmm_kernel, layout=layout, rope_blocks=rope_blocks, n_w=len(ws), w_of=w_of, aliased=bufs is not None),
        grid_spec=pltpu.PrefetchScalarGridSpec(
            num_scalar_prefetch=1,
            grid=(nblk,),
            in_specs=in_specs,
            out_specs=[pl.BlockSpec((half, nb), lambda n, s: (s[0], n)), anyspec],
            scratch_shapes=[
                pltpu.VMEM((half, D), BF16),
                pltpu.SemaphoreType.DMA((len(pieces),)),
                pltpu.SemaphoreType.DMA,
            ],
        ),
        out_shape=[jax.ShapeDtypeStruct((T, nblk * nb), BF16), jax.ShapeDtypeStruct((T, D), BF16)],
        input_output_aliases=aliases,
        compiler_params=pltpu.CompilerParams(dimension_semantics=("arbitrary",), vmem_limit_bytes=VMEM_LIMIT),
        cost_estimate=pl.CostEstimate(flops=2 * half * D * nblk * nb, bytes_accessed=half * D * 4 + nblk * nb * D * 2, transcendentals=0),
    )(scal, *args)


def rows_kernel(sc_ref, *refs, parts):
    n_l = len(parts)
    n_w = 1 + max(p[0] for p in parts)
    lhs = refs[:n_l]
    ws = refs[n_l:n_l + n_w]
    out_ref = refs[n_l + n_w]
    core = sc_ref[1]
    acc = None
    for ref, (wi, other, rows) in zip(lhs, parts):
        c = 1 - core if other else core
        d = dotf(ref[...], ws[wi][pl.ds(pl.multiple_of(c * rows, rows), rows), :], NN)
        acc = d if acc is None else acc + d
    out_ref[...] = acc.astype(BF16)


def rows_matmul(scal, lhs, lhs_maps, ws, parts, M, db):
    D = ws[0].shape[1]
    flops = 2 * M * D * sum(p[2] for p in parts)
    return pl.pallas_call(
        functools.partial(rows_kernel, parts=tuple(parts)),
        grid_spec=pltpu.PrefetchScalarGridSpec(
            num_scalar_prefetch=1,
            grid=(D // db,),
            in_specs=[pl.BlockSpec((M, l.shape[1]), m) for l, m in zip(lhs, lhs_maps)]
            + [pl.BlockSpec((w.shape[0], db), lambda i, s: (0, i)) for w in ws],
            out_specs=pl.BlockSpec((M, db), lambda i, s: (0, i)),
        ),
        out_shape=jax.ShapeDtypeStruct((M, D), BF16),
        compiler_params=pltpu.CompilerParams(dimension_semantics=("arbitrary",), vmem_limit_bytes=VMEM_LIMIT),
        cost_estimate=pl.CostEstimate(flops=flops, bytes_accessed=sum(w.size for w in ws) * 2, transcendentals=0),
    )(scal, *lhs, *ws)


def dw_kernel(sc_ref, a_ref, q0, q1, k0, k1, v0, v1, oq_ref, ok_ref, ov_ref):
    db = a_ref.shape[1]
    core = sc_ref[1]
    at = a_ref[...].T
    for pair, out_ref in (((q0, q1), oq_ref), ((k0, k1), ok_ref), ((v0, v1), ov_ref)):
        hh = pair[0].shape[1] // HEAD
        nh = 2 * hh
        for other, g_ref in enumerate(pair):
            c = 1 - core if other else core
            res = dotf(at, g_ref[...], NN)
            for h in range(hh):
                out_ref[pl.ds(c * hh + h, db, stride=nh), :] = res[:, h * HEAD:(h + 1) * HEAD]


def dw_proj(scal, a, gs, db):
    T, D = a.shape
    nhs = [2 * gs[0].shape[1] // HEAD, 2 * gs[2].shape[1] // HEAD, 2 * gs[4].shape[1] // HEAD]
    outs = pl.pallas_call(
        dw_kernel,
        grid_spec=pltpu.PrefetchScalarGridSpec(
            num_scalar_prefetch=1,
            grid=(D // db,),
            in_specs=[pl.BlockSpec((T, db), lambda i, s: (0, i))]
            + [pl.BlockSpec(g.shape, lambda i, s: (0, 0), pipeline_mode=pl.Buffered(1)) for g in gs],
            out_specs=[pl.BlockSpec((db * nh, HEAD), lambda i, s: (i, 0)) for nh in nhs],
        ),
        out_shape=[jax.ShapeDtypeStruct((D * nh, HEAD), F32) for nh in nhs],
        compiler_params=pltpu.CompilerParams(dimension_semantics=("arbitrary",), vmem_limit_bytes=VMEM_LIMIT),
        cost_estimate=pl.CostEstimate(flops=2 * T * D * sum(nhs) * HEAD, bytes_accessed=D * sum(nhs) * HEAD * 4, transcendentals=0),
        name="dw_proj",
    )(scal, a, *gs)
    return [o.reshape(D, nh, HEAD) for o, nh in zip(outs, nhs)]


def dwo_kernel(sc_ref, c0_ref, c1_ref, g_ref, out_ref, t_ref):
    core = sc_ref[1]
    n = c0_ref.shape[1]

    @pl.when(pl.program_id(0) == 0)
    def _():
        t_ref[pl.ds(pl.multiple_of(core * n, n), n), :] = c0_ref[...].T
        t_ref[pl.ds(pl.multiple_of((1 - core) * n, n), n), :] = c1_ref[...].T

    out_ref[...] = dotf(t_ref[...], g_ref[...], NN)


def dwo_proj(scal, c0, c1, go, db):
    T, D = go.shape
    n = c0.shape[1]
    return pl.pallas_call(
        dwo_kernel,
        grid_spec=pltpu.PrefetchScalarGridSpec(
            num_scalar_prefetch=1,
            grid=(D // db,),
            in_specs=[pl.BlockSpec((T, n), lambda i, s: (0, 0), pipeline_mode=pl.Buffered(1))] * 2
            + [pl.BlockSpec((T, db), lambda i, s: (0, i))],
            out_specs=pl.BlockSpec((2 * n, db), lambda i, s: (0, i)),
            scratch_shapes=[pltpu.VMEM((2 * n, T), BF16)],
        ),
        out_shape=jax.ShapeDtypeStruct((2 * n, D), F32),
        compiler_params=pltpu.CompilerParams(dimension_semantics=("arbitrary",), vmem_limit_bytes=VMEM_LIMIT),
        cost_estimate=pl.CostEstimate(flops=4 * T * D * n, bytes_accessed=2 * n * D * 4, transcendentals=0),
        name="dwo_proj",
    )(scal, c0, c1, go)


RB = 64


def post_kernel(p_ref, r_ref, h_ref, dy_ref, g_ref, *rest):
    y_ref, go_ref, dg_ref = rest[-3:]
    o = p_ref[...].astype(F32) + r_ref[...].astype(F32)
    inv = lax.rsqrt(jnp.mean(o * o, axis=-1, keepdims=True) + NORM_EPS)
    hat = o * inv
    g = g_ref[...]
    dy = dy_ref[...].astype(F32)
    y_ref[...] = (h_ref[...].astype(F32) + hat * g).astype(BF16)
    gg = dy * g
    go_ref[...] = (inv * (gg - hat * jnp.mean(gg * hat, axis=-1, keepdims=True))).astype(BF16)

    @pl.when(pl.program_id(0) == 0)
    def _():
        dg_ref[...] = jnp.zeros_like(dg_ref)

    dg_ref[...] += jnp.sum((dy * hat).reshape(RB // 8, 8, -1), axis=0)


def pre_kernel(p_ref, r_ref, h_ref, dy_ref, g_ref, *rest):
    dh_ref, dg_ref = rest[-2:]
    ga = p_ref[...].astype(F32) + r_ref[...].astype(F32)
    h = h_ref[...].astype(F32)
    inv = lax.rsqrt(jnp.mean(h * h, axis=-1, keepdims=True) + NORM_EPS)
    hat = h * inv
    gh = ga * g_ref[...]
    dh_ref[...] = (dy_ref[...].astype(F32) + inv * (gh - hat * jnp.mean(gh * hat, axis=-1, keepdims=True))).astype(BF16)

    @pl.when(pl.program_id(0) == 0)
    def _():
        dg_ref[...] = jnp.zeros_like(dg_ref)

    dg_ref[...] += jnp.sum((ga * hat).reshape(RB // 8, 8, -1), axis=0)


def norm_call(kernel, part, peer, hidden, d_out, g, c, buf, extra):
    M, D = part.shape
    n = M // RB
    loc = pl.BlockSpec((RB, D), lambda i: (i, 0))
    row = pl.BlockSpec((RB, D), lambda i: (c * n + i, 0))
    in_specs = [loc, loc, row, row, pl.BlockSpec((1, D), lambda i: (0, 0))]
    args = [part, peer, hidden, d_out, g.reshape(1, D)]
    aliases = {}
    if buf is not None:
        aliases = {len(args): 0}
        args.append(buf)
        in_specs.append(pl.BlockSpec(memory_space=pl.ANY))
    out_specs = [row] + ([loc] if extra else []) + [pl.BlockSpec((8, D), lambda i: (0, 0))]
    out_shape = [jax.ShapeDtypeStruct(hidden.shape, BF16)]
    if extra:
        out_shape.append(jax.ShapeDtypeStruct((M, D), BF16))
    out_shape.append(jax.ShapeDtypeStruct((8, D), F32))
    return pl.pallas_call(
        kernel, grid=(n,), in_specs=in_specs, out_specs=out_specs, out_shape=out_shape, input_output_aliases=aliases,
        compiler_params=pltpu.CompilerParams(dimension_semantics=("arbitrary",), vmem_limit_bytes=VMEM_LIMIT),
        cost_estimate=pl.CostEstimate(flops=M * D * 2000, bytes_accessed=M * D * 12, transcendentals=0),
    )(*args)


def a_kernel(h_ref, g_ref, a_ref):
    h = h_ref[...].astype(F32)
    inv = lax.rsqrt(jnp.mean(h * h, axis=-1, keepdims=True) + NORM_EPS)
    a_ref[...] = (h * inv * g_ref[...]).astype(BF16)


def a_call(hidden, g):
    M, D = hidden.shape
    row = pl.BlockSpec((RB, D), lambda i: (i, 0))
    return pl.pallas_call(
        a_kernel, grid=(M // RB,), in_specs=[row, pl.BlockSpec((1, D), lambda i: (0, 0))], out_specs=row,
        out_shape=jax.ShapeDtypeStruct((M, D), BF16),
        compiler_params=pltpu.CompilerParams(dimension_semantics=("arbitrary",)),
        cost_estimate=pl.CostEstimate(flops=M * D * 1000, bytes_accessed=M * D * 4, transcendentals=0),
        name="a_norm",
    )(hidden, g.reshape(1, D))


def solution(mesh):
    core_perm = [(0, 1), (1, 0), (2, 3), (3, 2)]
    x_perm = [(0, 2), (2, 0), (1, 3), (3, 1)]
    tp_perm = [(0, 1), (1, 0)]

    def to_core(v):
        return lax.ppermute(v, 'cp', core_perm)

    def to_x(v):
        return lax.ppermute(v, 'cp', x_perm)

    def to_tp(v):
        return lax.ppermute(v, 'tp', tp_perm)

    def device_fn(hidden, g_pre, w_q, w_k, w_v, w_o, g_post, d_out):
        tokens, D = hidden.shape
        T = 4 * tokens
        me = lax.axis_index('cp')
        tp = lax.axis_index('tp')
        core, xi = me % 2, me // 2
        HL = w_q.shape[1] // 2
        KL = w_k.shape[1] // 2
        cos, sin = rope_tables(T)
        base = jnp.stack([xi, core, me, me ^ 1]).astype(jnp.int32)
        mine, other = core * tokens, (1 - core) * tokens

        def two_way(blk, n):
            r1 = to_x(lax.dynamic_slice_in_dim(blk, tp * n, n, 0))
            r3 = to_x(blk[2 * n:])
            r2 = to_tp(r1)
            return [r1, r2, r3], [tp * n, (1 - tp) * n, 2 * n]

        def scalars(x_t, offs):
            return jnp.stack([x_t] + [jnp.asarray(o) for o in offs]).astype(jnp.int32)

        a_loc = a_call(hidden, g_pre)
        a_x, a_off = two_way(a_loc, 176)
        a_p = to_core(a_loc)
        a_xp = [to_core(r) for r in a_x]

        def w_t(w):
            return jnp.transpose(w, (1, 2, 0)).reshape(-1, D)

        wqt = w_t(w_q)
        wkt, wvt = w_t(w_k), w_t(w_v)
        wo2 = w_o.reshape(-1, D)
        nb = KL * HEAD
        ws = (wqt, wkt, wvt)
        nq = HL // KL

        def maps(ncore):
            return [
                lambda n, s: (s[ncore] * nq + jnp.minimum(n, nq - 1), 0),
                lambda n, s: (s[ncore], 0),
                lambda n, s: (s[ncore], 0),
            ]

        w_of = (0,) * nq + (1, 2)
        ropes = tuple(range(nq + 1))
        qkv, a_all = gather_matmul(scalars(xi, [mine, other, core]), [a_loc, a_p], ws, maps(3), w_of, ropes, cos, sin, T, nb)
        offs = [mine + o for o in a_off] + [other + o for o in a_off]
        qkv, a_all = gather_matmul(scalars(1 - xi, offs + [core]), a_x + a_xp, ws, maps(7), w_of, ropes, cos, sin, T, nb, bufs=(qkv, a_all))

        ctx, lse = attn_fwd(qkv, KL, HL)
        ctx_pr = to_core(lax.dynamic_slice_in_dim(ctx, (me ^ 1) * tokens, tokens, 0))
        nc = 2
        M = tokens // nc
        o_parts, o_peers = [], []
        for c in range(nc):
            op = rows_matmul(base, [ctx, ctx_pr], [lambda i, s, c=c: (s[2] * nc + c, 0), lambda i, s, c=c: (c, 0)],
                             [wo2], [(0, False, HL * HEAD), (0, True, HL * HEAD)], M, 768)
            o_parts.append(op)
            o_peers.append(to_tp(op))
        ctx_p = to_core(ctx)

        y_blk, gos, dgp = None, [], []
        for c in range(nc):
            y_blk, go, dg_ = norm_call(post_kernel, o_parts[c], o_peers[c], hidden, d_out, g_post, c, y_blk, True)
            gos.append(go)
            dgp.append(dg_)

        gx = [to_x(gos[0])]
        gx_off = [0]
        gp = [to_core(g) for g in gos]
        r, ro = two_way(gos[1], 96)
        gx += r
        gx_off += [M + o for o in ro]
        gxp = [to_core(g) for g in gx]
        own_off = [c * M for c in range(nc)]
        wo_map = lambda idx: [lambda n, s: (s[idx] * nq + n, 0)]
        offs = [mine + o for o in own_off] + [other + o for o in own_off]
        dctx, go_all = gather_matmul(scalars(xi, offs + [core]), gos + gp, (wo2,), wo_map(5), (0,) * nq, (), cos, sin, T, nb)
        offs = [mine + o for o in gx_off] + [other + o for o in gx_off]
        dctx, go_all = gather_matmul(scalars(1 - xi, offs + [core]), gx + gxp, (wo2,), wo_map(9), (0,) * nq, (), cos, sin, T, nb, bufs=(dctx, go_all))

        dqkv = attn_bwd(qkv, KL, HL, dctx, ctx, lse, cos, sin)
        dqkv_pr = [to_core(lax.dynamic_slice_in_dim(g, (me ^ 1) * tokens, tokens, 0)) for g in dqkv]
        dqkv_p = [to_core(g) for g in dqkv]
        ga_parts, ga_peers = [], []
        sizes = [HL * HEAD, KL * HEAD, KL * HEAD]
        for c in range(nc):
            gp_ = rows_matmul(base, list(dqkv) + dqkv_pr,
                              [lambda i, s, c=c: (s[2] * nc + c, 0)] * 3 + [lambda i, s, c=c: (c, 0)] * 3,
                              [wqt, wkt, wvt], [(j, o, sizes[j]) for o in (False, True) for j in range(3)], M, 512)
            ga_parts.append(gp_)
            ga_peers.append(to_tp(gp_))

        dwo = dwo_proj(base, ctx, ctx_p, go_all, 512).reshape(w_o.shape)
        dwq, dwk, dwv = dw_proj(base, a_all, [g for pair in zip(dqkv, dqkv_p) for g in pair], 256)

        grad_h, dgr = None, []
        for c in range(nc):
            grad_h, dg_ = norm_call(pre_kernel, ga_parts[c], ga_peers[c], hidden, d_out, g_pre, c, grad_h, False)
            dgr.append(dg_)
        dg = jnp.stack([sum(jnp.sum(v, axis=0) for v in dgr), sum(jnp.sum(v, axis=0) for v in dgp)])
        dg = dg + to_core(dg)
        dg = dg + to_x(dg)
        return y_blk, grad_h, dg[0], dwq, dwk, dwv, dwo, dg[1]


    row_spec = P('cp', None)
    head_spec = P(None, 'tp', None)
    out_head_spec = P('tp', None, None)
    return jax.shard_map(device_fn, mesh=mesh, in_specs=(row_spec, P(), head_spec, head_spec, head_spec, out_head_spec, P(), row_spec), out_specs=(row_spec, row_spec, P(), head_spec, head_spec, head_spec, out_head_spec, P()), check_vma=False)
```

```python
import functools

import jax
import jax.numpy as jnp
from jax import lax
from jax.experimental import pallas as pl
from jax.experimental.pallas import tpu as pltpu
from jax.sharding import PartitionSpec as P


SOFT_CAP = 30.0
NORM_EPS = 1e-5
ROPE_THETA = 10000.0
HEAD = 128
LOG2E = 1.4426950408889634
F32 = jnp.float32
BF16 = jnp.bfloat16

NT = (((1,), (1,)), ((), ()))
NN = (((1,), (0,)), ((), ()))
TN = (((0,), (0,)), ((), ()))


def dotf(a, b, dims):
    return lax.dot_general(a, b, dims, preferred_element_type=F32)


def rope_tables(length):
    half = HEAD // 2
    inv_freq = ROPE_THETA ** (-jnp.arange(half, dtype=F32) * 2.0 / HEAD)
    ang = jnp.arange(length).astype(F32)[:, None] * inv_freq[None, :]
    cos, sin = jnp.cos(ang), jnp.sin(ang)
    return jnp.concatenate([cos, cos], axis=-1), jnp.concatenate([-sin, sin], axis=-1)


QB = 256
KB = 256


def attn_fwd_kernel(q_ref, k_ref, v_ref, ctx_ref, lse_ref, acc_ref, sum_ref, *, k1, k2):
    i = pl.program_id(1)
    q = jnp.concatenate([q_ref[:, :HEAD], q_ref[:, HEAD:]], axis=0)
    acc_ref[...] = jnp.zeros_like(acc_ref)
    sum_ref[...] = jnp.zeros_like(sum_ref)

    def chunk(row0, mask):
        k = k_ref[pl.ds(row0, KB), :]
        v = v_ref[pl.ds(row0, KB), :]
        s = dotf(q, k, NT)
        p = jnp.exp2(jnp.tanh(s * k1) * k2)
        if mask is not None:
            p = jnp.where(mask, p, 0.0)
        part = p[:, :128]
        for c in range(1, KB // 128):
            part = part + p[:, c * 128:(c + 1) * 128]
        return part, dotf(p.astype(BF16), v, NN)

    def pair(j, carry):
        s0, a0 = chunk(pl.multiple_of(j * (2 * KB), 2 * KB), None)
        s1, a1 = chunk(pl.multiple_of(j * (2 * KB) + KB, KB), None)
        acc_ref[...] += a0 + a1
        sum_ref[...] += s0 + s1
        return carry

    lax.fori_loop(0, i // 2, pair, 0)

    @pl.when(i % 2 == 1)
    def _():
        s0, a0 = chunk(pl.multiple_of((i - 1) * KB, KB), None)
        acc_ref[...] += a0
        sum_ref[...] += s0

    rows = lax.broadcasted_iota(jnp.int32, (2 * QB, KB), 0) % QB
    cols = lax.broadcasted_iota(jnp.int32, (2 * QB, KB), 1)
    s0, a0 = chunk(pl.multiple_of(i * KB, KB), rows >= cols)
    total = jnp.sum(sum_ref[...] + s0, axis=1, keepdims=True)
    ctx = ((acc_ref[...] + a0) / total).astype(BF16)
    ctx_ref[:, :HEAD] = ctx[:QB]
    ctx_ref[:, HEAD:] = ctx[QB:]
    lse = jnp.broadcast_to(jnp.log2(total), (2 * QB, 128)).T
    lse_ref[0, 0:1, :] = lse[0:1, :QB]
    lse_ref[0, 1:2, :] = lse[0:1, QB:]


def attn_fwd(qkv, kvh, nq):
    T = qkv.shape[0]
    scale = HEAD ** -0.5
    return pl.pallas_call(
        functools.partial(attn_fwd_kernel, k1=scale / SOFT_CAP, k2=SOFT_CAP * LOG2E),
        grid=(kvh, T // QB),
        in_specs=[
            pl.BlockSpec((QB, 2 * HEAD), lambda h, i: (i, h)),
            pl.BlockSpec((T, HEAD), lambda h, i: (0, nq + h)),
            pl.BlockSpec((T, HEAD), lambda h, i: (0, nq + kvh + h)),
        ],
        out_specs=[
            pl.BlockSpec((QB, 2 * HEAD), lambda h, i: (i, h)),
            pl.BlockSpec((1, 2, QB), lambda h, i: (h, 0, i)),
        ],
        out_shape=[
            jax.ShapeDtypeStruct((T, nq * HEAD), BF16),
            jax.ShapeDtypeStruct((kvh, 2, T), F32),
        ],
        scratch_shapes=[pltpu.VMEM((2 * QB, HEAD), F32), pltpu.VMEM((2 * QB, 128), F32)],
        compiler_params=pltpu.CompilerParams(dimension_semantics=("arbitrary", "arbitrary")),
        cost_estimate=pl.CostEstimate(flops=int(2 * 2 * T * T * HEAD * kvh * 2), bytes_accessed=2 * qkv.size * 2, transcendentals=0),
        name="attn_fwd",
    )(qkv, qkv, qkv)


BQ = 256
BK = 512


def attn_bwd_kernel(q_ref, k_ref, v_ref, do_ref, ctx_ref, lse_ref, cos_ref, sin_ref, dq_ref, dk_ref, dv_ref,
                    dqa_ref, dka_ref, dva_ref, dd_ref, *, k1, k2, scale):
    J = pl.program_id(1)
    nq = q_ref.shape[0] // BQ
    r = BK // BQ

    @pl.when(J == 0)
    def _():
        dqa_ref[...] = jnp.zeros_like(dqa_ref)
        for g in range(2):
            for i in range(nq):
                sl = slice(i * BQ, (i + 1) * BQ)
                prod = do_ref[sl, g * HEAD:(g + 1) * HEAD].astype(F32) * ctx_ref[sl, g * HEAD:(g + 1) * HEAD].astype(F32)
                dd_ref[g, 0:1, sl] = jnp.sum(prod.T, axis=0, keepdims=True)

    dka_ref[...] = jnp.zeros_like(dka_ref)
    dva_ref[...] = jnp.zeros_like(dva_ref)
    k = k_ref[...]
    v = v_ref[...]

    def tile(i, mask):
        row0 = pl.multiple_of(i * BQ, BQ)
        rs = pl.ds(row0, BQ)
        dks, dvs = [], []
        for g in range(2):
            q = q_ref[rs, g * HEAD:(g + 1) * HEAD]
            do = do_ref[rs, g * HEAD:(g + 1) * HEAD]
            lse = lse_ref[0, g:g + 1, rs]
            dd = dd_ref[g, 0:1, rs]
            s = dotf(k, q, NT)
            u = jnp.tanh(s * k1)
            p = jnp.exp2(u * k2 - lse)
            if mask is not None:
                p = jnp.where(mask, p, 0.0)
            dp = dotf(v, do, NT)
            ds = (p * (dp - dd) * (1.0 - u * u)).astype(BF16)
            dvs.append(dotf(p.astype(BF16), do, NN))
            dks.append(dotf(ds, q, NN))
            dqa_ref[g, rs, :] += dotf(ds, k, TN)
        dva_ref[...] += dvs[0] + dvs[1]
        dka_ref[...] += dks[0] + dks[1]

    kpos = lax.broadcasted_iota(jnp.int32, (BK, BQ), 0)
    qpos = lax.broadcasted_iota(jnp.int32, (BK, BQ), 1)
    for m in range(r):
        tile(J * r + m, qpos + m * BQ >= kpos)

    def body(i, carry):
        tile(i, None)
        return carry

    lax.fori_loop(J * r + r, nq, body, 0)

    krow = pl.ds(pl.multiple_of(J * BK, BK), BK)

    def unrope(g, cos, sin):
        return (g * cos - pltpu.roll(g, HEAD // 2, 1) * sin) * scale

    dk_ref[...] = unrope(dka_ref[...], cos_ref[krow, :], sin_ref[krow, :]).astype(BF16)
    dv_ref[...] = dva_ref[...].astype(BF16)
    for g in range(2):
        dq_ref[:, g * HEAD:(g + 1) * HEAD] = unrope(dqa_ref[g, krow, :], cos_ref[krow, :], sin_ref[krow, :]).astype(BF16)


def attn_bwd(qkv, kvh, nq, do, ctx, lse, cos, sin):
    T = qkv.shape[0]
    scale = HEAD ** -0.5
    full2 = pl.BlockSpec((T, 2 * HEAD), lambda h, j: (0, h))
    kblk = pl.BlockSpec((BK, HEAD), lambda h, j: (j, h))
    tab = pl.BlockSpec((T, HEAD), lambda h, j: (0, 0))
    return pl.pallas_call(
        functools.partial(attn_bwd_kernel, k1=scale / SOFT_CAP, k2=SOFT_CAP * LOG2E, scale=scale),
        grid=(kvh, T // BK),
        in_specs=[full2, pl.BlockSpec((BK, HEAD), lambda h, j: (j, nq + h)), pl.BlockSpec((BK, HEAD), lambda h, j: (j, nq + kvh + h)), full2, full2, pl.BlockSpec((1, 2, T), lambda h, j: (h, 0, 0)), tab, tab],
        out_specs=[pl.BlockSpec((BK, 2 * HEAD), lambda h, j: (j, h)), kblk, kblk],
        out_shape=[
            jax.ShapeDtypeStruct((T, nq * HEAD), BF16),
            jax.ShapeDtypeStruct((T, kvh * HEAD), BF16),
            jax.ShapeDtypeStruct((T, kvh * HEAD), BF16),
        ],
        scratch_shapes=[
            pltpu.VMEM((2, T, HEAD), F32),
            pltpu.VMEM((BK, HEAD), F32),
            pltpu.VMEM((BK, HEAD), F32),
            pltpu.VMEM((2, 1, T), F32),
        ],
        compiler_params=pltpu.CompilerParams(dimension_semantics=("arbitrary", "arbitrary")),
        cost_estimate=pl.CostEstimate(flops=int(5 * 2 * T * T * HEAD * kvh), bytes_accessed=3 * qkv.size * 2, transcendentals=0),
        name="attn_bwd",
    )(qkv, qkv, qkv, do, ctx, lse, cos, sin)


VMEM_LIMIT = 64_000_000
KD = 512


def load_pieces(pieces, layout, sc_ref, x_ref, sem):
    cps = []
    for i, (slot, n) in enumerate(layout):
        blk = sc_ref[slot]
        off = pl.multiple_of(sc_ref[slot + 1], 16)
        cps.append(pltpu.make_async_copy(pieces[i], x_ref.at[blk, pl.ds(off, n)], sem.at[i]))
    return cps


def gmm_kernel(sc_ref, *refs, layout, mode, n_w, R, r0, aliased):
    np_ = len(layout)
    pieces = refs[:np_]
    ws = refs[np_:np_ + n_w]
    rest = refs[np_ + n_w:]
    if mode == "qkv":
        cos_ref, sin_ref = rest[:2]
        rest = rest[2:]
    if aliased:
        rest = rest[2:]
    out_ref, all_ref, x_ref, acc_ref, w_ref, sem_in, sem_out = rest
    i = pl.program_id(0)
    last = pl.num_programs(0) - 1
    B = x_ref.shape[0]
    core = sc_ref[1]
    cps = load_pieces(pieces, layout, sc_ref, x_ref, sem_in)
    outs = [pltpu.make_async_copy(x_ref.at[b], all_ref.at[sc_ref[0] * B + b, pl.ds(r0, R)], sem_out.at[b]) for b in range(B)]

    @pl.when(i == 0)
    def _():
        for c in cps:
            c.start()
        for c in cps:
            c.wait()
        for c in outs:
            c.start()

    ks = pl.ds(pl.multiple_of(i * KD, KD), KD)

    def products(b):
        x = x_ref[b, :, ks]
        if mode == "qkv":
            n = w_ref.shape[2] // 2
            half = pl.ds(pl.multiple_of(core * n, n), n)
            return [dotf(x, w_ref[0], NN), dotf(x, w_ref[1, :, half], NN), dotf(x, w_ref[2, :, half], NN)]
        return [dotf(x, ws[0][...], NT)]

    if mode == "qkv":
        for j in range(3):
            w_ref[j] = ws[j][...].reshape(w_ref.shape[1:])

    @pl.when(i == 0)
    def _():
        for b in range(B):
            o = 0
            for d in products(b):
                acc_ref[b, :, o:o + d.shape[1]] = d
                o += d.shape[1]

    @pl.when(i > 0)
    def _():
        for b in range(B):
            o = 0
            for d in products(b):
                acc_ref[b, :, o:o + d.shape[1]] += d
                o += d.shape[1]

    @pl.when(i == last)
    def _():
        N = acc_ref.shape[2]
        for b in range(B):
            if mode == "qkv":
                n_rope = N * 3 // 4
                c, s = cos_ref[b], sin_ref[b]
                for h in range(n_rope // HEAD):
                    r = acc_ref[b, :, h * HEAD:(h + 1) * HEAD]
                    out_ref[b, :, h * HEAD:(h + 1) * HEAD] = (r * c + pltpu.roll(r, HEAD // 2, 1) * s).astype(BF16)
                out_ref[b, :, n_rope:] = acc_ref[b, :, n_rope:].astype(BF16)
            else:
                out_ref[b] = acc_ref[b].astype(BF16)
        for c in outs:
            c.wait()


def gather_matmul(chip, core, places, pieces, ws, mode, tabs, B, R, r0, N, bufs=None):
    D = pieces[0].shape[1]
    tokens = 512
    nk = D // KD
    scal = jnp.stack([jnp.asarray(v, jnp.int32) for v in [chip, core] + [v for p in places for v in p]])
    layout = tuple((2 + 2 * i, p.shape[0]) for i, p in enumerate(pieces))
    anyspec = pl.BlockSpec(memory_space=pl.ANY)
    if mode == "qkv":
        hb = ws[1].shape[1]
        w_specs = [pl.BlockSpec((KD, hb, HEAD), lambda i, s: (i, s[1], 0))] + [pl.BlockSpec((KD, hb, HEAD), lambda i, s: (i, 0, 0))] * 2
        w_specs += [pl.BlockSpec((B, R, HEAD), lambda i, s: (s[0], 0, 0), pipeline_mode=pl.Buffered(1))] * 2
        wscr = pltpu.VMEM((3, KD, hb * HEAD), BF16)
    else:
        w_specs = [pl.BlockSpec((N, KD), lambda i, s: (s[1], i))]
        wscr = pltpu.VMEM((1, 16, HEAD), BF16)
    in_specs = [anyspec] * len(pieces) + w_specs
    args = list(pieces) + list(ws) + [t.reshape(4, tokens, HEAD) for t in tabs]
    aliases = {}
    if bufs is not None:
        aliases = {1 + len(args): 0, 2 + len(args): 1}
        in_specs += [anyspec, anyspec]
        args += list(bufs)
    return pl.pallas_call(
        functools.partial(gmm_kernel, layout=layout, mode=mode, n_w=len(ws), R=R, r0=r0, aliased=bufs is not None),
        grid_spec=pltpu.PrefetchScalarGridSpec(
            num_scalar_prefetch=1,
            grid=(nk,),
            in_specs=in_specs,
            out_specs=[pl.BlockSpec((B, R, N), lambda i, s: (s[0], r0 // R, 0), pipeline_mode=pl.Buffered(1)), anyspec],
            scratch_shapes=[
                pltpu.VMEM((B, R, D), BF16),
                pltpu.VMEM((B, R, N), F32),
                wscr,
                pltpu.SemaphoreType.DMA((len(pieces),)),
                pltpu.SemaphoreType.DMA((B,)),
            ],
        ),
        out_shape=[jax.ShapeDtypeStruct((4, tokens, N), BF16), jax.ShapeDtypeStruct((4, tokens, D), BF16)],
        input_output_aliases=aliases,
        compiler_params=pltpu.CompilerParams(dimension_semantics=("arbitrary",), vmem_limit_bytes=VMEM_LIMIT),
        cost_estimate=pl.CostEstimate(flops=2 * B * R * D * N, bytes_accessed=B * R * D * 4 + N * D * 2, transcendentals=0),
    )(scal, *args)


def orow_kernel(sc_ref, c0_ref, c1_ref, w_ref, out_ref):
    core = sc_ref[1]
    n = c0_ref.shape[1]
    own = w_ref[pl.ds(pl.multiple_of(core * n, n), n), :]
    oth = w_ref[pl.ds(pl.multiple_of((1 - core) * n, n), n), :]
    out_ref[...] = (dotf(c0_ref[...], own, NN) + dotf(c1_ref[...], oth, NN)).astype(BF16)


def o_rows(scal, ctx, ctx_pr, w, c, nc, M, db):
    n, D = ctx.shape[1], w.shape[1]
    return pl.pallas_call(
        orow_kernel,
        grid_spec=pltpu.PrefetchScalarGridSpec(
            num_scalar_prefetch=1,
            grid=(D // db,),
            in_specs=[
                pl.BlockSpec((M, n), lambda i, s: (s[2] * nc + c, 0)),
                pl.BlockSpec((M, n), lambda i, s: (c, 0)),
                pl.BlockSpec((2 * n, db), lambda i, s: (0, i)),
            ],
            out_specs=pl.BlockSpec((M, db), lambda i, s: (0, i)),
        ),
        out_shape=jax.ShapeDtypeStruct((M, D), BF16),
        compiler_params=pltpu.CompilerParams(dimension_semantics=("arbitrary",), vmem_limit_bytes=VMEM_LIMIT),
        cost_estimate=pl.CostEstimate(flops=4 * M * D * n, bytes_accessed=w.size * 2, transcendentals=0),
    )(scal, ctx, ctx_pr, w)


def ga_kernel(sc_ref, q0, k0, v0, q1, k1, v1, wq_ref, wk_ref, wv_ref, out_ref, wq_s, wk_s, wv_s):
    core = sc_ref[1]
    acc = None
    for w_ref, s_ref, own, oth in ((wq_ref, wq_s, q0, q1), (wk_ref, wk_s, k0, k1), (wv_ref, wv_s, v0, v1)):
        s_ref[...] = w_ref[...].reshape(s_ref.shape)
        n = own.shape[1]
        for c, g in ((core, own), (1 - core, oth)):
            d = dotf(g[...], s_ref[:, pl.ds(pl.multiple_of(c * n, n), n)], NT)
            acc = d if acc is None else acc + d
    out_ref[...] = acc.astype(BF16)


def ga_rows(scal, own, oth, ws, M, db):
    D = ws[0].shape[0]
    return pl.pallas_call(
        ga_kernel,
        grid_spec=pltpu.PrefetchScalarGridSpec(
            num_scalar_prefetch=1,
            grid=(D // db,),
            in_specs=[pl.BlockSpec((M, g.shape[1]), lambda i, s: (s[2], 0)) for g in own]
            + [pl.BlockSpec((M, g.shape[1]), lambda i, s: (0, 0)) for g in oth]
            + [pl.BlockSpec((db,) + w.shape[1:], lambda i, s: (i, 0, 0)) for w in ws],
            out_specs=pl.BlockSpec((M, db), lambda i, s: (0, i)),
            scratch_shapes=[pltpu.VMEM((db, w.shape[1] * HEAD), BF16) for w in ws],
        ),
        out_shape=jax.ShapeDtypeStruct((M, D), BF16),
        compiler_params=pltpu.CompilerParams(dimension_semantics=("arbitrary",), vmem_limit_bytes=VMEM_LIMIT),
        cost_estimate=pl.CostEstimate(flops=2 * M * sum(w.size for w in ws), bytes_accessed=sum(w.size for w in ws) * 2, transcendentals=0),
    )(scal, *own, *oth, *ws)


def dw_kernel(sc_ref, a_ref, q0, q1, k0, k1, v0, v1, oq_ref, ok_ref, ov_ref):
    db = a_ref.shape[1]
    core = sc_ref[1]
    at = a_ref[...].T
    for pair, out_ref in (((q0, q1), oq_ref), ((k0, k1), ok_ref), ((v0, v1), ov_ref)):
        hh = pair[0].shape[1] // HEAD
        nh = 2 * hh
        for other, g_ref in enumerate(pair):
            c = 1 - core if other else core
            res = dotf(at, g_ref[...], NN)
            for h in range(hh):
                out_ref[pl.ds(c * hh + h, db, stride=nh), :] = res[:, h * HEAD:(h + 1) * HEAD]


def dw_proj(scal, a, gs, db):
    T, D = a.shape
    nhs = [2 * gs[0].shape[1] // HEAD, 2 * gs[2].shape[1] // HEAD, 2 * gs[4].shape[1] // HEAD]
    outs = pl.pallas_call(
        dw_kernel,
        grid_spec=pltpu.PrefetchScalarGridSpec(
            num_scalar_prefetch=1,
            grid=(D // db,),
            in_specs=[pl.BlockSpec((T, db), lambda i, s: (0, i))]
            + [pl.BlockSpec(g.shape, lambda i, s: (0, 0), pipeline_mode=pl.Buffered(1)) for g in gs],
            out_specs=[pl.BlockSpec((db * nh, HEAD), lambda i, s: (i, 0)) for nh in nhs],
        ),
        out_shape=[jax.ShapeDtypeStruct((D * nh, HEAD), F32) for nh in nhs],
        compiler_params=pltpu.CompilerParams(dimension_semantics=("arbitrary",), vmem_limit_bytes=VMEM_LIMIT),
        cost_estimate=pl.CostEstimate(flops=2 * T * D * sum(nhs) * HEAD, bytes_accessed=D * sum(nhs) * HEAD * 4, transcendentals=0),
        name="dw_proj",
    )(scal, a, *gs)
    return [o.reshape(D, nh, HEAD) for o, nh in zip(outs, nhs)]


def dwo_kernel(sc_ref, c0_ref, c1_ref, g_ref, out_ref, t_ref):
    core = sc_ref[1]
    n = c0_ref.shape[1]

    @pl.when(pl.program_id(0) == 0)
    def _():
        t_ref[pl.ds(pl.multiple_of(core * n, n), n), :] = c0_ref[...].T
        t_ref[pl.ds(pl.multiple_of((1 - core) * n, n), n), :] = c1_ref[...].T

    out_ref[...] = dotf(t_ref[...], g_ref[...], NN)


def dwo_proj(scal, c0, c1, go, db):
    T, D = go.shape
    n = c0.shape[1]
    return pl.pallas_call(
        dwo_kernel,
        grid_spec=pltpu.PrefetchScalarGridSpec(
            num_scalar_prefetch=1,
            grid=(D // db,),
            in_specs=[pl.BlockSpec((T, n), lambda i, s: (0, 0), pipeline_mode=pl.Buffered(1))] * 2
            + [pl.BlockSpec((T, db), lambda i, s: (0, i))],
            out_specs=pl.BlockSpec((2 * n, db), lambda i, s: (0, i)),
            scratch_shapes=[pltpu.VMEM((2 * n, T), BF16)],
        ),
        out_shape=jax.ShapeDtypeStruct((2 * n, D), F32),
        compiler_params=pltpu.CompilerParams(dimension_semantics=("arbitrary",), vmem_limit_bytes=VMEM_LIMIT),
        cost_estimate=pl.CostEstimate(flops=4 * T * D * n, bytes_accessed=2 * n * D * 4, transcendentals=0),
        name="dwo_proj",
    )(scal, c0, c1, go)


RB = 64


def post_kernel(p_ref, r_ref, h_ref, dy_ref, g_ref, *rest):
    y_ref, go_ref, dg_ref = rest[-3:]
    o = p_ref[...].astype(F32) + r_ref[...].astype(F32)
    inv = lax.rsqrt(jnp.mean(o * o, axis=-1, keepdims=True) + NORM_EPS)
    hat = o * inv
    g = g_ref[...]
    dy = dy_ref[...].astype(F32)
    y_ref[...] = (h_ref[...].astype(F32) + hat * g).astype(BF16)
    gg = dy * g
    go_ref[...] = (inv * (gg - hat * jnp.mean(gg * hat, axis=-1, keepdims=True))).astype(BF16)

    @pl.when(pl.program_id(0) == 0)
    def _():
        dg_ref[...] = jnp.zeros_like(dg_ref)

    dg_ref[...] += jnp.sum((dy * hat).reshape(RB // 8, 8, -1), axis=0)


def pre_kernel(p_ref, r_ref, h_ref, dy_ref, g_ref, *rest):
    dh_ref, dg_ref = rest[-2:]
    ga = p_ref[...].astype(F32) + r_ref[...].astype(F32)
    h = h_ref[...].astype(F32)
    inv = lax.rsqrt(jnp.mean(h * h, axis=-1, keepdims=True) + NORM_EPS)
    hat = h * inv
    gh = ga * g_ref[...]
    dh_ref[...] = (dy_ref[...].astype(F32) + inv * (gh - hat * jnp.mean(gh * hat, axis=-1, keepdims=True))).astype(BF16)

    @pl.when(pl.program_id(0) == 0)
    def _():
        dg_ref[...] = jnp.zeros_like(dg_ref)

    dg_ref[...] += jnp.sum((ga * hat).reshape(RB // 8, 8, -1), axis=0)


def norm_call(kernel, part, peer, hidden, d_out, g, c, buf, extra):
    M, D = part.shape
    n = M // RB
    loc = pl.BlockSpec((RB, D), lambda i: (i, 0))
    row = pl.BlockSpec((RB, D), lambda i: (c * n + i, 0))
    in_specs = [loc, loc, row, row, pl.BlockSpec((1, D), lambda i: (0, 0))]
    args = [part, peer, hidden, d_out, g.reshape(1, D)]
    aliases = {}
    if buf is not None:
        aliases = {len(args): 0}
        args.append(buf)
        in_specs.append(pl.BlockSpec(memory_space=pl.ANY))
    out_specs = [row] + ([loc] if extra else []) + [pl.BlockSpec((8, D), lambda i: (0, 0))]
    out_shape = [jax.ShapeDtypeStruct(hidden.shape, BF16)]
    if extra:
        out_shape.append(jax.ShapeDtypeStruct((M, D), BF16))
    out_shape.append(jax.ShapeDtypeStruct((8, D), F32))
    return pl.pallas_call(
        kernel, grid=(n,), in_specs=in_specs, out_specs=out_specs, out_shape=out_shape, input_output_aliases=aliases,
        compiler_params=pltpu.CompilerParams(dimension_semantics=("arbitrary",), vmem_limit_bytes=VMEM_LIMIT),
        cost_estimate=pl.CostEstimate(flops=M * D * 2000, bytes_accessed=M * D * 12, transcendentals=0),
    )(*args)


def a_kernel(h_ref, g_ref, a_ref):
    h = h_ref[...].astype(F32)
    inv = lax.rsqrt(jnp.mean(h * h, axis=-1, keepdims=True) + NORM_EPS)
    a_ref[...] = (h * inv * g_ref[...]).astype(BF16)


def a_call(hidden, g):
    M, D = hidden.shape
    row = pl.BlockSpec((RB, D), lambda i: (i, 0))
    return pl.pallas_call(
        a_kernel, grid=(M // RB,), in_specs=[row, pl.BlockSpec((1, D), lambda i: (0, 0))], out_specs=row,
        out_shape=jax.ShapeDtypeStruct((M, D), BF16),
        compiler_params=pltpu.CompilerParams(dimension_semantics=("arbitrary",)),
        cost_estimate=pl.CostEstimate(flops=M * D * 1000, bytes_accessed=M * D * 4, transcendentals=0),
        name="a_norm",
    )(hidden, g.reshape(1, D))


def solution(mesh):
    core_perm = [(0, 1), (1, 0), (2, 3), (3, 2)]
    x_perm = [(0, 2), (2, 0), (1, 3), (3, 1)]
    tp_perm = [(0, 1), (1, 0)]

    def to_core(v):
        return lax.ppermute(v, 'cp', core_perm)

    def to_x(v):
        return lax.ppermute(v, 'cp', x_perm)

    def to_tp(v):
        return lax.ppermute(v, 'tp', tp_perm)

    def device_fn(hidden, g_pre, w_q, w_k, w_v, w_o, g_post, d_out):
        tokens, D = hidden.shape
        T = 4 * tokens
        me = lax.axis_index('cp')
        tp = lax.axis_index('tp')
        core, xi = me % 2, me // 2
        HL = w_q.shape[1] // 2
        KL = w_k.shape[1] // 2
        cos, sin = lax.optimization_barrier(rope_tables(T))
        base = jnp.stack([xi, core, me, me ^ 1]).astype(jnp.int32)

        def two_way(blk, n):
            r1 = to_x(lax.dynamic_slice_in_dim(blk, tp * n, n, 0))
            r3 = to_x(blk[2 * n:])
            r2 = to_tp(r1)
            return [r1, r2, r3], [tp * n, (1 - tp) * n, 2 * n]

        a_loc = a_call(hidden, g_pre)
        a_x, a_off = two_way(a_loc, 176)
        a_p = to_core(a_loc)
        a_xp = [to_core(r) for r in a_x]
        wo2 = w_o.reshape(-1, D)
        N = (HL + 2 * KL) * HEAD
        qkv_args = ((w_q, w_k, w_v), "qkv", (cos, sin), 2, tokens, 0, N)
        bufs = gather_matmul(xi, core, [(core, 0), (1 - core, 0)], [a_loc, a_p], *qkv_args)
        places = [(core, o) for o in a_off] + [(1 - core, o) for o in a_off]
        qkv, a_all = gather_matmul(1 - xi, core, places, a_x + a_xp, *qkv_args, bufs=bufs)
        qkv = qkv.reshape(T, N)
        a_all = a_all.reshape(T, D)

        ctx, lse = attn_fwd(qkv, KL, HL)
        ctx_pr = to_core(lax.dynamic_slice_in_dim(ctx, (me ^ 1) * tokens, tokens, 0))
        nc = 4
        M = tokens // nc
        o_parts, o_peers = [], []
        for c in range(nc):
            op = o_rows(base, ctx, ctx_pr, wo2, c, nc, M, 1536)
            o_parts.append(op)
            o_peers.append(to_tp(op))
        ctx_p = to_core(ctx)

        y_blk, gos, dgp = None, [], []
        for c in range(nc):
            y_blk, go, dg_ = norm_call(post_kernel, o_parts[c], o_peers[c], hidden, d_out, g_post, c, y_blk, True)
            gos.append(go)
            dgp.append(dg_)

        gx = [to_x(g) for g in gos[:-1]]
        gp = [to_core(g) for g in gos]
        r, r_off = two_way(gos[-1], 48)
        gxp = [to_core(g) for g in gx]
        rp = [to_core(g) for g in r]
        HN = HL * HEAD
        early = [c * M for c in range(nc - 1)]
        RE = (nc - 1) * M
        places = [(core, o) for o in early] + [(1 - core, o) for o in early]
        bufs = gather_matmul(xi, core, places, gos[:-1] + gp[:-1], (wo2,), "nt", (), 2, RE, 0, HN)
        bufs = gather_matmul(1 - xi, core, places, gx + gxp, (wo2,), "nt", (), 2, RE, 0, HN, bufs=bufs)
        places = [(me, 0), (me ^ 1, 0)] + [(me ^ 2, o) for o in r_off] + [(me ^ 3, o) for o in r_off]
        dctx, go_all = gather_matmul(0, core, places, [gos[-1], gp[-1]] + r + rp, (wo2,), "nt", (), 4, M, RE, HN, bufs=bufs)
        dctx = dctx.reshape(T, HN)
        go_all = go_all.reshape(T, D)

        dqkv = attn_bwd(qkv, KL, HL, dctx, ctx, lse, cos, sin)
        dqkv_pr = [to_core(lax.dynamic_slice_in_dim(g, (me ^ 1) * tokens, tokens, 0)) for g in dqkv]
        dqkv_p = [to_core(g) for g in dqkv]
        ga_part = ga_rows(base, dqkv, dqkv_pr, (w_q, w_k, w_v), tokens, 512)
        ga_peer = to_tp(ga_part)

        dwo = dwo_proj(base, ctx, ctx_p, go_all, 512).reshape(w_o.shape)
        dwq, dwk, dwv = dw_proj(base, a_all, [g for pair in zip(dqkv, dqkv_p) for g in pair], 256)

        grad_h, dgr = norm_call(pre_kernel, ga_part, ga_peer, hidden, d_out, g_pre, 0, None, False)
        dg = jnp.stack([jnp.sum(dgr, axis=0), jnp.sum(sum(dgp), axis=0)])
        dg = dg + to_core(dg)
        dg = dg + to_x(dg)
        return y_blk, grad_h, dg[0], dwq, dwk, dwv, dwo, dg[1]


    row_spec = P('cp', None)
    head_spec = P(None, 'tp', None)
    out_head_spec = P('tp', None, None)
    return jax.shard_map(device_fn, mesh=mesh, in_specs=(row_spec, P(), head_spec, head_spec, head_spec, out_head_spec, P(), row_spec), out_specs=(row_spec, row_spec, P(), head_spec, head_spec, head_spec, out_head_spec, P()), check_vma=False)
```

```python
import functools

import jax
import jax.numpy as jnp
from jax import lax
from jax.experimental import pallas as pl
from jax.experimental.pallas import tpu as pltpu
from jax.sharding import PartitionSpec as P


SOFT_CAP = 30.0
NORM_EPS = 1e-5
ROPE_THETA = 10000.0
HEAD = 128
LOG2E = 1.4426950408889634
F32 = jnp.float32
BF16 = jnp.bfloat16

NT = (((1,), (1,)), ((), ()))
NN = (((1,), (0,)), ((), ()))


def dotf(a, b, dims):
    return lax.dot_general(a, b, dims, preferred_element_type=F32)


def rope_tables(length):
    half = HEAD // 2
    inv_freq = ROPE_THETA ** (-jnp.arange(half, dtype=F32) * 2.0 / HEAD)
    ang = jnp.arange(length).astype(F32)[:, None] * inv_freq[None, :]
    cos, sin = jnp.cos(ang), jnp.sin(ang)
    return jnp.concatenate([cos, cos], axis=-1), jnp.concatenate([-sin, sin], axis=-1)


QT = 512
SB = 256


def attn_fwd_kernel(q_ref, k_ref, v_ref, ctx_ref, lse_ref, q_s, acc_ref, sum_ref, *, k1, k2):
    i = pl.program_id(1)
    nt = QT // SB
    for t in range(nt):
        rows = slice(t * SB, (t + 1) * SB)
        q_s[t, :SB] = q_ref[rows, :HEAD]
        q_s[t, SB:] = q_ref[rows, HEAD:]
    acc_ref[...] = jnp.zeros_like(acc_ref)
    sum_ref[...] = jnp.zeros_like(sum_ref)

    def chunk(t, row0, mask):
        k = k_ref[pl.ds(row0, SB), :]
        v = v_ref[pl.ds(row0, SB), :]
        s = dotf(q_s[t], k, NT)
        p = jnp.exp2(jnp.tanh(s * k1) * k2)
        if mask is not None:
            p = jnp.where(mask, p, 0.0)
        part = p[:, :128]
        for c in range(1, SB // 128):
            part = part + p[:, c * 128:(c + 1) * 128]
        return part, dotf(p.astype(BF16), v, NN)

    def full(j, carry):
        for t in range(nt):
            ps = [chunk(t, pl.multiple_of(j * QT + m * SB, SB), None) for m in range(nt)]
            sum_ref[t] += ps[0][0] + ps[1][0]
            acc_ref[t] += ps[0][1] + ps[1][1]
        return carry

    lax.fori_loop(0, i, full, 0)

    rows = lax.broadcasted_iota(jnp.int32, (2 * SB, SB), 0) % SB
    cols = lax.broadcasted_iota(jnp.int32, (2 * SB, SB), 1)
    mask = rows >= cols
    for t in range(nt):
        ps = [chunk(t, pl.multiple_of(i * QT + m * SB, SB), mask if m == t else None) for m in range(t + 1)]
        tot, acc = sum_ref[t], acc_ref[t]
        for p in ps:
            tot, acc = tot + p[0], acc + p[1]
        total = jnp.sum(tot, axis=1, keepdims=True)
        ctx = (acc / total).astype(BF16)
        r = slice(t * SB, (t + 1) * SB)
        ctx_ref[r, :HEAD] = ctx[:SB]
        ctx_ref[r, HEAD:] = ctx[SB:]
        lse = jnp.broadcast_to(jnp.log2(total), (2 * SB, 128)).T
        lse_ref[0, 0:1, r] = lse[0:1, :SB]
        lse_ref[0, 1:2, r] = lse[0:1, SB:]


def attn_fwd(qkv, kvh, nq):
    T = qkv.shape[0]
    scale = HEAD ** -0.5
    return pl.pallas_call(
        functools.partial(attn_fwd_kernel, k1=scale / SOFT_CAP, k2=SOFT_CAP * LOG2E),
        grid=(kvh, T // QT),
        in_specs=[
            pl.BlockSpec((QT, 2 * HEAD), lambda h, i: (i, h)),
            pl.BlockSpec((T, HEAD), lambda h, i: (0, nq + h)),
            pl.BlockSpec((T, HEAD), lambda h, i: (0, nq + kvh + h)),
        ],
        out_specs=[
            pl.BlockSpec((QT, 2 * HEAD), lambda h, i: (i, h)),
            pl.BlockSpec((1, 2, QT), lambda h, i: (h, 0, i)),
        ],
        out_shape=[
            jax.ShapeDtypeStruct((T, nq * HEAD), BF16),
            jax.ShapeDtypeStruct((kvh, 2, T), F32),
        ],
        scratch_shapes=[
            pltpu.VMEM((QT // SB, 2 * SB, HEAD), BF16),
            pltpu.VMEM((QT // SB, 2 * SB, HEAD), F32),
            pltpu.VMEM((QT // SB, 2 * SB, 128), F32),
        ],
        compiler_params=pltpu.CompilerParams(dimension_semantics=("arbitrary", "arbitrary")),
        cost_estimate=pl.CostEstimate(flops=int(2 * 2 * T * T * HEAD * kvh * 2), bytes_accessed=2 * qkv.size * 2, transcendentals=0),
        name="attn_fwd",
    )(qkv, qkv, qkv)


BQ = 256
BK = 512


def attn_bwd_kernel(q_ref, k_ref, v_ref, do_ref, ctx_ref, lse_ref, cos_ref, sin_ref, dq_ref, dk_ref, dv_ref,
                    dqa_ref, dka_ref, dva_ref, dd_ref, kt_ref, *, k1, k2, scale):
    J = pl.program_id(1)
    nq = q_ref.shape[0] // BQ
    r = BK // BQ

    @pl.when(J == 0)
    def _():
        dqa_ref[...] = jnp.zeros_like(dqa_ref)
        for g in range(2):
            for i in range(nq):
                sl = slice(i * BQ, (i + 1) * BQ)
                prod = do_ref[sl, g * HEAD:(g + 1) * HEAD].astype(F32) * ctx_ref[sl, g * HEAD:(g + 1) * HEAD].astype(F32)
                dd_ref[g, 0:1, sl] = jnp.sum(prod.T, axis=0, keepdims=True)

    dka_ref[...] = jnp.zeros_like(dka_ref)
    dva_ref[...] = jnp.zeros_like(dva_ref)
    k = k_ref[...]
    v = v_ref[...]
    kt_ref[...] = k.T

    def tile(i, mask):
        row0 = pl.multiple_of(i * BQ, BQ)
        rs = pl.ds(row0, BQ)
        dks, dvs = [], []
        for g in range(2):
            q = q_ref[rs, g * HEAD:(g + 1) * HEAD]
            do = do_ref[rs, g * HEAD:(g + 1) * HEAD]
            lse = lse_ref[0, g:g + 1, rs]
            dd = dd_ref[g, 0:1, rs]
            s = dotf(k, q, NT)
            u = jnp.tanh(s * k1)
            p = jnp.exp2(u * k2 - lse)
            if mask is not None:
                p = jnp.where(mask, p, 0.0)
            dp = dotf(v, do, NT)
            ds = (p * (dp - dd) * (1.0 - u * u)).astype(BF16)
            dvs.append(dotf(p.astype(BF16), do, NN))
            dks.append(dotf(ds, q, NN))
            dqa_ref[g, :, rs] += dotf(kt_ref[...], ds, NN)
        dva_ref[...] += dvs[0] + dvs[1]
        dka_ref[...] += dks[0] + dks[1]

    kpos = lax.broadcasted_iota(jnp.int32, (BK, BQ), 0)
    qpos = lax.broadcasted_iota(jnp.int32, (BK, BQ), 1)
    for m in range(r):
        tile(J * r + m, qpos + m * BQ >= kpos)

    def body(j, carry):
        for m in range(r):
            tile(j * r + m, None)
        return carry

    lax.fori_loop(J + 1, nq // r, body, 0)

    krow = pl.ds(pl.multiple_of(J * BK, BK), BK)

    def unrope(g, cos, sin):
        return (g * cos - pltpu.roll(g, HEAD // 2, 1) * sin) * scale

    dk_ref[...] = unrope(dka_ref[...], cos_ref[krow, :], sin_ref[krow, :]).astype(BF16)
    dv_ref[...] = dva_ref[...].astype(BF16)
    for g in range(2):
        dq_ref[:, g * HEAD:(g + 1) * HEAD] = unrope(dqa_ref[g, :, krow].T, cos_ref[krow, :], sin_ref[krow, :]).astype(BF16)


def attn_bwd(qkv, kvh, nq, do, ctx, lse, cos, sin):
    T = qkv.shape[0]
    scale = HEAD ** -0.5
    full2 = pl.BlockSpec((T, 2 * HEAD), lambda h, j: (0, h))
    kblk = pl.BlockSpec((BK, HEAD), lambda h, j: (j, h))
    tab = pl.BlockSpec((T, HEAD), lambda h, j: (0, 0))
    return pl.pallas_call(
        functools.partial(attn_bwd_kernel, k1=scale / SOFT_CAP, k2=SOFT_CAP * LOG2E, scale=scale),
        grid=(kvh, T // BK),
        in_specs=[full2, pl.BlockSpec((BK, HEAD), lambda h, j: (j, nq + h)), pl.BlockSpec((BK, HEAD), lambda h, j: (j, nq + kvh + h)), full2, full2, pl.BlockSpec((1, 2, T), lambda h, j: (h, 0, 0)), tab, tab],
        out_specs=[pl.BlockSpec((BK, 2 * HEAD), lambda h, j: (j, h)), kblk, kblk],
        out_shape=[
            jax.ShapeDtypeStruct((T, nq * HEAD), BF16),
            jax.ShapeDtypeStruct((T, kvh * HEAD), BF16),
            jax.ShapeDtypeStruct((T, kvh * HEAD), BF16),
        ],
        scratch_shapes=[
            pltpu.VMEM((2, HEAD, T), F32),
            pltpu.VMEM((BK, HEAD), F32),
            pltpu.VMEM((BK, HEAD), F32),
            pltpu.VMEM((2, 1, T), F32),
            pltpu.VMEM((HEAD, BK), BF16),
        ],
        compiler_params=pltpu.CompilerParams(dimension_semantics=("arbitrary", "arbitrary")),
        cost_estimate=pl.CostEstimate(flops=int(5 * 2 * T * T * HEAD * kvh), bytes_accessed=3 * qkv.size * 2, transcendentals=0),
        name="attn_bwd",
    )(qkv, qkv, qkv, do, ctx, lse, cos, sin)


VMEM_LIMIT = 64_000_000
KD = 512


def gmm_kernel(sc_ref, *refs, layout, mode, n_w, R, r0, aliased):
    np_ = len(layout)
    pieces = refs[:np_]
    ws = refs[np_:np_ + n_w]
    rest = refs[np_ + n_w:]
    if mode == "qkv":
        cos_ref, sin_ref = rest[:2]
        rest = rest[2:]
    if aliased:
        rest = rest[2:]
    out_ref, all_ref, x_ref, acc_ref, w_ref, sem_in, sem_out = rest
    i = pl.program_id(0)
    last = pl.num_programs(0) - 1
    B = x_ref.shape[0]
    core = sc_ref[1]

    def cols(k):
        return pl.ds(pl.multiple_of(k * KD, KD), KD)

    def cp_in(p, k):
        slot, n = layout[p]
        off = pl.multiple_of(sc_ref[slot + 1], 16)
        return pltpu.make_async_copy(pieces[p].at[:, cols(k)], x_ref.at[sc_ref[slot], pl.ds(off, n), cols(k)], sem_in.at[k])

    def cp_out(b, k):
        return pltpu.make_async_copy(x_ref.at[b, :, cols(k)], all_ref.at[sc_ref[0] * B + b, pl.ds(r0, R), cols(k)], sem_out)

    @pl.when(i == 0)
    def _():
        @pl.loop(0, last + 1)
        def _(k):
            for p in range(np_):
                cp_in(p, k).start()

    for p in range(np_):
        cp_in(p, i).wait()
    for b in range(B):
        cp_out(b, i).start()

    ks = pl.ds(pl.multiple_of(i * KD, KD), KD)

    def products(b):
        x = x_ref[b, :, ks]
        if mode == "qkv":
            n = w_ref.shape[2] // 2
            half = pl.ds(pl.multiple_of(core * n, n), n)
            return [dotf(x, w_ref[0], NN), dotf(x, w_ref[1, :, half], NN), dotf(x, w_ref[2, :, half], NN)]
        return [dotf(x, ws[0][...], NT)]

    def prep():
        if mode == "qkv":
            for j in range(3):
                w_ref[j] = ws[j][...].reshape(w_ref.shape[1:])

    @pl.when(i == 0)
    def _():
        prep()
        for b in range(B):
            o = 0
            for d in products(b):
                acc_ref[b, :, o:o + d.shape[1]] = d
                o += d.shape[1]

    @pl.when(i > 0)
    def _():
        prep()
        for b in range(B):
            o = 0
            for d in products(b):
                acc_ref[b, :, o:o + d.shape[1]] += d
                o += d.shape[1]

    @pl.when(i == last)
    def _():
        N = acc_ref.shape[2]
        for b in range(B):
            if mode == "qkv":
                n_rope = N * 3 // 4
                c, s = cos_ref[b], sin_ref[b]
                for h in range(n_rope // HEAD):
                    r = acc_ref[b, :, h * HEAD:(h + 1) * HEAD]
                    out_ref[b, :, h * HEAD:(h + 1) * HEAD] = (r * c + pltpu.roll(r, HEAD // 2, 1) * s).astype(BF16)
                out_ref[b, :, n_rope:] = acc_ref[b, :, n_rope:].astype(BF16)
            else:
                out_ref[b] = acc_ref[b].astype(BF16)

        @pl.loop(0, last + 1)
        def _(k):
            for b in range(B):
                cp_out(b, k).wait()


def gather_matmul(chip, core, places, pieces, ws, mode, tabs, B, R, r0, N, bufs=None):
    D = pieces[0].shape[1]
    tokens = 512
    nk = D // KD
    scal = jnp.stack([jnp.asarray(v, jnp.int32) for v in [chip, core] + [v for p in places for v in p]])
    layout = tuple((2 + 2 * i, p.shape[0]) for i, p in enumerate(pieces))
    anyspec = pl.BlockSpec(memory_space=pl.ANY)
    if mode == "qkv":
        hb = ws[1].shape[1]
        w_specs = [pl.BlockSpec((KD, hb, HEAD), lambda i, s: (i, s[1], 0))] + [pl.BlockSpec((KD, hb, HEAD), lambda i, s: (i, 0, 0))] * 2
        w_specs += [pl.BlockSpec((B, R, HEAD), lambda i, s: (s[0], 0, 0), pipeline_mode=pl.Buffered(1))] * 2
        wscr = pltpu.VMEM((3, KD, hb * HEAD), BF16)
    else:
        w_specs = [pl.BlockSpec((N, KD), lambda i, s: (s[1], i))]
        wscr = pltpu.VMEM((1, 16, HEAD), BF16)
    in_specs = [anyspec] * len(pieces) + w_specs
    args = list(pieces) + list(ws) + [t.reshape(4, tokens, HEAD) for t in tabs]
    aliases = {}
    if bufs is not None:
        aliases = {1 + len(args): 0, 2 + len(args): 1}
        in_specs += [anyspec, anyspec]
        args += list(bufs)
    return pl.pallas_call(
        functools.partial(gmm_kernel, layout=layout, mode=mode, n_w=len(ws), R=R, r0=r0, aliased=bufs is not None),
        grid_spec=pltpu.PrefetchScalarGridSpec(
            num_scalar_prefetch=1,
            grid=(nk,),
            in_specs=in_specs,
            out_specs=[pl.BlockSpec((B, R, N), lambda i, s: (s[0], r0 // R, 0), pipeline_mode=pl.Buffered(1)), anyspec],
            scratch_shapes=[
                pltpu.VMEM((B, R, D), BF16),
                pltpu.VMEM((B, R, N), F32),
                wscr,
                pltpu.SemaphoreType.DMA((nk,)),
                pltpu.SemaphoreType.DMA,
            ],
        ),
        out_shape=[jax.ShapeDtypeStruct((4, tokens, N), BF16), jax.ShapeDtypeStruct((4, tokens, D), BF16)],
        input_output_aliases=aliases,
        compiler_params=pltpu.CompilerParams(dimension_semantics=("arbitrary",), vmem_limit_bytes=VMEM_LIMIT),
        cost_estimate=pl.CostEstimate(flops=2 * B * R * D * N, bytes_accessed=B * R * D * 4 + N * D * 2, transcendentals=0),
    )(scal, *args)


def orow_kernel(sc_ref, c0_ref, c1_ref, w_ref, out_ref, *, r0):
    core = sc_ref[1]
    n = c0_ref.shape[1]
    rows = slice(r0, r0 + out_ref.shape[0])
    own = w_ref[pl.ds(pl.multiple_of(core * n, n), n), :]
    oth = w_ref[pl.ds(pl.multiple_of((1 - core) * n, n), n), :]
    out_ref[...] = (dotf(c0_ref[rows, :], own, NN) + dotf(c1_ref[rows, :], oth, NN)).astype(BF16)


def o_rows(scal, ctx, ctx_pr, w, r0, M, db):
    n, D = ctx.shape[1], w.shape[1]
    tokens = ctx_pr.shape[0]
    return pl.pallas_call(
        functools.partial(orow_kernel, r0=r0),
        grid_spec=pltpu.PrefetchScalarGridSpec(
            num_scalar_prefetch=1,
            grid=(D // db,),
            in_specs=[
                pl.BlockSpec((tokens, n), lambda i, s: (s[2], 0)),
                pl.BlockSpec((tokens, n), lambda i, s: (0, 0)),
                pl.BlockSpec((2 * n, db), lambda i, s: (0, i)),
            ],
            out_specs=pl.BlockSpec((M, db), lambda i, s: (0, i)),
        ),
        out_shape=jax.ShapeDtypeStruct((M, D), BF16),
        compiler_params=pltpu.CompilerParams(dimension_semantics=("arbitrary",), vmem_limit_bytes=VMEM_LIMIT),
        cost_estimate=pl.CostEstimate(flops=4 * M * D * n, bytes_accessed=w.size * 2, transcendentals=0),
    )(scal, ctx, ctx_pr, w)


def ga_kernel(sc_ref, q0, k0, v0, q1, k1, v1, wq_ref, wk_ref, wv_ref, out_ref, wq_s, wk_s, wv_s):
    core = sc_ref[1]
    acc = None
    for w_ref, s_ref, own, oth in ((wq_ref, wq_s, q0, q1), (wk_ref, wk_s, k0, k1), (wv_ref, wv_s, v0, v1)):
        s_ref[...] = w_ref[...].reshape(s_ref.shape)
        n = own.shape[1]
        for c, g in ((core, own), (1 - core, oth)):
            d = dotf(g[...], s_ref[:, pl.ds(pl.multiple_of(c * n, n), n)], NT)
            acc = d if acc is None else acc + d
    out_ref[...] = acc.astype(BF16)


def ga_rows(scal, own, oth, ws, M, db):
    D = ws[0].shape[0]
    return pl.pallas_call(
        ga_kernel,
        grid_spec=pltpu.PrefetchScalarGridSpec(
            num_scalar_prefetch=1,
            grid=(D // db,),
            in_specs=[pl.BlockSpec((M, g.shape[1]), lambda i, s: (s[2], 0)) for g in own]
            + [pl.BlockSpec((M, g.shape[1]), lambda i, s: (0, 0)) for g in oth]
            + [pl.BlockSpec((db,) + w.shape[1:], lambda i, s: (i, 0, 0)) for w in ws],
            out_specs=pl.BlockSpec((M, db), lambda i, s: (0, i)),
            scratch_shapes=[pltpu.VMEM((db, w.shape[1] * HEAD), BF16) for w in ws],
        ),
        out_shape=jax.ShapeDtypeStruct((M, D), BF16),
        compiler_params=pltpu.CompilerParams(dimension_semantics=("arbitrary",), vmem_limit_bytes=VMEM_LIMIT),
        cost_estimate=pl.CostEstimate(flops=2 * M * sum(w.size for w in ws), bytes_accessed=sum(w.size for w in ws) * 2, transcendentals=0),
    )(scal, *own, *oth, *ws)


def dw_kernel(sc_ref, a_ref, q0, q1, k0, k1, v0, v1, oq_ref, ok_ref, ov_ref):
    db = a_ref.shape[1]
    core = sc_ref[1]
    at = a_ref[...].T
    for pair, out_ref in (((q0, q1), oq_ref), ((k0, k1), ok_ref), ((v0, v1), ov_ref)):
        hh = pair[0].shape[1] // HEAD
        nh = 2 * hh
        for other, g_ref in enumerate(pair):
            c = 1 - core if other else core
            res = dotf(at, g_ref[...], NN)
            for h in range(hh):
                out_ref[pl.ds(c * hh + h, db, stride=nh), :] = res[:, h * HEAD:(h + 1) * HEAD]


def dw_proj(scal, a, gs, db):
    T, D = a.shape
    nhs = [2 * gs[0].shape[1] // HEAD, 2 * gs[2].shape[1] // HEAD, 2 * gs[4].shape[1] // HEAD]
    outs = pl.pallas_call(
        dw_kernel,
        grid_spec=pltpu.PrefetchScalarGridSpec(
            num_scalar_prefetch=1,
            grid=(D // db,),
            in_specs=[pl.BlockSpec((T, db), lambda i, s: (0, i))]
            + [pl.BlockSpec(g.shape, lambda i, s: (0, 0), pipeline_mode=pl.Buffered(1)) for g in gs],
            out_specs=[pl.BlockSpec((db * nh, HEAD), lambda i, s: (i, 0)) for nh in nhs],
        ),
        out_shape=[jax.ShapeDtypeStruct((D * nh, HEAD), F32) for nh in nhs],
        compiler_params=pltpu.CompilerParams(dimension_semantics=("arbitrary",), vmem_limit_bytes=VMEM_LIMIT),
        cost_estimate=pl.CostEstimate(flops=2 * T * D * sum(nhs) * HEAD, bytes_accessed=D * sum(nhs) * HEAD * 4, transcendentals=0),
        name="dw_proj",
    )(scal, a, *gs)
    return [o.reshape(D, nh, HEAD) for o, nh in zip(outs, nhs)]


def dwo_kernel(sc_ref, c0_ref, c1_ref, g_ref, out_ref, t_ref):
    core = sc_ref[1]
    n = c0_ref.shape[1]

    @pl.when(pl.program_id(0) == 0)
    def _():
        t_ref[pl.ds(pl.multiple_of(core * n, n), n), :] = c0_ref[...].T
        t_ref[pl.ds(pl.multiple_of((1 - core) * n, n), n), :] = c1_ref[...].T

    out_ref[...] = dotf(t_ref[...], g_ref[...], NN)


def dwo_proj(scal, c0, c1, go, db):
    T, D = go.shape
    n = c0.shape[1]
    return pl.pallas_call(
        dwo_kernel,
        grid_spec=pltpu.PrefetchScalarGridSpec(
            num_scalar_prefetch=1,
            grid=(D // db,),
            in_specs=[pl.BlockSpec((T, n), lambda i, s: (0, 0), pipeline_mode=pl.Buffered(1))] * 2
            + [pl.BlockSpec((T, db), lambda i, s: (0, i))],
            out_specs=pl.BlockSpec((2 * n, db), lambda i, s: (0, i)),
            scratch_shapes=[pltpu.VMEM((2 * n, T), BF16)],
        ),
        out_shape=jax.ShapeDtypeStruct((2 * n, D), F32),
        compiler_params=pltpu.CompilerParams(dimension_semantics=("arbitrary",), vmem_limit_bytes=VMEM_LIMIT),
        cost_estimate=pl.CostEstimate(flops=4 * T * D * n, bytes_accessed=2 * n * D * 4, transcendentals=0),
        name="dwo_proj",
    )(scal, c0, c1, go)


RB = 64


def post_kernel(p_ref, r_ref, h_ref, dy_ref, g_ref, *rest):
    y_ref, go_ref, dg_ref = rest[-3:]
    o = p_ref[...].astype(F32) + r_ref[...].astype(F32)
    inv = lax.rsqrt(jnp.mean(o * o, axis=-1, keepdims=True) + NORM_EPS)
    hat = o * inv
    g = g_ref[...]
    dy = dy_ref[...].astype(F32)
    y_ref[...] = (h_ref[...].astype(F32) + hat * g).astype(BF16)
    gg = dy * g
    go_ref[...] = (inv * (gg - hat * jnp.mean(gg * hat, axis=-1, keepdims=True))).astype(BF16)

    @pl.when(pl.program_id(0) == 0)
    def _():
        dg_ref[...] = jnp.zeros_like(dg_ref)

    dg_ref[...] += jnp.sum((dy * hat).reshape(RB // 8, 8, -1), axis=0)


def pre_kernel(p_ref, r_ref, h_ref, dy_ref, g_ref, *rest):
    dh_ref, dg_ref = rest[-2:]
    ga = p_ref[...].astype(F32) + r_ref[...].astype(F32)
    h = h_ref[...].astype(F32)
    inv = lax.rsqrt(jnp.mean(h * h, axis=-1, keepdims=True) + NORM_EPS)
    hat = h * inv
    gh = ga * g_ref[...]
    dh_ref[...] = (dy_ref[...].astype(F32) + inv * (gh - hat * jnp.mean(gh * hat, axis=-1, keepdims=True))).astype(BF16)

    @pl.when(pl.program_id(0) == 0)
    def _():
        dg_ref[...] = jnp.zeros_like(dg_ref)

    dg_ref[...] += jnp.sum((ga * hat).reshape(RB // 8, 8, -1), axis=0)


def norm_call(kernel, part, peer, hidden, d_out, g, r0, buf, extra):
    M, D = part.shape
    n = M // RB
    loc = pl.BlockSpec((RB, D), lambda i: (i, 0))
    row = pl.BlockSpec((RB, D), lambda i: (r0 // RB + i, 0))
    in_specs = [loc, loc, row, row, pl.BlockSpec((1, D), lambda i: (0, 0))]
    args = [part, peer, hidden, d_out, g.reshape(1, D)]
    aliases = {}
    if buf is not None:
        aliases = {len(args): 0}
        args.append(buf)
        in_specs.append(pl.BlockSpec(memory_space=pl.ANY))
    out_specs = [row] + ([loc] if extra else []) + [pl.BlockSpec((8, D), lambda i: (0, 0))]
    out_shape = [jax.ShapeDtypeStruct(hidden.shape, BF16)]
    if extra:
        out_shape.append(jax.ShapeDtypeStruct((M, D), BF16))
    out_shape.append(jax.ShapeDtypeStruct((8, D), F32))
    return pl.pallas_call(
        kernel, grid=(n,), in_specs=in_specs, out_specs=out_specs, out_shape=out_shape, input_output_aliases=aliases,
        compiler_params=pltpu.CompilerParams(dimension_semantics=("arbitrary",), vmem_limit_bytes=VMEM_LIMIT),
        cost_estimate=pl.CostEstimate(flops=M * D * 2000, bytes_accessed=M * D * 12, transcendentals=0),
    )(*args)


def a_kernel(h_ref, g_ref, a_ref):
    h = h_ref[...].astype(F32)
    inv = lax.rsqrt(jnp.mean(h * h, axis=-1, keepdims=True) + NORM_EPS)
    a_ref[...] = (h * inv * g_ref[...]).astype(BF16)


def a_call(hidden, g):
    M, D = hidden.shape
    row = pl.BlockSpec((RB, D), lambda i: (i, 0))
    return pl.pallas_call(
        a_kernel, grid=(M // RB,), in_specs=[row, pl.BlockSpec((1, D), lambda i: (0, 0))], out_specs=row,
        out_shape=jax.ShapeDtypeStruct((M, D), BF16),
        compiler_params=pltpu.CompilerParams(dimension_semantics=("arbitrary",)),
        cost_estimate=pl.CostEstimate(flops=M * D * 1000, bytes_accessed=M * D * 4, transcendentals=0),
        name="a_norm",
    )(hidden, g.reshape(1, D))


def solution(mesh):
    core_perm = [(0, 1), (1, 0), (2, 3), (3, 2)]
    x_perm = [(0, 2), (2, 0), (1, 3), (3, 1)]
    tp_perm = [(0, 1), (1, 0)]

    def to_core(v):
        return lax.ppermute(v, 'cp', core_perm)

    def to_x(v):
        return lax.ppermute(v, 'cp', x_perm)

    def to_tp(v):
        return lax.ppermute(v, 'tp', tp_perm)

    def device_fn(hidden, g_pre, w_q, w_k, w_v, w_o, g_post, d_out):
        tokens, D = hidden.shape
        T = 4 * tokens
        me = lax.axis_index('cp')
        tp = lax.axis_index('tp')
        core, xi = me % 2, me // 2
        HL = w_q.shape[1] // 2
        KL = w_k.shape[1] // 2
        cos, sin = lax.optimization_barrier(rope_tables(T))
        base = jnp.stack([xi, core, me, me ^ 1]).astype(jnp.int32)

        def two_way(blk, n):
            r1 = to_x(lax.dynamic_slice_in_dim(blk, tp * n, n, 0))
            r3 = to_x(blk[2 * n:])
            r2 = to_tp(r1)
            return [r1, r2, r3], [tp * n, (1 - tp) * n, 2 * n]

        a_loc = a_call(hidden, g_pre)
        a_x, a_off = two_way(a_loc, 176)
        a_p = to_core(a_loc)
        a_xp = [to_core(r) for r in a_x]
        wo2 = w_o.reshape(-1, D)
        N = (HL + 2 * KL) * HEAD
        qkv_args = ((w_q, w_k, w_v), "qkv", (cos, sin), 2, tokens, 0, N)
        bufs = gather_matmul(xi, core, [(core, 0), (1 - core, 0)], [a_loc, a_p], *qkv_args)
        places = [(core, o) for o in a_off] + [(1 - core, o) for o in a_off]
        qkv, a_all = gather_matmul(1 - xi, core, places, a_x + a_xp, *qkv_args, bufs=bufs)
        qkv = qkv.reshape(T, N)
        a_all = a_all.reshape(T, D)

        ctx, lse = attn_fwd(qkv, KL, HL)
        ctx_pr = to_core(lax.dynamic_slice_in_dim(ctx, (me ^ 1) * tokens, tokens, 0))
        sizes = (128, 192, 128, 64)
        starts = [sum(sizes[:c]) for c in range(len(sizes))]
        o_parts, o_peers = [], []
        for c, M in enumerate(sizes):
            op = o_rows(base, ctx, ctx_pr, wo2, starts[c], M, 1536)
            o_parts.append(op)
            o_peers.append(to_tp(op))
        ctx_p = to_core(ctx)

        y_blk, gos, dgp = None, [], []
        for c in range(len(sizes)):
            y_blk, go, dg_ = norm_call(post_kernel, o_parts[c], o_peers[c], hidden, d_out, g_post, starts[c], y_blk, True)
            gos.append(go)
            dgp.append(dg_)

        gx = [to_x(g) for g in gos]
        gp = [to_core(g) for g in gos]
        gxp = [to_core(g) for g in gx]
        HN = HL * HEAD
        RE, RL = starts[-1], sizes[-1]
        places = [(core, o) for o in starts[:-1]] + [(1 - core, o) for o in starts[:-1]]
        bufs = gather_matmul(xi, core, places, gos[:-1] + gp[:-1], (wo2,), "nt", (), 2, RE, 0, HN)
        bufs = gather_matmul(1 - xi, core, places, gx[:-1] + gxp[:-1], (wo2,), "nt", (), 2, RE, 0, HN, bufs=bufs)
        places = [(me ^ rel, 0) for rel in range(4)]
        dctx, go_all = gather_matmul(0, core, places, [gos[-1], gp[-1], gx[-1], gxp[-1]], (wo2,), "nt", (), 4, RL, RE, HN, bufs=bufs)
        dctx = dctx.reshape(T, HN)
        go_all = go_all.reshape(T, D)

        dqkv = attn_bwd(qkv, KL, HL, dctx, ctx, lse, cos, sin)
        dqkv_pr = [to_core(lax.dynamic_slice_in_dim(g, (me ^ 1) * tokens, tokens, 0)) for g in dqkv]
        dqkv_p = [to_core(g) for g in dqkv]
        ga_part = ga_rows(base, dqkv, dqkv_pr, (w_q, w_k, w_v), tokens, 512)
        ga_peer = to_tp(ga_part)

        dwo = dwo_proj(base, ctx, ctx_p, go_all, 512).reshape(w_o.shape)
        dwq, dwk, dwv = dw_proj(base, a_all, [g for pair in zip(dqkv, dqkv_p) for g in pair], 256)

        grad_h, dgr = norm_call(pre_kernel, ga_part, ga_peer, hidden, d_out, g_pre, 0, None, False)
        dg = jnp.stack([jnp.sum(dgr, axis=0), jnp.sum(sum(dgp), axis=0)])
        dg = dg + to_core(dg)
        dg = dg + to_x(dg)
        return y_blk, grad_h, dg[0], dwq, dwk, dwv, dwo, dg[1]


    row_spec = P('cp', None)
    head_spec = P(None, 'tp', None)
    out_head_spec = P('tp', None, None)
    return jax.shard_map(device_fn, mesh=mesh, in_specs=(row_spec, P(), head_spec, head_spec, head_spec, out_head_spec, P(), row_spec), out_specs=(row_spec, row_spec, P(), head_spec, head_spec, head_spec, out_head_spec, P()), check_vma=False)
```

```python
import functools

import jax
import jax.numpy as jnp
from jax import lax
from jax.experimental import pallas as pl
from jax.experimental.pallas import tpu as pltpu
from jax.sharding import PartitionSpec as P


SOFT_CAP = 30.0
NORM_EPS = 1e-5
ROPE_THETA = 10000.0
HEAD = 128
LOG2E = 1.4426950408889634
F32 = jnp.float32
BF16 = jnp.bfloat16

NT = (((1,), (1,)), ((), ()))
NN = (((1,), (0,)), ((), ()))


def dotf(a, b, dims):
    return lax.dot_general(a, b, dims, preferred_element_type=F32)


def rope_tables(length):
    half = HEAD // 2
    inv_freq = ROPE_THETA ** (-jnp.arange(half, dtype=F32) * 2.0 / HEAD)
    ang = jnp.arange(length).astype(F32)[:, None] * inv_freq[None, :]
    cos, sin = jnp.cos(ang), jnp.sin(ang)
    return jnp.concatenate([cos, cos], axis=-1), jnp.concatenate([-sin, sin], axis=-1)


QT = 512
SB = 256


def attn_fwd_kernel(q_ref, k_ref, v_ref, ctx_ref, lse_ref, q_s, acc_ref, sum_ref, *, k1, k2):
    i = pl.program_id(1)
    nt = QT // SB
    for t in range(nt):
        rows = slice(t * SB, (t + 1) * SB)
        q_s[t, :SB] = q_ref[rows, :HEAD]
        q_s[t, SB:] = q_ref[rows, HEAD:]
    acc_ref[...] = jnp.zeros_like(acc_ref)
    sum_ref[...] = jnp.zeros_like(sum_ref)

    def chunk(t, row0, mask):
        k = k_ref[pl.ds(row0, SB), :]
        v = v_ref[pl.ds(row0, SB), :]
        s = dotf(q_s[t], k, NT)
        p = jnp.exp2(jnp.tanh(s * k1) * k2)
        if mask is not None:
            p = jnp.where(mask, p, 0.0)
        part = p[:, :128]
        for c in range(1, SB // 128):
            part = part + p[:, c * 128:(c + 1) * 128]
        return part, dotf(p.astype(BF16), v, NN)

    def full(j, carry):
        for t in range(nt):
            ps = [chunk(t, pl.multiple_of(j * QT + m * SB, SB), None) for m in range(nt)]
            sum_ref[t] += ps[0][0] + ps[1][0]
            acc_ref[t] += ps[0][1] + ps[1][1]
        return carry

    lax.fori_loop(0, i, full, 0)

    rows = lax.broadcasted_iota(jnp.int32, (2 * SB, SB), 0) % SB
    cols = lax.broadcasted_iota(jnp.int32, (2 * SB, SB), 1)
    mask = rows >= cols
    for t in range(nt):
        ps = [chunk(t, pl.multiple_of(i * QT + m * SB, SB), mask if m == t else None) for m in range(t + 1)]
        tot, acc = sum_ref[t], acc_ref[t]
        for p in ps:
            tot, acc = tot + p[0], acc + p[1]
        total = jnp.sum(tot, axis=1, keepdims=True)
        ctx = (acc / total).astype(BF16)
        r = slice(t * SB, (t + 1) * SB)
        ctx_ref[r, :HEAD] = ctx[:SB]
        ctx_ref[r, HEAD:] = ctx[SB:]
        lse = jnp.broadcast_to(jnp.log2(total), (2 * SB, 128)).T
        lse_ref[0, 0:1, r] = lse[0:1, :SB]
        lse_ref[0, 1:2, r] = lse[0:1, SB:]


def attn_fwd(qkv, kvh, nq):
    T = qkv.shape[0]
    scale = HEAD ** -0.5
    return pl.pallas_call(
        functools.partial(attn_fwd_kernel, k1=scale / SOFT_CAP, k2=SOFT_CAP * LOG2E),
        grid=(kvh, T // QT),
        in_specs=[
            pl.BlockSpec((QT, 2 * HEAD), lambda h, i: (i, h)),
            pl.BlockSpec((T, HEAD), lambda h, i: (0, nq + h)),
            pl.BlockSpec((T, HEAD), lambda h, i: (0, nq + kvh + h)),
        ],
        out_specs=[
            pl.BlockSpec((QT, 2 * HEAD), lambda h, i: (i, h)),
            pl.BlockSpec((1, 2, QT), lambda h, i: (h, 0, i)),
        ],
        out_shape=[
            jax.ShapeDtypeStruct((T, nq * HEAD), BF16),
            jax.ShapeDtypeStruct((kvh, 2, T), F32),
        ],
        scratch_shapes=[
            pltpu.VMEM((QT // SB, 2 * SB, HEAD), BF16),
            pltpu.VMEM((QT // SB, 2 * SB, HEAD), F32),
            pltpu.VMEM((QT // SB, 2 * SB, 128), F32),
        ],
        compiler_params=pltpu.CompilerParams(dimension_semantics=("arbitrary", "arbitrary")),
        cost_estimate=pl.CostEstimate(flops=int(2 * 2 * T * T * HEAD * kvh * 2), bytes_accessed=2 * qkv.size * 2, transcendentals=0),
        name="attn_fwd",
    )(qkv, qkv, qkv)


BQ = 256
BK = 512


def attn_bwd_kernel(q_ref, k_ref, v_ref, do_ref, ctx_ref, lse_ref, cos_ref, sin_ref, dq_ref, dk_ref, dv_ref,
                    dqa_ref, dka_ref, dva_ref, dd_ref, kt_ref, *, k1, k2, scale):
    J = pl.program_id(1)
    nq = q_ref.shape[0] // BQ
    r = BK // BQ

    @pl.when(J == 0)
    def _():
        dqa_ref[...] = jnp.zeros_like(dqa_ref)
        for g in range(2):
            for i in range(nq):
                sl = slice(i * BQ, (i + 1) * BQ)
                prod = do_ref[sl, g * HEAD:(g + 1) * HEAD].astype(F32) * ctx_ref[sl, g * HEAD:(g + 1) * HEAD].astype(F32)
                dd_ref[g, 0:1, sl] = jnp.sum(prod.T, axis=0, keepdims=True)

    dka_ref[...] = jnp.zeros_like(dka_ref)
    dva_ref[...] = jnp.zeros_like(dva_ref)
    k = k_ref[...]
    v = v_ref[...]
    kt_ref[...] = k.T

    def tile(i, mask):
        row0 = pl.multiple_of(i * BQ, BQ)
        rs = pl.ds(row0, BQ)
        dks, dvs = [], []
        for g in range(2):
            q = q_ref[rs, g * HEAD:(g + 1) * HEAD]
            do = do_ref[rs, g * HEAD:(g + 1) * HEAD]
            lse = lse_ref[0, g:g + 1, rs]
            dd = dd_ref[g, 0:1, rs]
            s = dotf(k, q, NT)
            u = jnp.tanh(s * k1)
            p = jnp.exp2(u * k2 - lse)
            if mask is not None:
                p = jnp.where(mask, p, 0.0)
            dp = dotf(v, do, NT)
            ds = (p * (dp - dd) * (1.0 - u * u)).astype(BF16)
            dvs.append(dotf(p.astype(BF16), do, NN))
            dks.append(dotf(ds, q, NN))
            dqa_ref[g, :, rs] += dotf(kt_ref[...], ds, NN)
        dva_ref[...] += dvs[0] + dvs[1]
        dka_ref[...] += dks[0] + dks[1]

    kpos = lax.broadcasted_iota(jnp.int32, (BK, BQ), 0)
    qpos = lax.broadcasted_iota(jnp.int32, (BK, BQ), 1)
    for m in range(r):
        tile(J * r + m, qpos + m * BQ >= kpos)

    def body(j, carry):
        for m in range(r):
            tile(j * r + m, None)
        return carry

    lax.fori_loop(J + 1, nq // r, body, 0)

    krow = pl.ds(pl.multiple_of(J * BK, BK), BK)

    def unrope(g, cos, sin):
        return (g * cos - pltpu.roll(g, HEAD // 2, 1) * sin) * scale

    dk_ref[...] = unrope(dka_ref[...], cos_ref[krow, :], sin_ref[krow, :]).astype(BF16)
    dv_ref[...] = dva_ref[...].astype(BF16)
    for g in range(2):
        dq_ref[:, g * HEAD:(g + 1) * HEAD] = unrope(dqa_ref[g, :, krow].T, cos_ref[krow, :], sin_ref[krow, :]).astype(BF16)


def attn_bwd(qkv, kvh, nq, do, ctx, lse, cos, sin):
    T = qkv.shape[0]
    scale = HEAD ** -0.5
    full2 = pl.BlockSpec((T, 2 * HEAD), lambda h, j: (0, h))
    kblk = pl.BlockSpec((BK, HEAD), lambda h, j: (j, h))
    tab = pl.BlockSpec((T, HEAD), lambda h, j: (0, 0))
    return pl.pallas_call(
        functools.partial(attn_bwd_kernel, k1=scale / SOFT_CAP, k2=SOFT_CAP * LOG2E, scale=scale),
        grid=(kvh, T // BK),
        in_specs=[full2, pl.BlockSpec((BK, HEAD), lambda h, j: (j, nq + h)), pl.BlockSpec((BK, HEAD), lambda h, j: (j, nq + kvh + h)), full2, full2, pl.BlockSpec((1, 2, T), lambda h, j: (h, 0, 0)), tab, tab],
        out_specs=[pl.BlockSpec((BK, 2 * HEAD), lambda h, j: (j, h)), kblk, kblk],
        out_shape=[
            jax.ShapeDtypeStruct((T, nq * HEAD), BF16),
            jax.ShapeDtypeStruct((T, kvh * HEAD), BF16),
            jax.ShapeDtypeStruct((T, kvh * HEAD), BF16),
        ],
        scratch_shapes=[
            pltpu.VMEM((2, HEAD, T), F32),
            pltpu.VMEM((BK, HEAD), F32),
            pltpu.VMEM((BK, HEAD), F32),
            pltpu.VMEM((2, 1, T), F32),
            pltpu.VMEM((HEAD, BK), BF16),
        ],
        compiler_params=pltpu.CompilerParams(dimension_semantics=("arbitrary", "arbitrary")),
        cost_estimate=pl.CostEstimate(flops=int(5 * 2 * T * T * HEAD * kvh), bytes_accessed=3 * qkv.size * 2, transcendentals=0),
        name="attn_bwd",
    )(qkv, qkv, qkv, do, ctx, lse, cos, sin)


VMEM_LIMIT = 64_000_000


def gmm_kernel(sc_ref, *refs, layout, mode, R, r0, B, n_rope, aliased):
    np_ = len(layout)
    pieces = refs[:np_]
    w_ref = refs[np_]
    rest = refs[np_ + 1:]
    if mode == "qkv":
        cos_ref, sin_ref = rest[:2]
        rest = rest[2:]
    if aliased:
        rest = rest[2:]
    out_ref, all_ref, x_ref, sem_in, sem_out = rest
    n = pl.program_id(0)
    last = pl.num_programs(0) - 1
    S, M, _ = x_ref.shape
    per = M // R

    def cp_in(p):
        slot, rows = layout[p]
        off = pl.multiple_of(sc_ref[2 + B + p], 16)
        return pltpu.make_async_copy(pieces[p], x_ref.at[slot, pl.ds(off, rows)], sem_in.at[p])

    def cp_out(s, j):
        return pltpu.make_async_copy(
            x_ref.at[s, pl.ds(j * R, R)], all_ref.at[sc_ref[0] * B + sc_ref[2 + s * per + j], pl.ds(r0, R)], sem_out.at[s * per + j])

    @pl.when(n == 0)
    def _():
        for p in range(np_):
            cp_in(p).start()

    for s in range(S):
        @pl.when(n == 0)
        def _(s=s):
            for p in range(np_):
                if layout[p][0] == s:
                    cp_in(p).wait()
            for j in range(per):
                cp_out(s, j).start()

        res = dotf(x_ref[s], w_ref[...], NN if mode == "qkv" else NT)
        for j in range(per):
            dst = sc_ref[2 + s * per + j]
            rows = res[j * R:(j + 1) * R]
            if mode == "qkv":
                c = jnp.where(n < n_rope, cos_ref[dst], 1.0)
                t = jnp.where(n < n_rope, sin_ref[dst], 0.0)
                for h in range(rows.shape[1] // HEAD):
                    r = rows[:, h * HEAD:(h + 1) * HEAD]
                    out_ref[dst, :, h * HEAD:(h + 1) * HEAD] = (r * c + pltpu.roll(r, HEAD // 2, 1) * t).astype(BF16)
            else:
                out_ref[dst] = rows.astype(BF16)

    @pl.when(n == last)
    def _():
        for s in range(S):
            for j in range(per):
                cp_out(s, j).wait()


def gather_matmul(chip, core, places, pieces, w, mode, tabs, S, dsts, R, r0, N, bufs=None):
    D = pieces[0].shape[1]
    tokens, nb = 512, 512
    B = len(dsts)
    scal = jnp.stack([jnp.asarray(v, jnp.int32) for v in [chip, core] + list(dsts) + [o for _, o in places]])
    layout = tuple((slot, p.shape[0]) for (slot, _), p in zip(places, pieces))
    anyspec = pl.BlockSpec(memory_space=pl.ANY)
    if mode == "qkv":
        w_specs = [pl.BlockSpec((D, nb), lambda n, s: (0, n))]
        w_specs += [pl.BlockSpec((B, R, HEAD), lambda n, s: (s[0], 0, 0), pipeline_mode=pl.Buffered(1))] * 2
    else:
        w_specs = [pl.BlockSpec((nb, D), lambda n, s: (s[1] * (N // nb) + n, 0))]
    in_specs = [anyspec] * len(pieces) + w_specs
    args = list(pieces) + [w] + [t.reshape(4, tokens, HEAD) for t in tabs]
    aliases = {}
    if bufs is not None:
        aliases = {1 + len(args): 0, 2 + len(args): 1}
        in_specs += [anyspec, anyspec]
        args += list(bufs)
    return pl.pallas_call(
        functools.partial(gmm_kernel, layout=layout, mode=mode, R=R, r0=r0, B=B, n_rope=(N * 3 // 4) // nb, aliased=bufs is not None),
        grid_spec=pltpu.PrefetchScalarGridSpec(
            num_scalar_prefetch=1,
            grid=(N // nb,),
            in_specs=in_specs,
            out_specs=[pl.BlockSpec((B, R, nb), lambda n, s: (s[0], r0 // R, n)), anyspec],
            scratch_shapes=[
                pltpu.VMEM((S, B * R // S, D), BF16),
                pltpu.SemaphoreType.DMA((len(pieces),)),
                pltpu.SemaphoreType.DMA((B,)),
            ],
        ),
        out_shape=[jax.ShapeDtypeStruct((4, tokens, N), BF16), jax.ShapeDtypeStruct((4, tokens, D), BF16)],
        input_output_aliases=aliases,
        compiler_params=pltpu.CompilerParams(dimension_semantics=("arbitrary",), vmem_limit_bytes=VMEM_LIMIT),
        cost_estimate=pl.CostEstimate(flops=2 * B * R * D * N, bytes_accessed=B * R * D * 4 + N * D * 2, transcendentals=0),
    )(scal, *args)


def w_kernel(c_ref, wq_ref, wk_ref, wv_ref, out_ref, s_ref):
    nq, n = wq_ref.shape[1] * HEAD, s_ref.shape[2] // 2
    out_ref[:, :nq] = wq_ref[...].reshape(-1, nq)
    half = pl.ds(pl.multiple_of(c_ref[0] * n, n), n)
    for j, ref in enumerate((wk_ref, wv_ref)):
        s_ref[j] = ref[...].reshape(-1, 2 * n)
        out_ref[:, nq + j * n:nq + (j + 1) * n] = s_ref[j, :, half]


def w_layout(c, w_q, w_k, w_v, db):
    D, hb = w_k.shape[:2]
    nq, n = w_q.shape[1] // 2, hb // 2
    N = (nq + 2 * n) * HEAD
    return pl.pallas_call(
        w_kernel,
        grid_spec=pltpu.PrefetchScalarGridSpec(
            num_scalar_prefetch=1,
            grid=(D // db,),
            in_specs=[pl.BlockSpec((db, nq, HEAD), lambda i, s: (i, s[0], 0))] + [pl.BlockSpec((db, hb, HEAD), lambda i, s: (i, 0, 0))] * 2,
            out_specs=pl.BlockSpec((db, N), lambda i, s: (i, 0)),
            scratch_shapes=[pltpu.VMEM((2, db, hb * HEAD), BF16)],
        ),
        out_shape=jax.ShapeDtypeStruct((D, N), BF16),
        compiler_params=pltpu.CompilerParams(dimension_semantics=("arbitrary",), vmem_limit_bytes=VMEM_LIMIT),
        cost_estimate=pl.CostEstimate(flops=D * N * 500, bytes_accessed=D * N * 5, transcendentals=0),
    )(jnp.reshape(c, (1,)).astype(jnp.int32), w_q, w_k, w_v)


def orow_kernel(sc_ref, c0_ref, c1_ref, w_ref, out_ref, *, r0):
    core = sc_ref[1]
    n = c0_ref.shape[1]
    rows = slice(r0, r0 + out_ref.shape[0])
    own = w_ref[pl.ds(pl.multiple_of(core * n, n), n), :]
    oth = w_ref[pl.ds(pl.multiple_of((1 - core) * n, n), n), :]
    out_ref[...] = (dotf(c0_ref[rows, :], own, NN) + dotf(c1_ref[rows, :], oth, NN)).astype(BF16)


def o_rows(scal, ctx, ctx_pr, w, r0, M, db):
    n, D = ctx.shape[1], w.shape[1]
    tokens = ctx_pr.shape[0]
    return pl.pallas_call(
        functools.partial(orow_kernel, r0=r0),
        grid_spec=pltpu.PrefetchScalarGridSpec(
            num_scalar_prefetch=1,
            grid=(D // db,),
            in_specs=[
                pl.BlockSpec((tokens, n), lambda i, s: (s[2], 0)),
                pl.BlockSpec((tokens, n), lambda i, s: (0, 0)),
                pl.BlockSpec((2 * n, db), lambda i, s: (0, i)),
            ],
            out_specs=pl.BlockSpec((M, db), lambda i, s: (0, i)),
        ),
        out_shape=jax.ShapeDtypeStruct((M, D), BF16),
        compiler_params=pltpu.CompilerParams(dimension_semantics=("arbitrary",), vmem_limit_bytes=VMEM_LIMIT),
        cost_estimate=pl.CostEstimate(flops=4 * M * D * n, bytes_accessed=w.size * 2, transcendentals=0),
    )(scal, ctx, ctx_pr, w)


def ga_kernel(sc_ref, q0, k0, v0, q1, k1, v1, w0_ref, w1_ref, out_ref):
    acc = None
    for w_ref, gs in ((w0_ref, (q0, k0, v0)), (w1_ref, (q1, k1, v1))):
        o = 0
        for g in gs:
            n = g.shape[1]
            d = dotf(g[...], w_ref[:, o:o + n], NT)
            acc = d if acc is None else acc + d
            o += n
    out_ref[...] = acc.astype(BF16)


def ga_rows(scal, own, oth, ws, M, db):
    D, N = ws[0].shape
    return pl.pallas_call(
        ga_kernel,
        grid_spec=pltpu.PrefetchScalarGridSpec(
            num_scalar_prefetch=1,
            grid=(D // db,),
            in_specs=[pl.BlockSpec((M, g.shape[1]), lambda i, s: (s[2], 0)) for g in own]
            + [pl.BlockSpec((M, g.shape[1]), lambda i, s: (0, 0)) for g in oth]
            + [pl.BlockSpec((db, N), lambda i, s: (i, 0)) for w in ws],
            out_specs=pl.BlockSpec((M, db), lambda i, s: (0, i)),
        ),
        out_shape=jax.ShapeDtypeStruct((M, D), BF16),
        compiler_params=pltpu.CompilerParams(dimension_semantics=("arbitrary",), vmem_limit_bytes=VMEM_LIMIT),
        cost_estimate=pl.CostEstimate(flops=4 * M * D * N, bytes_accessed=4 * D * N, transcendentals=0),
    )(scal, *own, *oth, *ws)


def dw_kernel(sc_ref, a_ref, q0, q1, k0, k1, v0, v1, oq_ref, ok_ref, ov_ref):
    db = a_ref.shape[1]
    core = sc_ref[1]
    at = a_ref[...].T
    for pair, out_ref in (((q0, q1), oq_ref), ((k0, k1), ok_ref), ((v0, v1), ov_ref)):
        hh = pair[0].shape[1] // HEAD
        nh = 2 * hh
        for other, g_ref in enumerate(pair):
            c = 1 - core if other else core
            res = dotf(at, g_ref[...], NN)
            for h in range(hh):
                out_ref[pl.ds(c * hh + h, db, stride=nh), :] = res[:, h * HEAD:(h + 1) * HEAD]


def dw_proj(scal, a, gs, db):
    T, D = a.shape
    nhs = [2 * gs[0].shape[1] // HEAD, 2 * gs[2].shape[1] // HEAD, 2 * gs[4].shape[1] // HEAD]
    outs = pl.pallas_call(
        dw_kernel,
        grid_spec=pltpu.PrefetchScalarGridSpec(
            num_scalar_prefetch=1,
            grid=(D // db,),
            in_specs=[pl.BlockSpec((T, db), lambda i, s: (0, i))]
            + [pl.BlockSpec(g.shape, lambda i, s: (0, 0), pipeline_mode=pl.Buffered(1)) for g in gs],
            out_specs=[pl.BlockSpec((db * nh, HEAD), lambda i, s: (i, 0)) for nh in nhs],
        ),
        out_shape=[jax.ShapeDtypeStruct((D * nh, HEAD), F32) for nh in nhs],
        compiler_params=pltpu.CompilerParams(dimension_semantics=("arbitrary",), vmem_limit_bytes=VMEM_LIMIT),
        cost_estimate=pl.CostEstimate(flops=2 * T * D * sum(nhs) * HEAD, bytes_accessed=D * sum(nhs) * HEAD * 4, transcendentals=0),
        name="dw_proj",
    )(scal, a, *gs)
    return [o.reshape(D, nh, HEAD) for o, nh in zip(outs, nhs)]


def dwo_kernel(sc_ref, c0_ref, c1_ref, g_ref, out_ref, t_ref):
    core = sc_ref[1]
    n = c0_ref.shape[1]

    @pl.when(pl.program_id(0) == 0)
    def _():
        t_ref[pl.ds(pl.multiple_of(core * n, n), n), :] = c0_ref[...].T
        t_ref[pl.ds(pl.multiple_of((1 - core) * n, n), n), :] = c1_ref[...].T

    out_ref[...] = dotf(t_ref[...], g_ref[...], NN)


def dwo_proj(scal, c0, c1, go, db):
    T, D = go.shape
    n = c0.shape[1]
    return pl.pallas_call(
        dwo_kernel,
        grid_spec=pltpu.PrefetchScalarGridSpec(
            num_scalar_prefetch=1,
            grid=(D // db,),
            in_specs=[pl.BlockSpec((T, n), lambda i, s: (0, 0), pipeline_mode=pl.Buffered(1))] * 2
            + [pl.BlockSpec((T, db), lambda i, s: (0, i))],
            out_specs=pl.BlockSpec((2 * n, db), lambda i, s: (0, i)),
            scratch_shapes=[pltpu.VMEM((2 * n, T), BF16)],
        ),
        out_shape=jax.ShapeDtypeStruct((2 * n, D), F32),
        compiler_params=pltpu.CompilerParams(dimension_semantics=("arbitrary",), vmem_limit_bytes=VMEM_LIMIT),
        cost_estimate=pl.CostEstimate(flops=4 * T * D * n, bytes_accessed=2 * n * D * 4, transcendentals=0),
        name="dwo_proj",
    )(scal, c0, c1, go)


RB = 64


def post_kernel(p_ref, r_ref, h_ref, dy_ref, g_ref, *rest):
    y_ref, go_ref, dg_ref = rest[-3:]
    o = p_ref[...].astype(F32) + r_ref[...].astype(F32)
    inv = lax.rsqrt(jnp.mean(o * o, axis=-1, keepdims=True) + NORM_EPS)
    hat = o * inv
    g = g_ref[...]
    dy = dy_ref[...].astype(F32)
    y_ref[...] = (h_ref[...].astype(F32) + hat * g).astype(BF16)
    gg = dy * g
    go_ref[...] = (inv * (gg - hat * jnp.mean(gg * hat, axis=-1, keepdims=True))).astype(BF16)

    @pl.when(pl.program_id(0) == 0)
    def _():
        dg_ref[...] = jnp.zeros_like(dg_ref)

    dg_ref[...] += jnp.sum((dy * hat).reshape(RB // 8, 8, -1), axis=0)


def pre_kernel(p_ref, r_ref, h_ref, dy_ref, g_ref, *rest):
    dh_ref, dg_ref = rest[-2:]
    ga = p_ref[...].astype(F32) + r_ref[...].astype(F32)
    h = h_ref[...].astype(F32)
    inv = lax.rsqrt(jnp.mean(h * h, axis=-1, keepdims=True) + NORM_EPS)
    hat = h * inv
    gh = ga * g_ref[...]
    dh_ref[...] = (dy_ref[...].astype(F32) + inv * (gh - hat * jnp.mean(gh * hat, axis=-1, keepdims=True))).astype(BF16)

    @pl.when(pl.program_id(0) == 0)
    def _():
        dg_ref[...] = jnp.zeros_like(dg_ref)

    dg_ref[...] += jnp.sum((ga * hat).reshape(RB // 8, 8, -1), axis=0)


def norm_call(kernel, part, peer, hidden, d_out, g, r0, buf, extra):
    M, D = part.shape
    n = M // RB
    loc = pl.BlockSpec((RB, D), lambda i: (i, 0))
    row = pl.BlockSpec((RB, D), lambda i: (r0 // RB + i, 0))
    in_specs = [loc, loc, row, row, pl.BlockSpec((1, D), lambda i: (0, 0))]
    args = [part, peer, hidden, d_out, g.reshape(1, D)]
    aliases = {}
    if buf is not None:
        aliases = {len(args): 0}
        args.append(buf)
        in_specs.append(pl.BlockSpec(memory_space=pl.ANY))
    out_specs = [row] + ([loc] if extra else []) + [pl.BlockSpec((8, D), lambda i: (0, 0))]
    out_shape = [jax.ShapeDtypeStruct(hidden.shape, BF16)]
    if extra:
        out_shape.append(jax.ShapeDtypeStruct((M, D), BF16))
    out_shape.append(jax.ShapeDtypeStruct((8, D), F32))
    return pl.pallas_call(
        kernel, grid=(n,), in_specs=in_specs, out_specs=out_specs, out_shape=out_shape, input_output_aliases=aliases,
        compiler_params=pltpu.CompilerParams(dimension_semantics=("arbitrary",), vmem_limit_bytes=VMEM_LIMIT),
        cost_estimate=pl.CostEstimate(flops=M * D * 2000, bytes_accessed=M * D * 12, transcendentals=0),
    )(*args)


def a_kernel(h_ref, g_ref, a_ref):
    h = h_ref[...].astype(F32)
    inv = lax.rsqrt(jnp.mean(h * h, axis=-1, keepdims=True) + NORM_EPS)
    a_ref[...] = (h * inv * g_ref[...]).astype(BF16)


def a_call(hidden, g):
    M, D = hidden.shape
    row = pl.BlockSpec((RB, D), lambda i: (i, 0))
    return pl.pallas_call(
        a_kernel, grid=(M // RB,), in_specs=[row, pl.BlockSpec((1, D), lambda i: (0, 0))], out_specs=row,
        out_shape=jax.ShapeDtypeStruct((M, D), BF16),
        compiler_params=pltpu.CompilerParams(dimension_semantics=("arbitrary",)),
        cost_estimate=pl.CostEstimate(flops=M * D * 1000, bytes_accessed=M * D * 4, transcendentals=0),
        name="a_norm",
    )(hidden, g.reshape(1, D))


def solution(mesh):
    core_perm = [(0, 1), (1, 0), (2, 3), (3, 2)]
    x_perm = [(0, 2), (2, 0), (1, 3), (3, 1)]
    tp_perm = [(0, 1), (1, 0)]

    def to_core(v):
        return lax.ppermute(v, 'cp', core_perm)

    def to_x(v):
        return lax.ppermute(v, 'cp', x_perm)

    def to_tp(v):
        return lax.ppermute(v, 'tp', tp_perm)

    def device_fn(hidden, g_pre, w_q, w_k, w_v, w_o, g_post, d_out):
        tokens, D = hidden.shape
        T = 4 * tokens
        me = lax.axis_index('cp')
        tp = lax.axis_index('tp')
        core, xi = me % 2, me // 2
        HL = w_q.shape[1] // 2
        KL = w_k.shape[1] // 2
        cos, sin = lax.optimization_barrier(rope_tables(T))
        base = jnp.stack([xi, core, me, me ^ 1]).astype(jnp.int32)

        def two_way(blk, n):
            r1 = to_x(lax.dynamic_slice_in_dim(blk, tp * n, n, 0))
            r3 = to_x(blk[2 * n:])
            r2 = to_tp(r1)
            return [r1, r2, r3], [tp * n, (1 - tp) * n, 2 * n]

        a_loc = a_call(hidden, g_pre)
        a_x, a_off = two_way(a_loc, 176)
        a_p = to_core(a_loc)
        a_xp = [to_core(r) for r in a_x]
        wo2 = w_o.reshape(-1, D)
        N = (HL + 2 * KL) * HEAD
        w_own = w_layout(core, w_q, w_k, w_v, 512)
        w_oth = w_layout(1 - core, w_q, w_k, w_v, 512)
        qkv_args = (w_own, "qkv", (cos, sin), 2, [core, 1 - core], tokens, 0, N)
        bufs = gather_matmul(xi, core, [(0, 0), (1, 0)], [a_loc, a_p], *qkv_args)
        places = [(0, o) for o in a_off] + [(1, o) for o in a_off]
        qkv, a_all = gather_matmul(1 - xi, core, places, a_x + a_xp, *qkv_args, bufs=bufs)
        qkv = qkv.reshape(T, N)
        a_all = a_all.reshape(T, D)

        ctx, lse = attn_fwd(qkv, KL, HL)
        ctx_pr = to_core(lax.dynamic_slice_in_dim(ctx, (me ^ 1) * tokens, tokens, 0))
        sizes = (128, 192, 128, 64)
        starts = [sum(sizes[:c]) for c in range(len(sizes))]
        o_parts, o_peers = [], []
        for c, M in enumerate(sizes):
            op = o_rows(base, ctx, ctx_pr, wo2, starts[c], M, 1536)
            o_parts.append(op)
            o_peers.append(to_tp(op))
        ctx_p = to_core(ctx)

        y_blk, gos, dgp = None, [], []
        for c in range(len(sizes)):
            y_blk, go, dg_ = norm_call(post_kernel, o_parts[c], o_peers[c], hidden, d_out, g_post, starts[c], y_blk, True)
            gos.append(go)
            dgp.append(dg_)

        gx = [to_x(g) for g in gos]
        gp = [to_core(g) for g in gos]
        gxp = [to_core(g) for g in gx]
        HN = HL * HEAD
        RE, RL = starts[-1], sizes[-1]
        places = [(c, o) for c in range(2) for o in starts[:-1]]
        pair = [core, 1 - core]
        bufs = gather_matmul(xi, core, places, gos[:-1] + gp[:-1], wo2, "nt", (), 2, pair, RE, 0, HN)
        bufs = gather_matmul(1 - xi, core, places, gx[:-1] + gxp[:-1], wo2, "nt", (), 2, pair, RE, 0, HN, bufs=bufs)
        places = [(0, rel * RL) for rel in range(4)]
        dctx, go_all = gather_matmul(0, core, places, [gos[-1], gp[-1], gx[-1], gxp[-1]], wo2, "nt", (), 1, [me ^ rel for rel in range(4)],
                                     RL, RE, HN, bufs=bufs)
        dctx = dctx.reshape(T, HN)
        go_all = go_all.reshape(T, D)

        dqkv = attn_bwd(qkv, KL, HL, dctx, ctx, lse, cos, sin)
        dqkv_pr = [to_core(lax.dynamic_slice_in_dim(g, (me ^ 1) * tokens, tokens, 0)) for g in dqkv]
        dqkv_p = [to_core(g) for g in dqkv]
        ga_part = ga_rows(base, dqkv, dqkv_pr, (w_own, w_oth), tokens, 512)
        ga_peer = to_tp(ga_part)

        dwo = dwo_proj(base, ctx, ctx_p, go_all, 512).reshape(w_o.shape)
        dwq, dwk, dwv = dw_proj(base, a_all, [g for pair in zip(dqkv, dqkv_p) for g in pair], 256)

        grad_h, dgr = norm_call(pre_kernel, ga_part, ga_peer, hidden, d_out, g_pre, 0, None, False)
        dg = jnp.stack([jnp.sum(dgr, axis=0), jnp.sum(sum(dgp), axis=0)])
        dg = dg + to_core(dg)
        dg = dg + to_x(dg)
        return y_blk, grad_h, dg[0], dwq, dwk, dwv, dwo, dg[1]


    row_spec = P('cp', None)
    head_spec = P(None, 'tp', None)
    out_head_spec = P('tp', None, None)
    return jax.shard_map(device_fn, mesh=mesh, in_specs=(row_spec, P(), head_spec, head_spec, head_spec, out_head_spec, P(), row_spec), out_specs=(row_spec, row_spec, P(), head_spec, head_spec, head_spec, out_head_spec, P()), check_vma=False)
```

```python
import functools

import jax
import jax.numpy as jnp
from jax import lax
from jax.experimental import pallas as pl
from jax.experimental.pallas import tpu as pltpu
from jax.sharding import PartitionSpec as P


SOFT_CAP = 30.0
NORM_EPS = 1e-5
ROPE_THETA = 10000.0
HEAD = 128
LOG2E = 1.4426950408889634
F32 = jnp.float32
BF16 = jnp.bfloat16

NT = (((1,), (1,)), ((), ()))
NN = (((1,), (0,)), ((), ()))


def dotf(a, b, dims):
    return lax.dot_general(a, b, dims, preferred_element_type=F32)


def rope_tables(length):
    half = HEAD // 2
    inv_freq = ROPE_THETA ** (-jnp.arange(half, dtype=F32) * 2.0 / HEAD)
    ang = jnp.arange(length).astype(F32)[:, None] * inv_freq[None, :]
    cos, sin = jnp.cos(ang), jnp.sin(ang)
    return jnp.concatenate([cos, cos], axis=-1), jnp.concatenate([-sin, sin], axis=-1)


QT = 512
SB = 256


def attn_fwd_kernel(q_ref, k_ref, v_ref, ctx_ref, lse_ref, q_s, acc_ref, sum_ref, *, k1, k2):
    i = pl.program_id(1)
    nt = QT // SB
    for t in range(nt):
        rows = slice(t * SB, (t + 1) * SB)
        q_s[t, :SB] = q_ref[rows, :HEAD]
        q_s[t, SB:] = q_ref[rows, HEAD:]
    acc_ref[...] = jnp.zeros_like(acc_ref)
    sum_ref[...] = jnp.zeros_like(sum_ref)

    def chunk(t, row0, mask):
        k = k_ref[pl.ds(row0, SB), :]
        v = v_ref[pl.ds(row0, SB), :]
        s = dotf(q_s[t], k, NT)
        p = jnp.exp2(jnp.tanh(s * k1) * k2)
        if mask is not None:
            p = jnp.where(mask, p, 0.0)
        part = p[:, :128]
        for c in range(1, SB // 128):
            part = part + p[:, c * 128:(c + 1) * 128]
        return part, dotf(p.astype(BF16), v, NN)

    def full(j, carry):
        for t in range(nt):
            ps = [chunk(t, pl.multiple_of(j * QT + m * SB, SB), None) for m in range(nt)]
            sum_ref[t] += ps[0][0] + ps[1][0]
            acc_ref[t] += ps[0][1] + ps[1][1]
        return carry

    lax.fori_loop(0, i, full, 0)

    rows = lax.broadcasted_iota(jnp.int32, (2 * SB, SB), 0) % SB
    cols = lax.broadcasted_iota(jnp.int32, (2 * SB, SB), 1)
    mask = rows >= cols
    for t in range(nt):
        ps = [chunk(t, pl.multiple_of(i * QT + m * SB, SB), mask if m == t else None) for m in range(t + 1)]
        tot, acc = sum_ref[t], acc_ref[t]
        for p in ps:
            tot, acc = tot + p[0], acc + p[1]
        total = jnp.sum(tot, axis=1, keepdims=True)
        ctx = (acc / total).astype(BF16)
        r = slice(t * SB, (t + 1) * SB)
        ctx_ref[r, :HEAD] = ctx[:SB]
        ctx_ref[r, HEAD:] = ctx[SB:]
        lse = jnp.broadcast_to(jnp.log2(total), (2 * SB, 128)).T
        lse_ref[0, 0:1, r] = lse[0:1, :SB]
        lse_ref[0, 1:2, r] = lse[0:1, SB:]


def attn_fwd(qkv, kvh, nq):
    T = qkv.shape[0]
    scale = HEAD ** -0.5
    return pl.pallas_call(
        functools.partial(attn_fwd_kernel, k1=scale / SOFT_CAP, k2=SOFT_CAP * LOG2E),
        grid=(kvh, T // QT),
        in_specs=[
            pl.BlockSpec((QT, 2 * HEAD), lambda h, i: (i, h)),
            pl.BlockSpec((T, HEAD), lambda h, i: (0, nq + h)),
            pl.BlockSpec((T, HEAD), lambda h, i: (0, nq + kvh + h)),
        ],
        out_specs=[
            pl.BlockSpec((QT, 2 * HEAD), lambda h, i: (i, h)),
            pl.BlockSpec((1, 2, QT), lambda h, i: (h, 0, i)),
        ],
        out_shape=[
            jax.ShapeDtypeStruct((T, nq * HEAD), BF16),
            jax.ShapeDtypeStruct((kvh, 2, T), F32),
        ],
        scratch_shapes=[
            pltpu.VMEM((QT // SB, 2 * SB, HEAD), BF16),
            pltpu.VMEM((QT // SB, 2 * SB, HEAD), F32),
            pltpu.VMEM((QT // SB, 2 * SB, 128), F32),
        ],
        compiler_params=pltpu.CompilerParams(dimension_semantics=("arbitrary", "arbitrary")),
        cost_estimate=pl.CostEstimate(flops=int(2 * 2 * T * T * HEAD * kvh * 2), bytes_accessed=2 * qkv.size * 2, transcendentals=0),
        name="attn_fwd",
    )(qkv, qkv, qkv)


BQ = 256
BK = 512


def attn_bwd_kernel(q_ref, k_ref, v_ref, do_ref, ctx_ref, lse_ref, cos_ref, sin_ref, dq_ref, dk_ref, dv_ref,
                    dqa_ref, dka_ref, dva_ref, dd_ref, kt_ref, *, k1, k2, scale):
    J = pl.program_id(1)
    nq = q_ref.shape[0] // BQ
    r = BK // BQ

    @pl.when(J == 0)
    def _():
        dqa_ref[...] = jnp.zeros_like(dqa_ref)
        for g in range(2):
            for i in range(nq):
                sl = slice(i * BQ, (i + 1) * BQ)
                prod = do_ref[sl, g * HEAD:(g + 1) * HEAD].astype(F32) * ctx_ref[sl, g * HEAD:(g + 1) * HEAD].astype(F32)
                dd_ref[g, 0:1, sl] = jnp.sum(prod.T, axis=0, keepdims=True)

    dka_ref[...] = jnp.zeros_like(dka_ref)
    dva_ref[...] = jnp.zeros_like(dva_ref)
    k = k_ref[...]
    v = v_ref[...]
    kt_ref[...] = k.T

    def tile(i, mask):
        row0 = pl.multiple_of(i * BQ, BQ)
        rs = pl.ds(row0, BQ)
        dks, dvs = [], []
        for g in range(2):
            q = q_ref[rs, g * HEAD:(g + 1) * HEAD]
            do = do_ref[rs, g * HEAD:(g + 1) * HEAD]
            lse = lse_ref[0, g:g + 1, rs]
            dd = dd_ref[g, 0:1, rs]
            s = dotf(k, q, NT)
            u = jnp.tanh(s * k1)
            p = jnp.exp2(u * k2 - lse)
            if mask is not None:
                p = jnp.where(mask, p, 0.0)
            dp = dotf(v, do, NT)
            ds = (p * (dp - dd) * (1.0 - u * u)).astype(BF16)
            dvs.append(dotf(p.astype(BF16), do, NN))
            dks.append(dotf(ds, q, NN))
            dqa_ref[g, :, rs] += dotf(kt_ref[...], ds, NN)
        dva_ref[...] += dvs[0] + dvs[1]
        dka_ref[...] += dks[0] + dks[1]

    kpos = lax.broadcasted_iota(jnp.int32, (BK, BQ), 0)
    qpos = lax.broadcasted_iota(jnp.int32, (BK, BQ), 1)
    for m in range(r):
        tile(J * r + m, qpos + m * BQ >= kpos)

    def body(j, carry):
        for m in range(r):
            tile(j * r + m, None)
        return carry

    lax.fori_loop(J + 1, nq // r, body, 0)

    krow = pl.ds(pl.multiple_of(J * BK, BK), BK)

    def unrope(g, cos, sin):
        return (g * cos - pltpu.roll(g, HEAD // 2, 1) * sin) * scale

    dk_ref[...] = unrope(dka_ref[...], cos_ref[krow, :], sin_ref[krow, :]).astype(BF16)
    dv_ref[...] = dva_ref[...].astype(BF16)
    for g in range(2):
        dq_ref[:, g * HEAD:(g + 1) * HEAD] = unrope(dqa_ref[g, :, krow].T, cos_ref[krow, :], sin_ref[krow, :]).astype(BF16)


def attn_bwd(qkv, kvh, nq, do, ctx, lse, cos, sin):
    T = qkv.shape[0]
    scale = HEAD ** -0.5
    full2 = pl.BlockSpec((T, 2 * HEAD), lambda h, j: (0, h))
    kblk = pl.BlockSpec((BK, HEAD), lambda h, j: (j, h))
    tab = pl.BlockSpec((T, HEAD), lambda h, j: (0, 0))
    return pl.pallas_call(
        functools.partial(attn_bwd_kernel, k1=scale / SOFT_CAP, k2=SOFT_CAP * LOG2E, scale=scale),
        grid=(kvh, T // BK),
        in_specs=[full2, pl.BlockSpec((BK, HEAD), lambda h, j: (j, nq + h)), pl.BlockSpec((BK, HEAD), lambda h, j: (j, nq + kvh + h)), full2, full2, pl.BlockSpec((1, 2, T), lambda h, j: (h, 0, 0)), tab, tab],
        out_specs=[pl.BlockSpec((BK, 2 * HEAD), lambda h, j: (j, h)), kblk, kblk],
        out_shape=[
            jax.ShapeDtypeStruct((T, nq * HEAD), BF16),
            jax.ShapeDtypeStruct((T, kvh * HEAD), BF16),
            jax.ShapeDtypeStruct((T, kvh * HEAD), BF16),
        ],
        scratch_shapes=[
            pltpu.VMEM((2, HEAD, T), F32),
            pltpu.VMEM((BK, HEAD), F32),
            pltpu.VMEM((BK, HEAD), F32),
            pltpu.VMEM((2, 1, T), F32),
            pltpu.VMEM((HEAD, BK), BF16),
        ],
        compiler_params=pltpu.CompilerParams(dimension_semantics=("arbitrary", "arbitrary")),
        cost_estimate=pl.CostEstimate(flops=int(5 * 2 * T * T * HEAD * kvh), bytes_accessed=3 * qkv.size * 2, transcendentals=0),
        name="attn_bwd",
    )(qkv, qkv, qkv, do, ctx, lse, cos, sin)


VMEM_LIMIT = 64_000_000


def gmm_kernel(sc_ref, *refs, layout, mode, R, r0, B, n_rope, aliased):
    np_ = len(layout)
    pieces = refs[:np_]
    w_ref = refs[np_]
    rest = refs[np_ + 1:]
    if mode == "qkv":
        cos_ref, sin_ref = rest[:2]
        rest = rest[2:]
    if aliased:
        rest = rest[2:]
    out_ref, all_ref, x_ref, sem_in, sem_out = rest
    n = pl.program_id(0)
    last = pl.num_programs(0) - 1
    S, M, _ = x_ref.shape
    per = M // R

    def cp_in(p):
        slot, rows = layout[p]
        off = pl.multiple_of(sc_ref[2 + B + p], 16)
        return pltpu.make_async_copy(pieces[p], x_ref.at[slot, pl.ds(off, rows)], sem_in.at[p])

    def cp_out(s, j):
        return pltpu.make_async_copy(
            x_ref.at[s, pl.ds(j * R, R)], all_ref.at[sc_ref[0] * B + sc_ref[2 + s * per + j], pl.ds(r0, R)], sem_out.at[s * per + j])

    @pl.when(n == 0)
    def _():
        for p in range(np_):
            cp_in(p).start()

    for s in range(S):
        @pl.when(n == 0)
        def _(s=s):
            for p in range(np_):
                if layout[p][0] == s:
                    cp_in(p).wait()
            for j in range(per):
                cp_out(s, j).start()

        res = dotf(x_ref[s], w_ref[...], NN if mode == "qkv" else NT)
        for j in range(per):
            dst = sc_ref[2 + s * per + j]
            rows = res[j * R:(j + 1) * R]
            if mode == "qkv":
                c = jnp.where(n < n_rope, cos_ref[dst], 1.0)
                t = jnp.where(n < n_rope, sin_ref[dst], 0.0)
                for h in range(rows.shape[1] // HEAD):
                    r = rows[:, h * HEAD:(h + 1) * HEAD]
                    out_ref[dst, :, h * HEAD:(h + 1) * HEAD] = (r * c + pltpu.roll(r, HEAD // 2, 1) * t).astype(BF16)
            else:
                out_ref[dst] = rows.astype(BF16)

    @pl.when(n == last)
    def _():
        for s in range(S):
            for j in range(per):
                cp_out(s, j).wait()


def gather_matmul(chip, core, places, pieces, w, mode, tabs, S, dsts, R, r0, N, bufs=None):
    D = pieces[0].shape[1]
    tokens, nb = 512, 512
    B = len(dsts)
    scal = jnp.stack([jnp.asarray(v, jnp.int32) for v in [chip, core] + list(dsts) + [o for _, o in places]])
    layout = tuple((slot, p.shape[0]) for (slot, _), p in zip(places, pieces))
    anyspec = pl.BlockSpec(memory_space=pl.ANY)
    if mode == "qkv":
        w_specs = [pl.BlockSpec((D, nb), lambda n, s: (0, n))]
        w_specs += [pl.BlockSpec((B, R, HEAD), lambda n, s: (s[0], 0, 0), pipeline_mode=pl.Buffered(1))] * 2
    else:
        w_specs = [pl.BlockSpec((nb, D), lambda n, s: (s[1] * (N // nb) + n, 0))]
    in_specs = [anyspec] * len(pieces) + w_specs
    args = list(pieces) + [w] + [t.reshape(4, tokens, HEAD) for t in tabs]
    aliases = {}
    if bufs is not None:
        aliases = {1 + len(args): 0, 2 + len(args): 1}
        in_specs += [anyspec, anyspec]
        args += list(bufs)
    return pl.pallas_call(
        functools.partial(gmm_kernel, layout=layout, mode=mode, R=R, r0=r0, B=B, n_rope=(N * 3 // 4) // nb, aliased=bufs is not None),
        grid_spec=pltpu.PrefetchScalarGridSpec(
            num_scalar_prefetch=1,
            grid=(N // nb,),
            in_specs=in_specs,
            out_specs=[pl.BlockSpec((B, R, nb), lambda n, s: (s[0], r0 // R, n)), anyspec],
            scratch_shapes=[
                pltpu.VMEM((S, B * R // S, D), BF16),
                pltpu.SemaphoreType.DMA((len(pieces),)),
                pltpu.SemaphoreType.DMA((B,)),
            ],
        ),
        out_shape=[jax.ShapeDtypeStruct((4, tokens, N), BF16), jax.ShapeDtypeStruct((4, tokens, D), BF16)],
        input_output_aliases=aliases,
        compiler_params=pltpu.CompilerParams(dimension_semantics=("arbitrary",), vmem_limit_bytes=VMEM_LIMIT),
        cost_estimate=pl.CostEstimate(flops=2 * B * R * D * N, bytes_accessed=B * R * D * 4 + N * D * 2, transcendentals=0),
    )(scal, *args)


def w_kernel(c_ref, wq_ref, wk_ref, wv_ref, out_ref, s_ref):
    nq, n = wq_ref.shape[1] * HEAD, s_ref.shape[2] // 2
    out_ref[:, :nq] = wq_ref[...].reshape(-1, nq)
    half = pl.ds(pl.multiple_of(c_ref[0] * n, n), n)
    for j, ref in enumerate((wk_ref, wv_ref)):
        s_ref[j] = ref[...].reshape(-1, 2 * n)
        out_ref[:, nq + j * n:nq + (j + 1) * n] = s_ref[j, :, half]


def w_layout(c, w_q, w_k, w_v, db, part=0, parts=1):
    D, hb = w_k.shape[:2]
    D //= parts
    i0 = part * (D // db)
    nq, n = w_q.shape[1] // 2, hb // 2
    N = (nq + 2 * n) * HEAD
    return pl.pallas_call(
        w_kernel,
        grid_spec=pltpu.PrefetchScalarGridSpec(
            num_scalar_prefetch=1,
            grid=(D // db,),
            in_specs=[pl.BlockSpec((db, nq, HEAD), lambda i, s: (i0 + i, s[0], 0))] + [pl.BlockSpec((db, hb, HEAD), lambda i, s: (i0 + i, 0, 0))] * 2,
            out_specs=pl.BlockSpec((db, N), lambda i, s: (i, 0)),
            scratch_shapes=[pltpu.VMEM((2, db, hb * HEAD), BF16)],
        ),
        out_shape=jax.ShapeDtypeStruct((D, N), BF16),
        compiler_params=pltpu.CompilerParams(dimension_semantics=("arbitrary",), vmem_limit_bytes=VMEM_LIMIT),
        cost_estimate=pl.CostEstimate(flops=D * N * 500, bytes_accessed=D * N * 5, transcendentals=0),
    )(jnp.reshape(c, (1,)).astype(jnp.int32), w_q, w_k, w_v)


def orow_kernel(sc_ref, c0_ref, c1_ref, w_ref, out_ref, *, r0):
    core = sc_ref[1]
    n = c0_ref.shape[1]
    rows = slice(r0, r0 + out_ref.shape[0])
    own = w_ref[pl.ds(pl.multiple_of(core * n, n), n), :]
    oth = w_ref[pl.ds(pl.multiple_of((1 - core) * n, n), n), :]
    out_ref[...] = (dotf(c0_ref[rows, :], own, NN) + dotf(c1_ref[rows, :], oth, NN)).astype(BF16)


def o_rows(scal, ctx, ctx_pr, w, r0, M, db):
    n, D = ctx.shape[1], w.shape[1]
    tokens = ctx_pr.shape[0]
    return pl.pallas_call(
        functools.partial(orow_kernel, r0=r0),
        grid_spec=pltpu.PrefetchScalarGridSpec(
            num_scalar_prefetch=1,
            grid=(D // db,),
            in_specs=[
                pl.BlockSpec((tokens, n), lambda i, s: (s[2], 0)),
                pl.BlockSpec((tokens, n), lambda i, s: (0, 0)),
                pl.BlockSpec((2 * n, db), lambda i, s: (0, i)),
            ],
            out_specs=pl.BlockSpec((M, db), lambda i, s: (0, i)),
        ),
        out_shape=jax.ShapeDtypeStruct((M, D), BF16),
        compiler_params=pltpu.CompilerParams(dimension_semantics=("arbitrary",), vmem_limit_bytes=VMEM_LIMIT),
        cost_estimate=pl.CostEstimate(flops=4 * M * D * n, bytes_accessed=w.size * 2, transcendentals=0),
    )(scal, ctx, ctx_pr, w)


def ga_kernel(sc_ref, q0, k0, v0, q1, k1, v1, w0_ref, wa_ref, wb_ref, out_ref, w1_ref):
    i = pl.program_id(0)
    half = pl.num_programs(0) // 2

    @pl.when(i < half)
    def _():
        w1_ref[...] = wa_ref[...]

    @pl.when(i >= half)
    def _():
        w1_ref[...] = wb_ref[...]

    acc = None
    for w_ref, gs in ((w0_ref, (q0, k0, v0)), (w1_ref, (q1, k1, v1))):
        o = 0
        for g in gs:
            n = g.shape[1]
            d = dotf(g[...], w_ref[:, o:o + n], NT)
            acc = d if acc is None else acc + d
            o += n
    out_ref[...] = acc.astype(BF16)


def ga_rows(scal, own, oth, ws, M, db):
    D, N = ws[0].shape
    half = D // db // 2
    return pl.pallas_call(
        ga_kernel,
        grid_spec=pltpu.PrefetchScalarGridSpec(
            num_scalar_prefetch=1,
            grid=(D // db,),
            in_specs=[pl.BlockSpec((M, g.shape[1]), lambda i, s: (s[2], 0)) for g in own]
            + [pl.BlockSpec((M, g.shape[1]), lambda i, s: (0, 0)) for g in oth]
            + [pl.BlockSpec((db, N), lambda i, s: (i, 0)), pl.BlockSpec((db, N), lambda i, s: (jnp.minimum(i, half - 1), 0)),
               pl.BlockSpec((db, N), lambda i, s: (jnp.maximum(i - half, 0), 0))],
            out_specs=pl.BlockSpec((M, db), lambda i, s: (0, i)),
            scratch_shapes=[pltpu.VMEM((db, N), BF16)],
        ),
        out_shape=jax.ShapeDtypeStruct((M, D), BF16),
        compiler_params=pltpu.CompilerParams(dimension_semantics=("arbitrary",), vmem_limit_bytes=VMEM_LIMIT),
        cost_estimate=pl.CostEstimate(flops=4 * M * D * N, bytes_accessed=4 * D * N, transcendentals=0),
    )(scal, *own, *oth, *ws)


def dw_kernel(sc_ref, a_ref, q0, q1, k0, k1, v0, v1, oq_ref, ok_ref, ov_ref):
    db = a_ref.shape[1]
    core = sc_ref[1]
    at = a_ref[...].T
    for pair, out_ref in (((q0, q1), oq_ref), ((k0, k1), ok_ref), ((v0, v1), ov_ref)):
        hh = pair[0].shape[1] // HEAD
        nh = 2 * hh
        for other, g_ref in enumerate(pair):
            c = 1 - core if other else core
            res = dotf(at, g_ref[...], NN)
            for h in range(hh):
                out_ref[pl.ds(c * hh + h, db, stride=nh), :] = res[:, h * HEAD:(h + 1) * HEAD]


def dw_proj(scal, a, gs, db):
    T, D = a.shape
    nhs = [2 * gs[0].shape[1] // HEAD, 2 * gs[2].shape[1] // HEAD, 2 * gs[4].shape[1] // HEAD]
    outs = pl.pallas_call(
        dw_kernel,
        grid_spec=pltpu.PrefetchScalarGridSpec(
            num_scalar_prefetch=1,
            grid=(D // db,),
            in_specs=[pl.BlockSpec((T, db), lambda i, s: (0, i))]
            + [pl.BlockSpec(g.shape, lambda i, s: (0, 0), pipeline_mode=pl.Buffered(1)) for g in gs],
            out_specs=[pl.BlockSpec((db * nh, HEAD), lambda i, s: (i, 0)) for nh in nhs],
        ),
        out_shape=[jax.ShapeDtypeStruct((D * nh, HEAD), F32) for nh in nhs],
        compiler_params=pltpu.CompilerParams(dimension_semantics=("arbitrary",), vmem_limit_bytes=VMEM_LIMIT),
        cost_estimate=pl.CostEstimate(flops=2 * T * D * sum(nhs) * HEAD, bytes_accessed=D * sum(nhs) * HEAD * 4, transcendentals=0),
        name="dw_proj",
    )(scal, a, *gs)
    return [o.reshape(D, nh, HEAD) for o, nh in zip(outs, nhs)]


def dwo_kernel(sc_ref, c0_ref, c1_ref, g_ref, out_ref, t_ref):
    core = sc_ref[1]
    n = c0_ref.shape[1]

    @pl.when(pl.program_id(0) == 0)
    def _():
        t_ref[pl.ds(pl.multiple_of(core * n, n), n), :] = c0_ref[...].T
        t_ref[pl.ds(pl.multiple_of((1 - core) * n, n), n), :] = c1_ref[...].T

    out_ref[...] = dotf(t_ref[...], g_ref[...], NN)


def dwo_proj(scal, c0, c1, go, db):
    T, D = go.shape
    n = c0.shape[1]
    return pl.pallas_call(
        dwo_kernel,
        grid_spec=pltpu.PrefetchScalarGridSpec(
            num_scalar_prefetch=1,
            grid=(D // db,),
            in_specs=[pl.BlockSpec((T, n), lambda i, s: (0, 0), pipeline_mode=pl.Buffered(1))] * 2
            + [pl.BlockSpec((T, db), lambda i, s: (0, i))],
            out_specs=pl.BlockSpec((2 * n, db), lambda i, s: (0, i)),
            scratch_shapes=[pltpu.VMEM((2 * n, T), BF16)],
        ),
        out_shape=jax.ShapeDtypeStruct((2 * n, D), F32),
        compiler_params=pltpu.CompilerParams(dimension_semantics=("arbitrary",), vmem_limit_bytes=VMEM_LIMIT),
        cost_estimate=pl.CostEstimate(flops=4 * T * D * n, bytes_accessed=2 * n * D * 4, transcendentals=0),
        name="dwo_proj",
    )(scal, c0, c1, go)


RB = 64


def post_kernel(p_ref, r_ref, h_ref, dy_ref, g_ref, *rest):
    y_ref, go_ref, dg_ref = rest[-3:]
    o = p_ref[...].astype(F32) + r_ref[...].astype(F32)
    inv = lax.rsqrt(jnp.mean(o * o, axis=-1, keepdims=True) + NORM_EPS)
    hat = o * inv
    g = g_ref[...]
    dy = dy_ref[...].astype(F32)
    y_ref[...] = (h_ref[...].astype(F32) + hat * g).astype(BF16)
    gg = dy * g
    go_ref[...] = (inv * (gg - hat * jnp.mean(gg * hat, axis=-1, keepdims=True))).astype(BF16)

    @pl.when(pl.program_id(0) == 0)
    def _():
        dg_ref[...] = jnp.zeros_like(dg_ref)

    dg_ref[...] += jnp.sum((dy * hat).reshape(RB // 8, 8, -1), axis=0)


def pre_kernel(p_ref, r_ref, h_ref, dy_ref, g_ref, *rest):
    dh_ref, dg_ref = rest[-2:]
    ga = p_ref[...].astype(F32) + r_ref[...].astype(F32)
    h = h_ref[...].astype(F32)
    inv = lax.rsqrt(jnp.mean(h * h, axis=-1, keepdims=True) + NORM_EPS)
    hat = h * inv
    gh = ga * g_ref[...]
    dh_ref[...] = (dy_ref[...].astype(F32) + inv * (gh - hat * jnp.mean(gh * hat, axis=-1, keepdims=True))).astype(BF16)

    @pl.when(pl.program_id(0) == 0)
    def _():
        dg_ref[...] = jnp.zeros_like(dg_ref)

    dg_ref[...] += jnp.sum((ga * hat).reshape(RB // 8, 8, -1), axis=0)


def norm_call(kernel, part, peer, hidden, d_out, g, r0, buf, extra):
    M, D = part.shape
    n = M // RB
    loc = pl.BlockSpec((RB, D), lambda i: (i, 0))
    row = pl.BlockSpec((RB, D), lambda i: (r0 // RB + i, 0))
    in_specs = [loc, loc, row, row, pl.BlockSpec((1, D), lambda i: (0, 0))]
    args = [part, peer, hidden, d_out, g.reshape(1, D)]
    aliases = {}
    if buf is not None:
        aliases = {len(args): 0}
        args.append(buf)
        in_specs.append(pl.BlockSpec(memory_space=pl.ANY))
    out_specs = [row] + ([loc] if extra else []) + [pl.BlockSpec((8, D), lambda i: (0, 0))]
    out_shape = [jax.ShapeDtypeStruct(hidden.shape, BF16)]
    if extra:
        out_shape.append(jax.ShapeDtypeStruct((M, D), BF16))
    out_shape.append(jax.ShapeDtypeStruct((8, D), F32))
    return pl.pallas_call(
        kernel, grid=(n,), in_specs=in_specs, out_specs=out_specs, out_shape=out_shape, input_output_aliases=aliases,
        compiler_params=pltpu.CompilerParams(dimension_semantics=("arbitrary",), vmem_limit_bytes=VMEM_LIMIT),
        cost_estimate=pl.CostEstimate(flops=M * D * 2000, bytes_accessed=M * D * 12, transcendentals=0),
    )(*args)


def a_kernel(h_ref, g_ref, a_ref):
    h = h_ref[...].astype(F32)
    inv = lax.rsqrt(jnp.mean(h * h, axis=-1, keepdims=True) + NORM_EPS)
    a_ref[...] = (h * inv * g_ref[...]).astype(BF16)


def a_call(hidden, g):
    M, D = hidden.shape
    row = pl.BlockSpec((RB, D), lambda i: (i, 0))
    return pl.pallas_call(
        a_kernel, grid=(M // RB,), in_specs=[row, pl.BlockSpec((1, D), lambda i: (0, 0))], out_specs=row,
        out_shape=jax.ShapeDtypeStruct((M, D), BF16),
        compiler_params=pltpu.CompilerParams(dimension_semantics=("arbitrary",)),
        cost_estimate=pl.CostEstimate(flops=M * D * 1000, bytes_accessed=M * D * 4, transcendentals=0),
        name="a_norm",
    )(hidden, g.reshape(1, D))


def solution(mesh):
    core_perm = [(0, 1), (1, 0), (2, 3), (3, 2)]
    x_perm = [(0, 2), (2, 0), (1, 3), (3, 1)]
    tp_perm = [(0, 1), (1, 0)]

    def to_core(v):
        return lax.ppermute(v, 'cp', core_perm)

    def to_x(v):
        return lax.ppermute(v, 'cp', x_perm)

    def to_tp(v):
        return lax.ppermute(v, 'tp', tp_perm)

    def device_fn(hidden, g_pre, w_q, w_k, w_v, w_o, g_post, d_out):
        tokens, D = hidden.shape
        T = 4 * tokens
        me = lax.axis_index('cp')
        tp = lax.axis_index('tp')
        core, xi = me % 2, me // 2
        HL = w_q.shape[1] // 2
        KL = w_k.shape[1] // 2
        cos, sin = lax.optimization_barrier(rope_tables(T))
        base = jnp.stack([xi, core, me, me ^ 1]).astype(jnp.int32)

        def two_way(blk, n):
            r1 = to_x(lax.dynamic_slice_in_dim(blk, tp * n, n, 0))
            r3 = to_x(blk[2 * n:])
            r2 = to_tp(r1)
            return [r1, r2, r3], [tp * n, (1 - tp) * n, 2 * n]

        a_loc = a_call(hidden, g_pre)
        a_x, a_off = two_way(a_loc, 176)
        a_p = to_core(a_loc)
        a_xp = [to_core(r) for r in a_x]
        wo2 = w_o.reshape(-1, D)
        N = (HL + 2 * KL) * HEAD
        w_own = w_layout(core, w_q, w_k, w_v, 512)
        w_oth = [w_layout(1 - core, w_q, w_k, w_v, 384, p, 2) for p in range(2)]
        qkv_args = (w_own, "qkv", (cos, sin), 2, [core, 1 - core], tokens, 0, N)
        bufs = gather_matmul(xi, core, [(0, 0), (1, 0)], [a_loc, a_p], *qkv_args)
        places = [(0, o) for o in a_off] + [(1, o) for o in a_off]
        qkv, a_all = gather_matmul(1 - xi, core, places, a_x + a_xp, *qkv_args, bufs=bufs)
        qkv = qkv.reshape(T, N)
        a_all = a_all.reshape(T, D)

        ctx, lse = attn_fwd(qkv, KL, HL)
        ctx_pr = to_core(lax.dynamic_slice_in_dim(ctx, (me ^ 1) * tokens, tokens, 0))
        sizes = (128, 128, 128, 128)
        starts = [sum(sizes[:c]) for c in range(len(sizes))]
        o_parts, o_peers = [], []
        for c, M in enumerate(sizes):
            op = o_rows(base, ctx, ctx_pr, wo2, starts[c], M, 1536)
            o_parts.append(op)
            o_peers.append(to_tp(op))
        ctx_p = to_core(ctx)

        y_blk, gos, dgp = None, [], []
        for c in range(len(sizes)):
            y_blk, go, dg_ = norm_call(post_kernel, o_parts[c], o_peers[c], hidden, d_out, g_post, starts[c], y_blk, True)
            gos.append(go)
            dgp.append(dg_)

        gx = [to_x(g) for g in gos]
        gp = [to_core(g) for g in gos]
        gxp = [to_core(g) for g in gx]
        HN = HL * HEAD
        RE, RL = starts[-1], sizes[-1]
        places = [(c, o) for c in range(2) for o in starts[:-1]]
        pair = [core, 1 - core]
        bufs = gather_matmul(xi, core, places, gos[:-1] + gp[:-1], wo2, "nt", (), 2, pair, RE, 0, HN)
        bufs = gather_matmul(1 - xi, core, places, gx[:-1] + gxp[:-1], wo2, "nt", (), 2, pair, RE, 0, HN, bufs=bufs)
        places = [(0, rel * RL) for rel in range(4)]
        dctx, go_all = gather_matmul(0, core, places, [gos[-1], gp[-1], gx[-1], gxp[-1]], wo2, "nt", (), 1, [me ^ rel for rel in range(4)],
                                     RL, RE, HN, bufs=bufs)
        dctx = dctx.reshape(T, HN)
        go_all = go_all.reshape(T, D)

        dqkv = attn_bwd(qkv, KL, HL, dctx, ctx, lse, cos, sin)
        dqkv_pr = [to_core(lax.dynamic_slice_in_dim(g, (me ^ 1) * tokens, tokens, 0)) for g in dqkv]
        dqkv_p = [to_core(g) for g in dqkv]
        ga_part = ga_rows(base, dqkv, dqkv_pr, (w_own, *w_oth), tokens, 384)
        ga_peer = to_tp(ga_part)

        dwo = dwo_proj(base, ctx, ctx_p, go_all, 512).reshape(w_o.shape)
        dwq, dwk, dwv = dw_proj(base, a_all, [g for pair in zip(dqkv, dqkv_p) for g in pair], 512)

        grad_h, dgr = norm_call(pre_kernel, ga_part, ga_peer, hidden, d_out, g_pre, 0, None, False)
        dg = jnp.stack([jnp.sum(dgr, axis=0), jnp.sum(sum(dgp), axis=0)])
        dg = dg + to_core(dg)
        dg = dg + to_x(dg)
        return y_blk, grad_h, dg[0], dwq, dwk, dwv, dwo, dg[1]


    row_spec = P('cp', None)
    head_spec = P(None, 'tp', None)
    out_head_spec = P('tp', None, None)
    return jax.shard_map(device_fn, mesh=mesh, in_specs=(row_spec, P(), head_spec, head_spec, head_spec, out_head_spec, P(), row_spec), out_specs=(row_spec, row_spec, P(), head_spec, head_spec, head_spec, out_head_spec, P()), check_vma=False)
```

```python
import functools

import jax
import jax.numpy as jnp
from jax import lax
from jax.experimental import pallas as pl
from jax.experimental.pallas import tpu as pltpu
from jax.sharding import PartitionSpec as P


SOFT_CAP = 30.0
NORM_EPS = 1e-5
ROPE_THETA = 10000.0
HEAD = 128
LOG2E = 1.4426950408889634
F32 = jnp.float32
BF16 = jnp.bfloat16

NT = (((1,), (1,)), ((), ()))
NN = (((1,), (0,)), ((), ()))


def dotf(a, b, dims):
    return lax.dot_general(a, b, dims, preferred_element_type=F32)


def rope_tables(length):
    half = HEAD // 2
    inv_freq = ROPE_THETA ** (-jnp.arange(half, dtype=F32) * 2.0 / HEAD)
    ang = jnp.arange(length).astype(F32)[:, None] * inv_freq[None, :]
    cos, sin = jnp.cos(ang), jnp.sin(ang)
    return jnp.concatenate([cos, cos], axis=-1), jnp.concatenate([-sin, sin], axis=-1)


QT = 512
SB = 256


def attn_fwd_kernel(q_ref, k_ref, v_ref, ctx_ref, lse_ref, q_s, acc_ref, sum_ref, *, k1, k2):
    i = pl.program_id(1)
    nt = QT // SB
    for t in range(nt):
        rows = slice(t * SB, (t + 1) * SB)
        q_s[t, :SB] = q_ref[rows, :HEAD]
        q_s[t, SB:] = q_ref[rows, HEAD:]
    acc_ref[...] = jnp.zeros_like(acc_ref)
    sum_ref[...] = jnp.zeros_like(sum_ref)

    def chunk(t, row0, mask):
        k = k_ref[pl.ds(row0, SB), :]
        v = v_ref[pl.ds(row0, SB), :]
        s = dotf(q_s[t], k, NT)
        p = jnp.exp2(jnp.tanh(s * k1) * k2)
        if mask is not None:
            p = jnp.where(mask, p, 0.0)
        part = p[:, :128]
        for c in range(1, SB // 128):
            part = part + p[:, c * 128:(c + 1) * 128]
        return part, dotf(p.astype(BF16), v, NN)

    def full(j, carry):
        for t in range(nt):
            ps = [chunk(t, pl.multiple_of(j * QT + m * SB, SB), None) for m in range(nt)]
            sum_ref[t] += ps[0][0] + ps[1][0]
            acc_ref[t] += ps[0][1] + ps[1][1]
        return carry

    lax.fori_loop(0, i, full, 0)

    rows = lax.broadcasted_iota(jnp.int32, (2 * SB, SB), 0) % SB
    cols = lax.broadcasted_iota(jnp.int32, (2 * SB, SB), 1)
    mask = rows >= cols
    for t in range(nt):
        ps = [chunk(t, pl.multiple_of(i * QT + m * SB, SB), mask if m == t else None) for m in range(t + 1)]
        tot, acc = sum_ref[t], acc_ref[t]
        for p in ps:
            tot, acc = tot + p[0], acc + p[1]
        total = jnp.sum(tot, axis=1, keepdims=True)
        ctx = (acc / total).astype(BF16)
        r = slice(t * SB, (t + 1) * SB)
        ctx_ref[r, :HEAD] = ctx[:SB]
        ctx_ref[r, HEAD:] = ctx[SB:]
        lse = jnp.broadcast_to(jnp.log2(total), (2 * SB, 128)).T
        lse_ref[0, 0:1, r] = lse[0:1, :SB]
        lse_ref[0, 1:2, r] = lse[0:1, SB:]


def attn_fwd(qkv, kvh, nq):
    T = qkv.shape[0]
    scale = HEAD ** -0.5
    return pl.pallas_call(
        functools.partial(attn_fwd_kernel, k1=scale / SOFT_CAP, k2=SOFT_CAP * LOG2E),
        grid=(kvh, T // QT),
        in_specs=[
            pl.BlockSpec((QT, 2 * HEAD), lambda h, i: (i, h)),
            pl.BlockSpec((T, HEAD), lambda h, i: (0, nq + h)),
            pl.BlockSpec((T, HEAD), lambda h, i: (0, nq + kvh + h)),
        ],
        out_specs=[
            pl.BlockSpec((QT, 2 * HEAD), lambda h, i: (i, h)),
            pl.BlockSpec((1, 2, QT), lambda h, i: (h, 0, i)),
        ],
        out_shape=[
            jax.ShapeDtypeStruct((T, nq * HEAD), BF16),
            jax.ShapeDtypeStruct((kvh, 2, T), F32),
        ],
        scratch_shapes=[
            pltpu.VMEM((QT // SB, 2 * SB, HEAD), BF16),
            pltpu.VMEM((QT // SB, 2 * SB, HEAD), F32),
            pltpu.VMEM((QT // SB, 2 * SB, 128), F32),
        ],
        compiler_params=pltpu.CompilerParams(dimension_semantics=("arbitrary", "arbitrary")),
        cost_estimate=pl.CostEstimate(flops=int(2 * 2 * T * T * HEAD * kvh * 2), bytes_accessed=2 * qkv.size * 2, transcendentals=0),
        name="attn_fwd",
    )(qkv, qkv, qkv)


BQ = 256
BK = 512


def attn_bwd_kernel(q_ref, k_ref, v_ref, do_ref, ctx_ref, lse_ref, cos_ref, sin_ref, dq_ref, dk_ref, dv_ref,
                    dqa_ref, dka_ref, dva_ref, dd_ref, kt_ref, *, k1, k2, scale):
    J = pl.program_id(1)
    nq = q_ref.shape[0] // BQ
    r = BK // BQ

    @pl.when(J == 0)
    def _():
        dqa_ref[...] = jnp.zeros_like(dqa_ref)
        for g in range(2):
            for i in range(nq):
                sl = slice(i * BQ, (i + 1) * BQ)
                prod = do_ref[sl, g * HEAD:(g + 1) * HEAD].astype(F32) * ctx_ref[sl, g * HEAD:(g + 1) * HEAD].astype(F32)
                dd_ref[g, 0:1, sl] = jnp.sum(prod.T, axis=0, keepdims=True)

    dka_ref[...] = jnp.zeros_like(dka_ref)
    dva_ref[...] = jnp.zeros_like(dva_ref)
    k = k_ref[...]
    v = v_ref[...]
    kt_ref[...] = k.T

    def tile(i, mask):
        row0 = pl.multiple_of(i * BQ, BQ)
        rs = pl.ds(row0, BQ)
        dks, dvs = [], []
        for g in range(2):
            q = q_ref[rs, g * HEAD:(g + 1) * HEAD]
            do = do_ref[rs, g * HEAD:(g + 1) * HEAD]
            lse = lse_ref[0, g:g + 1, rs]
            dd = dd_ref[g, 0:1, rs]
            s = dotf(k, q, NT)
            u = jnp.tanh(s * k1)
            p = jnp.exp2(u * k2 - lse)
            if mask is not None:
                p = jnp.where(mask, p, 0.0)
            dp = dotf(v, do, NT)
            ds = (p * (dp - dd) * (1.0 - u * u)).astype(BF16)
            dvs.append(dotf(p.astype(BF16), do, NN))
            dks.append(dotf(ds, q, NN))
            dqa_ref[g, :, rs] += dotf(kt_ref[...], ds, NN)
        dva_ref[...] += dvs[0] + dvs[1]
        dka_ref[...] += dks[0] + dks[1]

    kpos = lax.broadcasted_iota(jnp.int32, (BK, BQ), 0)
    qpos = lax.broadcasted_iota(jnp.int32, (BK, BQ), 1)
    for m in range(r):
        tile(J * r + m, qpos + m * BQ >= kpos)

    def body(j, carry):
        for m in range(r):
            tile(j * r + m, None)
        return carry

    lax.fori_loop(J + 1, nq // r, body, 0)

    krow = pl.ds(pl.multiple_of(J * BK, BK), BK)

    def unrope(g, cos, sin):
        return (g * cos - pltpu.roll(g, HEAD // 2, 1) * sin) * scale

    dk_ref[...] = unrope(dka_ref[...], cos_ref[krow, :], sin_ref[krow, :]).astype(BF16)
    dv_ref[...] = dva_ref[...].astype(BF16)
    for g in range(2):
        dq_ref[:, g * HEAD:(g + 1) * HEAD] = unrope(dqa_ref[g, :, krow].T, cos_ref[krow, :], sin_ref[krow, :]).astype(BF16)


def attn_bwd(qkv, kvh, nq, do, ctx, lse, cos, sin):
    T = qkv.shape[0]
    scale = HEAD ** -0.5
    full2 = pl.BlockSpec((T, 2 * HEAD), lambda h, j: (0, h))
    kblk = pl.BlockSpec((BK, HEAD), lambda h, j: (j, h))
    tab = pl.BlockSpec((T, HEAD), lambda h, j: (0, 0))
    return pl.pallas_call(
        functools.partial(attn_bwd_kernel, k1=scale / SOFT_CAP, k2=SOFT_CAP * LOG2E, scale=scale),
        grid=(kvh, T // BK),
        in_specs=[full2, pl.BlockSpec((BK, HEAD), lambda h, j: (j, nq + h)), pl.BlockSpec((BK, HEAD), lambda h, j: (j, nq + kvh + h)), full2, full2, pl.BlockSpec((1, 2, T), lambda h, j: (h, 0, 0)), tab, tab],
        out_specs=[pl.BlockSpec((BK, 2 * HEAD), lambda h, j: (j, h)), kblk, kblk],
        out_shape=[
            jax.ShapeDtypeStruct((T, nq * HEAD), BF16),
            jax.ShapeDtypeStruct((T, kvh * HEAD), BF16),
            jax.ShapeDtypeStruct((T, kvh * HEAD), BF16),
        ],
        scratch_shapes=[
            pltpu.VMEM((2, HEAD, T), F32),
            pltpu.VMEM((BK, HEAD), F32),
            pltpu.VMEM((BK, HEAD), F32),
            pltpu.VMEM((2, 1, T), F32),
            pltpu.VMEM((HEAD, BK), BF16),
        ],
        compiler_params=pltpu.CompilerParams(dimension_semantics=("arbitrary", "arbitrary")),
        cost_estimate=pl.CostEstimate(flops=int(5 * 2 * T * T * HEAD * kvh), bytes_accessed=3 * qkv.size * 2, transcendentals=0),
        name="attn_bwd",
    )(qkv, qkv, qkv, do, ctx, lse, cos, sin)


VMEM_LIMIT = 64_000_000


def gmm_kernel(sc_ref, *refs, layout, mode, R, r0, B, n_rope, aliased):
    np_ = len(layout)
    pieces = refs[:np_]
    w_ref = refs[np_]
    rest = refs[np_ + 1:]
    if mode == "qkv":
        cos_ref, sin_ref = rest[:2]
        rest = rest[2:]
    if aliased:
        rest = rest[2:]
    out_ref, all_ref, x_ref, sem_in, sem_out = rest
    n = pl.program_id(0)
    last = pl.num_programs(0) - 1
    S, M, _ = x_ref.shape
    per = M // R

    def cp_in(p):
        slot, rows = layout[p]
        off = pl.multiple_of(sc_ref[2 + B + p], 16)
        return pltpu.make_async_copy(pieces[p], x_ref.at[slot, pl.ds(off, rows)], sem_in.at[p])

    def cp_out(s, j):
        return pltpu.make_async_copy(
            x_ref.at[s, pl.ds(j * R, R)], all_ref.at[sc_ref[0] * B + sc_ref[2 + s * per + j], pl.ds(r0, R)], sem_out.at[s * per + j])

    @pl.when(n == 0)
    def _():
        for p in range(np_):
            cp_in(p).start()

    for s in range(S):
        @pl.when(n == 0)
        def _(s=s):
            for p in range(np_):
                if layout[p][0] == s:
                    cp_in(p).wait()
            for j in range(per):
                cp_out(s, j).start()

        res = dotf(x_ref[s], w_ref[...], NN if mode == "qkv" else NT)
        for j in range(per):
            dst = sc_ref[2 + s * per + j]
            rows = res[j * R:(j + 1) * R]
            if mode == "qkv":
                c = jnp.where(n < n_rope, cos_ref[dst], 1.0)
                t = jnp.where(n < n_rope, sin_ref[dst], 0.0)
                for h in range(rows.shape[1] // HEAD):
                    r = rows[:, h * HEAD:(h + 1) * HEAD]
                    out_ref[dst, :, h * HEAD:(h + 1) * HEAD] = (r * c + pltpu.roll(r, HEAD // 2, 1) * t).astype(BF16)
            else:
                out_ref[dst] = rows.astype(BF16)

    @pl.when(n == last)
    def _():
        for s in range(S):
            for j in range(per):
                cp_out(s, j).wait()


def gather_matmul(chip, core, places, pieces, w, mode, tabs, S, dsts, R, r0, N, bufs=None):
    D = pieces[0].shape[1]
    tokens, nb = 512, 512
    B = len(dsts)
    scal = jnp.stack([jnp.asarray(v, jnp.int32) for v in [chip, core] + list(dsts) + [o for _, o in places]])
    layout = tuple((slot, p.shape[0]) for (slot, _), p in zip(places, pieces))
    anyspec = pl.BlockSpec(memory_space=pl.ANY)
    if mode == "qkv":
        w_specs = [pl.BlockSpec((D, nb), lambda n, s: (0, n))]
        w_specs += [pl.BlockSpec((B, R, HEAD), lambda n, s: (s[0], 0, 0), pipeline_mode=pl.Buffered(1))] * 2
    else:
        w_specs = [pl.BlockSpec((nb, D), lambda n, s: (s[1] * (N // nb) + n, 0))]
    in_specs = [anyspec] * len(pieces) + w_specs
    args = list(pieces) + [w] + [t.reshape(4, tokens, HEAD) for t in tabs]
    aliases = {}
    if bufs is not None:
        aliases = {1 + len(args): 0, 2 + len(args): 1}
        in_specs += [anyspec, anyspec]
        args += list(bufs)
    return pl.pallas_call(
        functools.partial(gmm_kernel, layout=layout, mode=mode, R=R, r0=r0, B=B, n_rope=(N * 3 // 4) // nb, aliased=bufs is not None),
        grid_spec=pltpu.PrefetchScalarGridSpec(
            num_scalar_prefetch=1,
            grid=(N // nb,),
            in_specs=in_specs,
            out_specs=[pl.BlockSpec((B, R, nb), lambda n, s: (s[0], r0 // R, n)), anyspec],
            scratch_shapes=[
                pltpu.VMEM((S, B * R // S, D), BF16),
                pltpu.SemaphoreType.DMA((len(pieces),)),
                pltpu.SemaphoreType.DMA((B,)),
            ],
        ),
        out_shape=[jax.ShapeDtypeStruct((4, tokens, N), BF16), jax.ShapeDtypeStruct((4, tokens, D), BF16)],
        input_output_aliases=aliases,
        compiler_params=pltpu.CompilerParams(dimension_semantics=("arbitrary",), vmem_limit_bytes=VMEM_LIMIT),
        cost_estimate=pl.CostEstimate(flops=2 * B * R * D * N, bytes_accessed=B * R * D * 4 + N * D * 2, transcendentals=0),
    )(scal, *args)


def w_kernel(c_ref, wq_ref, wk_ref, wv_ref, *rest):
    out_ref, s_ref = rest[-2:]
    nq, n = wq_ref.shape[1] * HEAD, s_ref.shape[2] // 2
    out_ref[:, :nq] = wq_ref[...].reshape(-1, nq)
    half = pl.ds(pl.multiple_of(c_ref[0] * n, n), n)
    for j, ref in enumerate((wk_ref, wv_ref)):
        s_ref[j] = ref[...].reshape(-1, 2 * n)
        out_ref[:, nq + j * n:nq + (j + 1) * n] = s_ref[j, :, half]


def w_layout(c, w_q, w_k, w_v, db, i0=0, n_blocks=None, buf=None):
    D, hb = w_k.shape[:2]
    nq, n = w_q.shape[1] // 2, hb // 2
    N = (nq + 2 * n) * HEAD
    steps = D // db if n_blocks is None else n_blocks
    in_specs = [pl.BlockSpec((db, nq, HEAD), lambda i, s: (i0 + i, s[0], 0))] + [pl.BlockSpec((db, hb, HEAD), lambda i, s: (i0 + i, 0, 0))] * 2
    args, aliases = [w_q, w_k, w_v], {}
    if buf is not None:
        in_specs.append(pl.BlockSpec(memory_space=pl.ANY))
        args.append(buf)
        aliases = {4: 0}
    return pl.pallas_call(
        w_kernel,
        grid_spec=pltpu.PrefetchScalarGridSpec(
            num_scalar_prefetch=1,
            grid=(steps,),
            in_specs=in_specs,
            out_specs=pl.BlockSpec((db, N), lambda i, s: (i0 + i, 0)),
            scratch_shapes=[pltpu.VMEM((2, db, hb * HEAD), BF16)],
        ),
        out_shape=jax.ShapeDtypeStruct((D, N), BF16),
        input_output_aliases=aliases,
        compiler_params=pltpu.CompilerParams(dimension_semantics=("arbitrary",), vmem_limit_bytes=VMEM_LIMIT),
        cost_estimate=pl.CostEstimate(flops=steps * db * N * 500, bytes_accessed=steps * db * N * 5, transcendentals=0),
    )(jnp.reshape(c, (1,)).astype(jnp.int32), *args)


def orow_kernel(sc_ref, c0_ref, c1_ref, w_ref, out_ref, *, r0):
    core = sc_ref[1]
    n = c0_ref.shape[1]
    rows = slice(r0, r0 + out_ref.shape[0])
    own = w_ref[pl.ds(pl.multiple_of(core * n, n), n), :]
    oth = w_ref[pl.ds(pl.multiple_of((1 - core) * n, n), n), :]
    out_ref[...] = (dotf(c0_ref[rows, :], own, NN) + dotf(c1_ref[rows, :], oth, NN)).astype(BF16)


def o_rows(scal, ctx, ctx_pr, w, r0, M, db):
    n, D = ctx.shape[1], w.shape[1]
    tokens = ctx_pr.shape[0]
    return pl.pallas_call(
        functools.partial(orow_kernel, r0=r0),
        grid_spec=pltpu.PrefetchScalarGridSpec(
            num_scalar_prefetch=1,
            grid=(D // db,),
            in_specs=[
                pl.BlockSpec((tokens, n), lambda i, s: (s[2], 0)),
                pl.BlockSpec((tokens, n), lambda i, s: (0, 0)),
                pl.BlockSpec((2 * n, db), lambda i, s: (0, i)),
            ],
            out_specs=pl.BlockSpec((M, db), lambda i, s: (0, i)),
        ),
        out_shape=jax.ShapeDtypeStruct((M, D), BF16),
        compiler_params=pltpu.CompilerParams(dimension_semantics=("arbitrary",), vmem_limit_bytes=VMEM_LIMIT),
        cost_estimate=pl.CostEstimate(flops=4 * M * D * n, bytes_accessed=w.size * 2, transcendentals=0),
    )(scal, ctx, ctx_pr, w)


def ga_kernel(sc_ref, q0, k0, v0, q1, k1, v1, w0_ref, w1_ref, out_ref):
    acc = None
    for w_ref, gs in ((w0_ref, (q0, k0, v0)), (w1_ref, (q1, k1, v1))):
        o = 0
        for g in gs:
            n = g.shape[1]
            d = dotf(g[...], w_ref[:, o:o + n], NT)
            acc = d if acc is None else acc + d
            o += n
    out_ref[...] = acc.astype(BF16)


def ga_rows(scal, own, oth, ws, M, db):
    D, N = ws[0].shape
    return pl.pallas_call(
        ga_kernel,
        grid_spec=pltpu.PrefetchScalarGridSpec(
            num_scalar_prefetch=1,
            grid=(D // db,),
            in_specs=[pl.BlockSpec((M, g.shape[1]), lambda i, s: (s[2], 0)) for g in own]
            + [pl.BlockSpec((M, g.shape[1]), lambda i, s: (0, 0)) for g in oth]
            + [pl.BlockSpec((db, N), lambda i, s: (i, 0)) for w in ws],
            out_specs=pl.BlockSpec((M, db), lambda i, s: (0, i)),
        ),
        out_shape=jax.ShapeDtypeStruct((M, D), BF16),
        compiler_params=pltpu.CompilerParams(dimension_semantics=("arbitrary",), vmem_limit_bytes=VMEM_LIMIT),
        cost_estimate=pl.CostEstimate(flops=4 * M * D * N, bytes_accessed=4 * D * N, transcendentals=0),
    )(scal, *own, *oth, *ws)


def dw_kernel(sc_ref, a_ref, q0, q1, k0, k1, v0, v1, h0_ref, h1_ref, oq_ref, ok_ref, ov_ref, oo_ref):
    db = a_ref.shape[1]
    core = sc_ref[1]
    nr = h0_ref.shape[0]
    oo_ref[pl.ds(pl.multiple_of(core * nr, nr), nr), :] = h0_ref[...]
    oo_ref[pl.ds(pl.multiple_of((1 - core) * nr, nr), nr), :] = h1_ref[...]
    at = a_ref[...].T
    for pair, out_ref in (((q0, q1), oq_ref), ((k0, k1), ok_ref), ((v0, v1), ov_ref)):
        hh = pair[0].shape[1] // HEAD
        nh = 2 * hh
        for other, g_ref in enumerate(pair):
            c = 1 - core if other else core
            res = dotf(at, g_ref[...], NN)
            for h in range(hh):
                out_ref[pl.ds(c * hh + h, db, stride=nh), :] = res[:, h * HEAD:(h + 1) * HEAD]


def dw_proj(scal, a, gs, halves, db):
    T, D = a.shape
    nhs = [2 * gs[0].shape[1] // HEAD, 2 * gs[2].shape[1] // HEAD, 2 * gs[4].shape[1] // HEAD]
    outs = pl.pallas_call(
        dw_kernel,
        grid_spec=pltpu.PrefetchScalarGridSpec(
            num_scalar_prefetch=1,
            grid=(D // db,),
            in_specs=[pl.BlockSpec((T, db), lambda i, s: (0, i))]
            + [pl.BlockSpec(g.shape, lambda i, s: (0, 0), pipeline_mode=pl.Buffered(1)) for g in gs]
            + [pl.BlockSpec((h.shape[0], db), lambda i, s: (0, i)) for h in halves],
            out_specs=[pl.BlockSpec((db * nh, HEAD), lambda i, s: (i, 0)) for nh in nhs]
            + [pl.BlockSpec((2 * halves[0].shape[0], db), lambda i, s: (0, i))],
        ),
        out_shape=[jax.ShapeDtypeStruct((D * nh, HEAD), F32) for nh in nhs] + [jax.ShapeDtypeStruct((2 * halves[0].shape[0], D), F32)],
        compiler_params=pltpu.CompilerParams(dimension_semantics=("arbitrary",), vmem_limit_bytes=VMEM_LIMIT),
        cost_estimate=pl.CostEstimate(flops=2 * T * D * sum(nhs) * HEAD, bytes_accessed=D * sum(nhs) * HEAD * 4, transcendentals=0),
        name="dw_proj",
    )(scal, a, *gs, *halves)
    return [o.reshape(D, nh, HEAD) for o, nh in zip(outs, nhs)] + [outs[3]]


def dwo_kernel(c_ref, g_ref, out_ref, t_ref):
    @pl.when(pl.program_id(0) == 0)
    def _():
        t_ref[...] = c_ref[...].T

    out_ref[...] = dotf(t_ref[...], g_ref[...], NN)


def dwo_proj(ctx, go, db):
    T, D = go.shape
    n = ctx.shape[1]
    return pl.pallas_call(
        dwo_kernel,
        grid=(D // db,),
        in_specs=[pl.BlockSpec((T, n), lambda i: (0, 0), pipeline_mode=pl.Buffered(1)), pl.BlockSpec((T, db), lambda i: (0, i))],
        out_specs=pl.BlockSpec((n, db), lambda i: (0, i)),
        scratch_shapes=[pltpu.VMEM((n, T), BF16)],
        out_shape=jax.ShapeDtypeStruct((n, D), F32),
        compiler_params=pltpu.CompilerParams(dimension_semantics=("arbitrary",), vmem_limit_bytes=VMEM_LIMIT),
        cost_estimate=pl.CostEstimate(flops=2 * T * D * n, bytes_accessed=n * D * 4, transcendentals=0),
        name="dwo_proj",
    )(ctx, go)


RB = 64


def post_kernel(p_ref, r_ref, h_ref, dy_ref, g_ref, *rest):
    y_ref, go_ref, dg_ref = rest[-3:]
    o = p_ref[...].astype(F32) + r_ref[...].astype(F32)
    inv = lax.rsqrt(jnp.mean(o * o, axis=-1, keepdims=True) + NORM_EPS)
    hat = o * inv
    g = g_ref[...]
    dy = dy_ref[...].astype(F32)
    y_ref[...] = (h_ref[...].astype(F32) + hat * g).astype(BF16)
    gg = dy * g
    go_ref[...] = (inv * (gg - hat * jnp.mean(gg * hat, axis=-1, keepdims=True))).astype(BF16)

    @pl.when(pl.program_id(0) == 0)
    def _():
        dg_ref[...] = jnp.zeros_like(dg_ref)

    dg_ref[...] += jnp.sum((dy * hat).reshape(RB // 8, 8, -1), axis=0)


def pre_kernel(p_ref, r_ref, h_ref, dy_ref, g_ref, *rest):
    dh_ref, dg_ref = rest[-2:]
    ga = p_ref[...].astype(F32) + r_ref[...].astype(F32)
    h = h_ref[...].astype(F32)
    inv = lax.rsqrt(jnp.mean(h * h, axis=-1, keepdims=True) + NORM_EPS)
    hat = h * inv
    gh = ga * g_ref[...]
    dh_ref[...] = (dy_ref[...].astype(F32) + inv * (gh - hat * jnp.mean(gh * hat, axis=-1, keepdims=True))).astype(BF16)

    @pl.when(pl.program_id(0) == 0)
    def _():
        dg_ref[...] = jnp.zeros_like(dg_ref)

    dg_ref[...] += jnp.sum((ga * hat).reshape(RB // 8, 8, -1), axis=0)


def norm_call(kernel, part, peer, hidden, d_out, g, r0, buf, extra):
    M, D = part.shape
    n = M // RB
    loc = pl.BlockSpec((RB, D), lambda i: (i, 0))
    row = pl.BlockSpec((RB, D), lambda i: (r0 // RB + i, 0))
    in_specs = [loc, loc, row, row, pl.BlockSpec((1, D), lambda i: (0, 0))]
    args = [part, peer, hidden, d_out, g.reshape(1, D)]
    aliases = {}
    if buf is not None:
        aliases = {len(args): 0}
        args.append(buf)
        in_specs.append(pl.BlockSpec(memory_space=pl.ANY))
    out_specs = [row] + ([loc] if extra else []) + [pl.BlockSpec((8, D), lambda i: (0, 0))]
    out_shape = [jax.ShapeDtypeStruct(hidden.shape, BF16)]
    if extra:
        out_shape.append(jax.ShapeDtypeStruct((M, D), BF16))
    out_shape.append(jax.ShapeDtypeStruct((8, D), F32))
    return pl.pallas_call(
        kernel, grid=(n,), in_specs=in_specs, out_specs=out_specs, out_shape=out_shape, input_output_aliases=aliases,
        compiler_params=pltpu.CompilerParams(dimension_semantics=("arbitrary",), vmem_limit_bytes=VMEM_LIMIT),
        cost_estimate=pl.CostEstimate(flops=M * D * 2000, bytes_accessed=M * D * 12, transcendentals=0),
    )(*args)


def a_kernel(h_ref, g_ref, a_ref):
    h = h_ref[...].astype(F32)
    inv = lax.rsqrt(jnp.mean(h * h, axis=-1, keepdims=True) + NORM_EPS)
    a_ref[...] = (h * inv * g_ref[...]).astype(BF16)


def a_call(hidden, g):
    M, D = hidden.shape
    row = pl.BlockSpec((RB, D), lambda i: (i, 0))
    return pl.pallas_call(
        a_kernel, grid=(M // RB,), in_specs=[row, pl.BlockSpec((1, D), lambda i: (0, 0))], out_specs=row,
        out_shape=jax.ShapeDtypeStruct((M, D), BF16),
        compiler_params=pltpu.CompilerParams(dimension_semantics=("arbitrary",)),
        cost_estimate=pl.CostEstimate(flops=M * D * 1000, bytes_accessed=M * D * 4, transcendentals=0),
        name="a_norm",
    )(hidden, g.reshape(1, D))


def solution(mesh):
    core_perm = [(0, 1), (1, 0), (2, 3), (3, 2)]
    x_perm = [(0, 2), (2, 0), (1, 3), (3, 1)]
    tp_perm = [(0, 1), (1, 0)]

    def to_core(v):
        return lax.ppermute(v, 'cp', core_perm)

    def to_x(v):
        return lax.ppermute(v, 'cp', x_perm)

    def to_tp(v):
        return lax.ppermute(v, 'tp', tp_perm)

    def device_fn(hidden, g_pre, w_q, w_k, w_v, w_o, g_post, d_out):
        tokens, D = hidden.shape
        T = 4 * tokens
        me = lax.axis_index('cp')
        tp = lax.axis_index('tp')
        core, xi = me % 2, me // 2
        HL = w_q.shape[1] // 2
        KL = w_k.shape[1] // 2
        cos, sin = lax.optimization_barrier(rope_tables(T))
        base = jnp.stack([xi, core, me, me ^ 1]).astype(jnp.int32)

        def two_way(blk, n):
            r1 = to_x(lax.dynamic_slice_in_dim(blk, tp * n, n, 0))
            r3 = to_x(blk[2 * n:])
            r2 = to_tp(r1)
            return [r1, r2, r3], [tp * n, (1 - tp) * n, 2 * n]

        a_loc = a_call(hidden, g_pre)
        a_x, a_off = two_way(a_loc, 160)
        a_p = to_core(a_loc)
        a_xp = [to_core(r) for r in a_x]
        wo2 = w_o.reshape(-1, D)
        N = (HL + 2 * KL) * HEAD
        w_own = w_layout(core, w_q, w_k, w_v, 512)
        w_oth = w_layout(1 - core, w_q, w_k, w_v, 512, 0, 4)
        w_oth = w_layout(1 - core, w_q, w_k, w_v, 512, 4, 5, w_oth)
        qkv_args = (w_own, "qkv", (cos, sin), 2, [core, 1 - core], tokens, 0, N)
        bufs = gather_matmul(xi, core, [(0, 0), (1, 0)], [a_loc, a_p], *qkv_args)
        places = [(0, o) for o in a_off] + [(1, o) for o in a_off]
        qkv, a_all = gather_matmul(1 - xi, core, places, a_x + a_xp, *qkv_args, bufs=bufs)
        qkv = qkv.reshape(T, N)
        a_all = a_all.reshape(T, D)

        ctx, lse = attn_fwd(qkv, KL, HL)
        ctx_pr = to_core(lax.dynamic_slice_in_dim(ctx, (me ^ 1) * tokens, tokens, 0))
        sizes = (128, 128, 128, 128)
        starts = [sum(sizes[:c]) for c in range(len(sizes))]
        o_parts, o_peers = [], []
        for c, M in enumerate(sizes):
            op = o_rows(base, ctx, ctx_pr, wo2, starts[c], M, 1536)
            o_parts.append(op)
            o_peers.append(to_tp(op))

        y_blk, gos, dgp = None, [], []
        for c in range(len(sizes)):
            y_blk, go, dg_ = norm_call(post_kernel, o_parts[c], o_peers[c], hidden, d_out, g_post, starts[c], y_blk, True)
            gos.append(go)
            dgp.append(dg_)

        gx = [to_x(g) for g in gos]
        gp = [to_core(g) for g in gos]
        gxp = [to_core(g) for g in gx]
        HN = HL * HEAD
        RE, RL = starts[-1], sizes[-1]
        places = [(c, o) for c in range(2) for o in starts[:-1]]
        pair = [core, 1 - core]
        bufs = gather_matmul(xi, core, places, gos[:-1] + gp[:-1], wo2, "nt", (), 2, pair, RE, 0, HN)
        bufs = gather_matmul(1 - xi, core, places, gx[:-1] + gxp[:-1], wo2, "nt", (), 2, pair, RE, 0, HN, bufs=bufs)
        places = [(0, rel * RL) for rel in range(4)]
        dctx, go_all = gather_matmul(0, core, places, [gos[-1], gp[-1], gx[-1], gxp[-1]], wo2, "nt", (), 1, [me ^ rel for rel in range(4)],
                                     RL, RE, HN, bufs=bufs)
        dctx = dctx.reshape(T, HN)
        go_all = go_all.reshape(T, D)

        dwo_own = dwo_proj(ctx, go_all, 512)
        dwo_peer = to_core(dwo_own)
        dqkv = attn_bwd(qkv, KL, HL, dctx, ctx, lse, cos, sin)
        dqkv_pr = [to_core(lax.dynamic_slice_in_dim(g, (me ^ 1) * tokens, tokens, 0)) for g in dqkv]
        dqkv_p = [to_core(g) for g in dqkv]
        ga_part = ga_rows(base, dqkv, dqkv_pr, (w_own, w_oth), tokens, 512)
        ga_peer = to_tp(ga_part)

        pairs = [g for pair in zip(dqkv, dqkv_p) for g in pair]
        dwq, dwk, dwv, dwo = dw_proj(base, a_all, pairs, (dwo_own, dwo_peer), 256)
        dwo = dwo.reshape(w_o.shape)

        grad_h, dgr = norm_call(pre_kernel, ga_part, ga_peer, hidden, d_out, g_pre, 0, None, False)
        dg = jnp.stack([jnp.sum(dgr, axis=0), jnp.sum(sum(dgp), axis=0)])
        dg = dg + to_core(dg)
        dg = dg + to_x(dg)
        return y_blk, grad_h, dg[0], dwq, dwk, dwv, dwo, dg[1]


    row_spec = P('cp', None)
    head_spec = P(None, 'tp', None)
    out_head_spec = P('tp', None, None)
    return jax.shard_map(device_fn, mesh=mesh, in_specs=(row_spec, P(), head_spec, head_spec, head_spec, out_head_spec, P(), row_spec), out_specs=(row_spec, row_spec, P(), head_spec, head_spec, head_spec, out_head_spec, P()), check_vma=False)
```

```python
import functools

import jax
import jax.numpy as jnp
from jax import lax
from jax.experimental import pallas as pl
from jax.experimental.pallas import tpu as pltpu
from jax.sharding import PartitionSpec as P


SOFT_CAP = 30.0
NORM_EPS = 1e-5
ROPE_THETA = 10000.0
HEAD = 128
LOG2E = 1.4426950408889634
F32 = jnp.float32
BF16 = jnp.bfloat16

NT = (((1,), (1,)), ((), ()))
NN = (((1,), (0,)), ((), ()))


def dotf(a, b, dims):
    return lax.dot_general(a, b, dims, preferred_element_type=F32)


def rope_tables(length):
    half = HEAD // 2
    inv_freq = ROPE_THETA ** (-jnp.arange(half, dtype=F32) * 2.0 / HEAD)
    ang = jnp.arange(length).astype(F32)[:, None] * inv_freq[None, :]
    cos, sin = jnp.cos(ang), jnp.sin(ang)
    return jnp.concatenate([cos, cos], axis=-1), jnp.concatenate([-sin, sin], axis=-1)


QT = 512
SB = 256


def attn_fwd_kernel(q_ref, k_ref, v_ref, ctx_ref, lse_ref, q_s, acc_ref, sum_ref, *, k1, k2):
    i = pl.program_id(1)
    nt = QT // SB
    for t in range(nt):
        rows = slice(t * SB, (t + 1) * SB)
        q_s[t, :SB] = q_ref[rows, :HEAD]
        q_s[t, SB:] = q_ref[rows, HEAD:]
    acc_ref[...] = jnp.zeros_like(acc_ref)
    sum_ref[...] = jnp.zeros_like(sum_ref)

    def chunk(t, row0, mask):
        k = k_ref[pl.ds(row0, SB), :]
        v = v_ref[pl.ds(row0, SB), :]
        s = dotf(q_s[t], k, NT)
        p = jnp.exp2(jnp.tanh(s * k1) * k2)
        if mask is not None:
            p = jnp.where(mask, p, 0.0)
        part = p[:, :128]
        for c in range(1, SB // 128):
            part = part + p[:, c * 128:(c + 1) * 128]
        return part, dotf(p.astype(BF16), v, NN)

    def full(j, carry):
        for t in range(nt):
            ps = [chunk(t, pl.multiple_of(j * QT + m * SB, SB), None) for m in range(nt)]
            sum_ref[t] += ps[0][0] + ps[1][0]
            acc_ref[t] += ps[0][1] + ps[1][1]
        return carry

    lax.fori_loop(0, i, full, 0)

    rows = lax.broadcasted_iota(jnp.int32, (2 * SB, SB), 0) % SB
    cols = lax.broadcasted_iota(jnp.int32, (2 * SB, SB), 1)
    mask = rows >= cols
    for t in range(nt):
        ps = [chunk(t, pl.multiple_of(i * QT + m * SB, SB), mask if m == t else None) for m in range(t + 1)]
        tot, acc = sum_ref[t], acc_ref[t]
        for p in ps:
            tot, acc = tot + p[0], acc + p[1]
        total = jnp.sum(tot, axis=1, keepdims=True)
        ctx = (acc / total).astype(BF16)
        r = slice(t * SB, (t + 1) * SB)
        ctx_ref[r, :HEAD] = ctx[:SB]
        ctx_ref[r, HEAD:] = ctx[SB:]
        lse = jnp.broadcast_to(jnp.log2(total), (2 * SB, 128)).T
        lse_ref[0, 0:1, r] = lse[0:1, :SB]
        lse_ref[0, 1:2, r] = lse[0:1, SB:]


def attn_fwd(qkv, kvh, nq):
    T = qkv.shape[0]
    scale = HEAD ** -0.5
    return pl.pallas_call(
        functools.partial(attn_fwd_kernel, k1=scale / SOFT_CAP, k2=SOFT_CAP * LOG2E),
        grid=(kvh, T // QT),
        in_specs=[
            pl.BlockSpec((QT, 2 * HEAD), lambda h, i: (i, h)),
            pl.BlockSpec((T, HEAD), lambda h, i: (0, nq + h)),
            pl.BlockSpec((T, HEAD), lambda h, i: (0, nq + kvh + h)),
        ],
        out_specs=[
            pl.BlockSpec((QT, 2 * HEAD), lambda h, i: (i, h)),
            pl.BlockSpec((1, 2, QT), lambda h, i: (h, 0, i)),
        ],
        out_shape=[
            jax.ShapeDtypeStruct((T, nq * HEAD), BF16),
            jax.ShapeDtypeStruct((kvh, 2, T), F32),
        ],
        scratch_shapes=[
            pltpu.VMEM((QT // SB, 2 * SB, HEAD), BF16),
            pltpu.VMEM((QT // SB, 2 * SB, HEAD), F32),
            pltpu.VMEM((QT // SB, 2 * SB, 128), F32),
        ],
        compiler_params=pltpu.CompilerParams(dimension_semantics=("arbitrary", "arbitrary")),
        cost_estimate=pl.CostEstimate(flops=int(2 * 2 * T * T * HEAD * kvh * 2), bytes_accessed=2 * qkv.size * 2, transcendentals=0),
        name="attn_fwd",
    )(qkv, qkv, qkv)


BQ = 256
BK = 512


def attn_bwd_kernel(sc_ref, q_ref, k_ref, v_ref, do_ref, ctx_ref, lse_ref, cos_ref, sin_ref, dq_ref, dk_ref, dv_ref, pq_ref, pk_ref, pv_ref,
                    dqa_ref, dka_ref, dva_ref, dd_ref, kt_ref, *, k1, k2, scale):
    J = pl.program_id(1)
    nq = q_ref.shape[0] // BQ
    r = BK // BQ

    @pl.when(J == 0)
    def _():
        dqa_ref[...] = jnp.zeros_like(dqa_ref)
        for g in range(2):
            for i in range(nq):
                sl = slice(i * BQ, (i + 1) * BQ)
                prod = do_ref[sl, g * HEAD:(g + 1) * HEAD].astype(F32) * ctx_ref[sl, g * HEAD:(g + 1) * HEAD].astype(F32)
                dd_ref[g, 0:1, sl] = jnp.sum(prod.T, axis=0, keepdims=True)

    dka_ref[...] = jnp.zeros_like(dka_ref)
    dva_ref[...] = jnp.zeros_like(dva_ref)
    k = k_ref[...]
    v = v_ref[...]
    kt_ref[...] = k.T

    def tile(i, mask):
        row0 = pl.multiple_of(i * BQ, BQ)
        rs = pl.ds(row0, BQ)
        dks, dvs = [], []
        for g in range(2):
            q = q_ref[rs, g * HEAD:(g + 1) * HEAD]
            do = do_ref[rs, g * HEAD:(g + 1) * HEAD]
            lse = lse_ref[0, g:g + 1, rs]
            dd = dd_ref[g, 0:1, rs]
            s = dotf(k, q, NT)
            u = jnp.tanh(s * k1)
            p = jnp.exp2(u * k2 - lse)
            if mask is not None:
                p = jnp.where(mask, p, 0.0)
            dp = dotf(v, do, NT)
            ds = (p * (dp - dd) * (1.0 - u * u)).astype(BF16)
            dvs.append(dotf(p.astype(BF16), do, NN))
            dks.append(dotf(ds, q, NN))
            dqa_ref[g, :, rs] += dotf(kt_ref[...], ds, NN)
        dva_ref[...] += dvs[0] + dvs[1]
        dka_ref[...] += dks[0] + dks[1]

    kpos = lax.broadcasted_iota(jnp.int32, (BK, BQ), 0)
    qpos = lax.broadcasted_iota(jnp.int32, (BK, BQ), 1)
    for m in range(r):
        tile(J * r + m, qpos + m * BQ >= kpos)

    def body(j, carry):
        for m in range(r):
            tile(j * r + m, None)
        return carry

    lax.fori_loop(J + 1, nq // r, body, 0)

    krow = pl.ds(pl.multiple_of(J * BK, BK), BK)

    def unrope(g, cos, sin):
        return (g * cos - pltpu.roll(g, HEAD // 2, 1) * sin) * scale

    dk_ref[...] = unrope(dka_ref[...], cos_ref[krow, :], sin_ref[krow, :]).astype(BF16)
    dv_ref[...] = dva_ref[...].astype(BF16)
    for g in range(2):
        dq_ref[:, g * HEAD:(g + 1) * HEAD] = unrope(dqa_ref[g, :, krow].T, cos_ref[krow, :], sin_ref[krow, :]).astype(BF16)

    @pl.when(J == sc_ref[3])
    def _():
        pq_ref[...] = dq_ref[...]
        pk_ref[...] = dk_ref[...]
        pv_ref[...] = dv_ref[...]


def attn_bwd(scal, qkv, kvh, nq, do, ctx, lse, cos, sin):
    T = qkv.shape[0]
    scale = HEAD ** -0.5
    full2 = pl.BlockSpec((T, 2 * HEAD), lambda h, j, s: (0, h))
    kblk = pl.BlockSpec((BK, HEAD), lambda h, j, s: (j, h))
    tab = pl.BlockSpec((T, HEAD), lambda h, j, s: (0, 0))
    return pl.pallas_call(
        functools.partial(attn_bwd_kernel, k1=scale / SOFT_CAP, k2=SOFT_CAP * LOG2E, scale=scale),
        grid_spec=pltpu.PrefetchScalarGridSpec(
            num_scalar_prefetch=1,
            grid=(kvh, T // BK),
            in_specs=[full2, pl.BlockSpec((BK, HEAD), lambda h, j, s: (j, nq + h)), pl.BlockSpec((BK, HEAD), lambda h, j, s: (j, nq + kvh + h)), full2, full2, pl.BlockSpec((1, 2, T), lambda h, j, s: (h, 0, 0)), tab, tab],
            out_specs=[pl.BlockSpec((BK, 2 * HEAD), lambda h, j, s: (j, h)), kblk, kblk,
                       pl.BlockSpec((BK, 2 * HEAD), lambda h, j, s: (0, h))] + [pl.BlockSpec((BK, HEAD), lambda h, j, s: (0, h))] * 2,
            scratch_shapes=[
                pltpu.VMEM((2, HEAD, T), F32),
                pltpu.VMEM((BK, HEAD), F32),
                pltpu.VMEM((BK, HEAD), F32),
                pltpu.VMEM((2, 1, T), F32),
                pltpu.VMEM((HEAD, BK), BF16),
            ],
        ),
        out_shape=[
            jax.ShapeDtypeStruct((T, nq * HEAD), BF16),
            jax.ShapeDtypeStruct((T, kvh * HEAD), BF16),
            jax.ShapeDtypeStruct((T, kvh * HEAD), BF16),
            jax.ShapeDtypeStruct((BK, nq * HEAD), BF16),
            jax.ShapeDtypeStruct((BK, kvh * HEAD), BF16),
            jax.ShapeDtypeStruct((BK, kvh * HEAD), BF16),
        ],
        compiler_params=pltpu.CompilerParams(dimension_semantics=("arbitrary", "arbitrary")),
        cost_estimate=pl.CostEstimate(flops=int(5 * 2 * T * T * HEAD * kvh), bytes_accessed=3 * qkv.size * 2, transcendentals=0),
        name="attn_bwd",
    )(scal, qkv, qkv, qkv, do, ctx, lse, cos, sin)


VMEM_LIMIT = 64_000_000


def gmm_kernel(sc_ref, *refs, layout, mode, R, r0, B, n_rope, aliased):
    np_ = len(layout)
    pieces = refs[:np_]
    w_ref = refs[np_]
    rest = refs[np_ + 1:]
    if mode == "qkv":
        cos_ref, sin_ref = rest[:2]
        rest = rest[2:]
    if aliased:
        rest = rest[2:]
    out_ref, all_ref, x_ref, sem_in, sem_out = rest
    n = pl.program_id(0)
    last = pl.num_programs(0) - 1
    S, M, _ = x_ref.shape
    per = M // R

    def cp_in(p):
        slot, rows = layout[p]
        off = pl.multiple_of(sc_ref[2 + B + p], 16)
        return pltpu.make_async_copy(pieces[p], x_ref.at[slot, pl.ds(off, rows)], sem_in.at[p])

    def cp_out(s, j):
        return pltpu.make_async_copy(
            x_ref.at[s, pl.ds(j * R, R)], all_ref.at[sc_ref[0] * B + sc_ref[2 + s * per + j], pl.ds(r0, R)], sem_out.at[s * per + j])

    @pl.when(n == 0)
    def _():
        for p in range(np_):
            cp_in(p).start()

    for s in range(S):
        @pl.when(n == 0)
        def _(s=s):
            for p in range(np_):
                if layout[p][0] == s:
                    cp_in(p).wait()
            for j in range(per):
                cp_out(s, j).start()

        res = dotf(x_ref[s], w_ref[...], NN if mode == "qkv" else NT)
        for j in range(per):
            dst = sc_ref[2 + s * per + j]
            rows = res[j * R:(j + 1) * R]
            if mode == "qkv":
                c = jnp.where(n < n_rope, cos_ref[dst], 1.0)
                t = jnp.where(n < n_rope, sin_ref[dst], 0.0)
                for h in range(rows.shape[1] // HEAD):
                    r = rows[:, h * HEAD:(h + 1) * HEAD]
                    out_ref[dst, :, h * HEAD:(h + 1) * HEAD] = (r * c + pltpu.roll(r, HEAD // 2, 1) * t).astype(BF16)
            else:
                out_ref[dst] = rows.astype(BF16)

    @pl.when(n == last)
    def _():
        for s in range(S):
            for j in range(per):
                cp_out(s, j).wait()


def gather_matmul(chip, core, places, pieces, w, mode, tabs, S, dsts, R, r0, N, bufs=None):
    D = pieces[0].shape[1]
    tokens, nb = 512, 512
    B = len(dsts)
    scal = jnp.stack([jnp.asarray(v, jnp.int32) for v in [chip, core] + list(dsts) + [o for _, o in places]])
    layout = tuple((slot, p.shape[0]) for (slot, _), p in zip(places, pieces))
    anyspec = pl.BlockSpec(memory_space=pl.ANY)
    if mode == "qkv":
        w_specs = [pl.BlockSpec((D, nb), lambda n, s: (0, n))]
        w_specs += [pl.BlockSpec((B, R, HEAD), lambda n, s: (s[0], 0, 0), pipeline_mode=pl.Buffered(1))] * 2
    else:
        w_specs = [pl.BlockSpec((nb, D), lambda n, s: (s[1] * (N // nb) + n, 0))]
    in_specs = [anyspec] * len(pieces) + w_specs
    args = list(pieces) + [w] + [t.reshape(4, tokens, HEAD) for t in tabs]
    aliases = {}
    if bufs is not None:
        aliases = {1 + len(args): 0, 2 + len(args): 1}
        in_specs += [anyspec, anyspec]
        args += list(bufs)
    return pl.pallas_call(
        functools.partial(gmm_kernel, layout=layout, mode=mode, R=R, r0=r0, B=B, n_rope=(N * 3 // 4) // nb, aliased=bufs is not None),
        grid_spec=pltpu.PrefetchScalarGridSpec(
            num_scalar_prefetch=1,
            grid=(N // nb,),
            in_specs=in_specs,
            out_specs=[pl.BlockSpec((B, R, nb), lambda n, s: (s[0], r0 // R, n)), anyspec],
            scratch_shapes=[
                pltpu.VMEM((S, B * R // S, D), BF16),
                pltpu.SemaphoreType.DMA((len(pieces),)),
                pltpu.SemaphoreType.DMA((B,)),
            ],
        ),
        out_shape=[jax.ShapeDtypeStruct((4, tokens, N), BF16), jax.ShapeDtypeStruct((4, tokens, D), BF16)],
        input_output_aliases=aliases,
        compiler_params=pltpu.CompilerParams(dimension_semantics=("arbitrary",), vmem_limit_bytes=VMEM_LIMIT),
        cost_estimate=pl.CostEstimate(flops=2 * B * R * D * N, bytes_accessed=B * R * D * 4 + N * D * 2, transcendentals=0),
    )(scal, *args)


def w_kernel(c_ref, wq_ref, wk_ref, wv_ref, *rest):
    out_ref, s_ref = rest[-2:]
    nq, n = wq_ref.shape[1] * HEAD, s_ref.shape[2] // 2
    out_ref[:, :nq] = wq_ref[...].reshape(-1, nq)
    half = pl.ds(pl.multiple_of(c_ref[0] * n, n), n)
    for j, ref in enumerate((wk_ref, wv_ref)):
        s_ref[j] = ref[...].reshape(-1, 2 * n)
        out_ref[:, nq + j * n:nq + (j + 1) * n] = s_ref[j, :, half]


def w_layout(c, w_q, w_k, w_v, db, i0=0, n_blocks=None, buf=None):
    D, hb = w_k.shape[:2]
    nq, n = w_q.shape[1] // 2, hb // 2
    N = (nq + 2 * n) * HEAD
    steps = D // db if n_blocks is None else n_blocks
    in_specs = [pl.BlockSpec((db, nq, HEAD), lambda i, s: (i0 + i, s[0], 0))] + [pl.BlockSpec((db, hb, HEAD), lambda i, s: (i0 + i, 0, 0))] * 2
    args, aliases = [w_q, w_k, w_v], {}
    if buf is not None:
        in_specs.append(pl.BlockSpec(memory_space=pl.ANY))
        args.append(buf)
        aliases = {4: 0}
    return pl.pallas_call(
        w_kernel,
        grid_spec=pltpu.PrefetchScalarGridSpec(
            num_scalar_prefetch=1,
            grid=(steps,),
            in_specs=in_specs,
            out_specs=pl.BlockSpec((db, N), lambda i, s: (i0 + i, 0)),
            scratch_shapes=[pltpu.VMEM((2, db, hb * HEAD), BF16)],
        ),
        out_shape=jax.ShapeDtypeStruct((D, N), BF16),
        input_output_aliases=aliases,
        compiler_params=pltpu.CompilerParams(dimension_semantics=("arbitrary",), vmem_limit_bytes=VMEM_LIMIT),
        cost_estimate=pl.CostEstimate(flops=steps * db * N * 500, bytes_accessed=steps * db * N * 5, transcendentals=0),
    )(jnp.reshape(c, (1,)).astype(jnp.int32), *args)


def orow_kernel(sc_ref, c0_ref, c1_ref, w_ref, out_ref, *, r0):
    core = sc_ref[1]
    n = c0_ref.shape[1]
    rows = slice(r0, r0 + out_ref.shape[0])
    own = w_ref[pl.ds(pl.multiple_of(core * n, n), n), :]
    oth = w_ref[pl.ds(pl.multiple_of((1 - core) * n, n), n), :]
    out_ref[...] = (dotf(c0_ref[rows, :], own, NN) + dotf(c1_ref[rows, :], oth, NN)).astype(BF16)


def o_rows(scal, ctx, ctx_pr, w, r0, M, db):
    n, D = ctx.shape[1], w.shape[1]
    tokens = ctx_pr.shape[0]
    return pl.pallas_call(
        functools.partial(orow_kernel, r0=r0),
        grid_spec=pltpu.PrefetchScalarGridSpec(
            num_scalar_prefetch=1,
            grid=(D // db,),
            in_specs=[
                pl.BlockSpec((tokens, n), lambda i, s: (s[2], 0)),
                pl.BlockSpec((tokens, n), lambda i, s: (0, 0)),
                pl.BlockSpec((2 * n, db), lambda i, s: (0, i)),
            ],
            out_specs=pl.BlockSpec((M, db), lambda i, s: (0, i)),
        ),
        out_shape=jax.ShapeDtypeStruct((M, D), BF16),
        compiler_params=pltpu.CompilerParams(dimension_semantics=("arbitrary",), vmem_limit_bytes=VMEM_LIMIT),
        cost_estimate=pl.CostEstimate(flops=4 * M * D * n, bytes_accessed=w.size * 2, transcendentals=0),
    )(scal, ctx, ctx_pr, w)


def ga_kernel(sc_ref, q0, k0, v0, q1, k1, v1, w0_ref, w1_ref, out_ref):
    acc = None
    for w_ref, gs in ((w0_ref, (q0, k0, v0)), (w1_ref, (q1, k1, v1))):
        o = 0
        for g in gs:
            n = g.shape[1]
            d = dotf(g[...], w_ref[:, o:o + n], NT)
            acc = d if acc is None else acc + d
            o += n
    out_ref[...] = acc.astype(BF16)


def ga_rows(scal, own, oth, ws, M, db):
    D, N = ws[0].shape
    return pl.pallas_call(
        ga_kernel,
        grid_spec=pltpu.PrefetchScalarGridSpec(
            num_scalar_prefetch=1,
            grid=(D // db,),
            in_specs=[pl.BlockSpec((M, g.shape[1]), lambda i, s: (s[2], 0)) for g in own]
            + [pl.BlockSpec((M, g.shape[1]), lambda i, s: (0, 0)) for g in oth]
            + [pl.BlockSpec((db, N), lambda i, s: (i, 0)) for w in ws],
            out_specs=pl.BlockSpec((M, db), lambda i, s: (0, i)),
        ),
        out_shape=jax.ShapeDtypeStruct((M, D), BF16),
        compiler_params=pltpu.CompilerParams(dimension_semantics=("arbitrary",), vmem_limit_bytes=VMEM_LIMIT),
        cost_estimate=pl.CostEstimate(flops=4 * M * D * N, bytes_accessed=4 * D * N, transcendentals=0),
    )(scal, *own, *oth, *ws)


def dw_kernel(sc_ref, a_ref, q0, q1, k0, k1, v0, v1, h0_ref, h1_ref, oq_ref, ok_ref, ov_ref, oo_ref):
    db = a_ref.shape[1]
    core = sc_ref[1]
    nr = h0_ref.shape[0]
    oo_ref[pl.ds(pl.multiple_of(core * nr, nr), nr), :] = h0_ref[...]
    oo_ref[pl.ds(pl.multiple_of((1 - core) * nr, nr), nr), :] = h1_ref[...]
    at = a_ref[...].T
    for pair, out_ref in (((q0, q1), oq_ref), ((k0, k1), ok_ref), ((v0, v1), ov_ref)):
        hh = pair[0].shape[1] // HEAD
        nh = 2 * hh
        for other, g_ref in enumerate(pair):
            c = 1 - core if other else core
            res = dotf(at, g_ref[...], NN)
            for h in range(hh):
                out_ref[pl.ds(c * hh + h, db, stride=nh), :] = res[:, h * HEAD:(h + 1) * HEAD]


def dw_proj(scal, a, gs, halves, db):
    T, D = a.shape
    nhs = [2 * gs[0].shape[1] // HEAD, 2 * gs[2].shape[1] // HEAD, 2 * gs[4].shape[1] // HEAD]
    outs = pl.pallas_call(
        dw_kernel,
        grid_spec=pltpu.PrefetchScalarGridSpec(
            num_scalar_prefetch=1,
            grid=(D // db,),
            in_specs=[pl.BlockSpec((T, db), lambda i, s: (0, i))]
            + [pl.BlockSpec(g.shape, lambda i, s: (0, 0), pipeline_mode=pl.Buffered(1)) for g in gs]
            + [pl.BlockSpec((h.shape[0], db), lambda i, s: (0, i)) for h in halves],
            out_specs=[pl.BlockSpec((db * nh, HEAD), lambda i, s: (i, 0)) for nh in nhs]
            + [pl.BlockSpec((2 * halves[0].shape[0], db), lambda i, s: (0, i))],
        ),
        out_shape=[jax.ShapeDtypeStruct((D * nh, HEAD), F32) for nh in nhs] + [jax.ShapeDtypeStruct((2 * halves[0].shape[0], D), F32)],
        compiler_params=pltpu.CompilerParams(dimension_semantics=("arbitrary",), vmem_limit_bytes=VMEM_LIMIT),
        cost_estimate=pl.CostEstimate(flops=2 * T * D * sum(nhs) * HEAD, bytes_accessed=D * sum(nhs) * HEAD * 4, transcendentals=0),
        name="dw_proj",
    )(scal, a, *gs, *halves)
    return [o.reshape(D, nh, HEAD) for o, nh in zip(outs, nhs)] + [outs[3]]


def dwo_kernel(c_ref, g_ref, out_ref, t_ref):
    @pl.when(pl.program_id(0) == 0)
    def _():
        t_ref[...] = c_ref[...].T

    out_ref[...] = dotf(t_ref[...], g_ref[...], NN)


def dwo_proj(ctx, go, db):
    T, D = go.shape
    n = ctx.shape[1]
    return pl.pallas_call(
        dwo_kernel,
        grid=(D // db,),
        in_specs=[pl.BlockSpec((T, n), lambda i: (0, 0), pipeline_mode=pl.Buffered(1)), pl.BlockSpec((T, db), lambda i: (0, i))],
        out_specs=pl.BlockSpec((n, db), lambda i: (0, i)),
        scratch_shapes=[pltpu.VMEM((n, T), BF16)],
        out_shape=jax.ShapeDtypeStruct((n, D), F32),
        compiler_params=pltpu.CompilerParams(dimension_semantics=("arbitrary",), vmem_limit_bytes=VMEM_LIMIT),
        cost_estimate=pl.CostEstimate(flops=2 * T * D * n, bytes_accessed=n * D * 4, transcendentals=0),
        name="dwo_proj",
    )(ctx, go)


RB = 64


def post_kernel(p_ref, r_ref, h_ref, dy_ref, g_ref, *rest):
    y_ref, go_ref, dg_ref = rest[-3:]
    o = p_ref[...].astype(F32) + r_ref[...].astype(F32)
    inv = lax.rsqrt(jnp.mean(o * o, axis=-1, keepdims=True) + NORM_EPS)
    hat = o * inv
    g = g_ref[...]
    dy = dy_ref[...].astype(F32)
    y_ref[...] = (h_ref[...].astype(F32) + hat * g).astype(BF16)
    gg = dy * g
    go_ref[...] = (inv * (gg - hat * jnp.mean(gg * hat, axis=-1, keepdims=True))).astype(BF16)

    @pl.when(pl.program_id(0) == 0)
    def _():
        dg_ref[...] = jnp.zeros_like(dg_ref)

    dg_ref[...] += jnp.sum((dy * hat).reshape(RB // 8, 8, -1), axis=0)


def pre_kernel(p_ref, r_ref, h_ref, dy_ref, g_ref, *rest):
    dh_ref, dg_ref = rest[-2:]
    ga = p_ref[...].astype(F32) + r_ref[...].astype(F32)
    h = h_ref[...].astype(F32)
    inv = lax.rsqrt(jnp.mean(h * h, axis=-1, keepdims=True) + NORM_EPS)
    hat = h * inv
    gh = ga * g_ref[...]
    dh_ref[...] = (dy_ref[...].astype(F32) + inv * (gh - hat * jnp.mean(gh * hat, axis=-1, keepdims=True))).astype(BF16)

    @pl.when(pl.program_id(0) == 0)
    def _():
        dg_ref[...] = jnp.zeros_like(dg_ref)

    dg_ref[...] += jnp.sum((ga * hat).reshape(RB // 8, 8, -1), axis=0)


def norm_call(kernel, part, peer, hidden, d_out, g, r0, buf, extra):
    M, D = part.shape
    n = M // RB
    loc = pl.BlockSpec((RB, D), lambda i: (i, 0))
    row = pl.BlockSpec((RB, D), lambda i: (r0 // RB + i, 0))
    in_specs = [loc, loc, row, row, pl.BlockSpec((1, D), lambda i: (0, 0))]
    args = [part, peer, hidden, d_out, g.reshape(1, D)]
    aliases = {}
    if buf is not None:
        aliases = {len(args): 0}
        args.append(buf)
        in_specs.append(pl.BlockSpec(memory_space=pl.ANY))
    out_specs = [row] + ([loc] if extra else []) + [pl.BlockSpec((8, D), lambda i: (0, 0))]
    out_shape = [jax.ShapeDtypeStruct(hidden.shape, BF16)]
    if extra:
        out_shape.append(jax.ShapeDtypeStruct((M, D), BF16))
    out_shape.append(jax.ShapeDtypeStruct((8, D), F32))
    return pl.pallas_call(
        kernel, grid=(n,), in_specs=in_specs, out_specs=out_specs, out_shape=out_shape, input_output_aliases=aliases,
        compiler_params=pltpu.CompilerParams(dimension_semantics=("arbitrary",), vmem_limit_bytes=VMEM_LIMIT),
        cost_estimate=pl.CostEstimate(flops=M * D * 2000, bytes_accessed=M * D * 12, transcendentals=0),
    )(*args)


def a_kernel(s_ref, h_ref, g_ref, a_ref):
    h = h_ref[...].astype(F32)
    inv = lax.rsqrt(jnp.mean(h * h, axis=-1, keepdims=True) + NORM_EPS)
    a_ref[...] = (h * inv * g_ref[...]).astype(BF16)


def a_call(hidden, g, idx, M, rb):
    D = hidden.shape[1]
    return pl.pallas_call(
        a_kernel,
        grid_spec=pltpu.PrefetchScalarGridSpec(
            num_scalar_prefetch=1,
            grid=(M // rb,),
            in_specs=[pl.BlockSpec((rb, D), lambda i, s: (s[0] * (M // rb) + i, 0)), pl.BlockSpec((1, D), lambda i, s: (0, 0))],
            out_specs=pl.BlockSpec((rb, D), lambda i, s: (i, 0)),
        ),
        out_shape=jax.ShapeDtypeStruct((M, D), BF16),
        compiler_params=pltpu.CompilerParams(dimension_semantics=("arbitrary",)),
        cost_estimate=pl.CostEstimate(flops=M * D * 1000, bytes_accessed=M * D * 4, transcendentals=0),
    )(jnp.reshape(idx, (1,)).astype(jnp.int32), hidden, g.reshape(1, D))


def solution(mesh):
    core_perm = [(0, 1), (1, 0), (2, 3), (3, 2)]
    x_perm = [(0, 2), (2, 0), (1, 3), (3, 1)]
    tp_perm = [(0, 1), (1, 0)]

    def to_core(v):
        return lax.ppermute(v, 'cp', core_perm)

    def to_x(v):
        return lax.ppermute(v, 'cp', x_perm)

    def to_tp(v):
        return lax.ppermute(v, 'tp', tp_perm)

    def device_fn(hidden, g_pre, w_q, w_k, w_v, w_o, g_post, d_out):
        tokens, D = hidden.shape
        T = 4 * tokens
        me = lax.axis_index('cp')
        tp = lax.axis_index('tp')
        core, xi = me % 2, me // 2
        HL = w_q.shape[1] // 2
        KL = w_k.shape[1] // 2
        cos, sin = lax.optimization_barrier(rope_tables(T))
        base = jnp.stack([xi, core, me, me ^ 1]).astype(jnp.int32)

        def two_way(first, blk, n):
            r1 = to_x(first)
            r3 = to_x(blk[2 * n:])
            r2 = to_tp(r1)
            return [r1, r2, r3], [tp * n, (1 - tp) * n, 2 * n]

        a_first = a_call(hidden, g_pre, tp, 160, 32)
        a_loc = a_call(hidden, g_pre, jnp.int32(0), tokens, 64)
        a_x, a_off = two_way(a_first, a_loc, 160)
        a_p = to_core(a_loc)
        a_xp = [to_core(r) for r in a_x]
        wo2 = w_o.reshape(-1, D)
        N = (HL + 2 * KL) * HEAD
        w_own = w_layout(core, w_q, w_k, w_v, 512)
        w_oth = w_layout(1 - core, w_q, w_k, w_v, 512, 0, 4)
        w_oth = w_layout(1 - core, w_q, w_k, w_v, 512, 4, 5, w_oth)
        qkv_args = (w_own, "qkv", (cos, sin), 2, [core, 1 - core], tokens, 0, N)
        bufs = gather_matmul(xi, core, [(0, 0), (1, 0)], [a_loc, a_p], *qkv_args)
        places = [(0, o) for o in a_off] + [(1, o) for o in a_off]
        qkv, a_all = gather_matmul(1 - xi, core, places, a_x + a_xp, *qkv_args, bufs=bufs)
        qkv = qkv.reshape(T, N)
        a_all = a_all.reshape(T, D)

        ctx, lse = attn_fwd(qkv, KL, HL)
        ctx_pr = to_core(lax.dynamic_slice_in_dim(ctx, (me ^ 1) * tokens, tokens, 0))
        sizes = (128, 128, 128, 128)
        starts = [sum(sizes[:c]) for c in range(len(sizes))]
        o_parts, o_peers = [], []
        for c, M in enumerate(sizes):
            op = o_rows(base, ctx, ctx_pr, wo2, starts[c], M, 1536)
            o_parts.append(op)
            o_peers.append(to_tp(op))

        y_blk, gos, dgp = None, [], []
        for c in range(len(sizes)):
            y_blk, go, dg_ = norm_call(post_kernel, o_parts[c], o_peers[c], hidden, d_out, g_post, starts[c], y_blk, True)
            gos.append(go)
            dgp.append(dg_)

        gx = [to_x(g) for g in gos]
        gp = [to_core(g) for g in gos]
        gxp = [to_core(g) for g in gx]
        HN = HL * HEAD
        RE, RL = starts[-1], sizes[-1]
        places = [(c, o) for c in range(2) for o in starts[:-1]]
        pair = [core, 1 - core]
        bufs = gather_matmul(xi, core, places, gos[:-1] + gp[:-1], wo2, "nt", (), 2, pair, RE, 0, HN)
        bufs = gather_matmul(1 - xi, core, places, gx[:-1] + gxp[:-1], wo2, "nt", (), 2, pair, RE, 0, HN, bufs=bufs)
        places = [(0, rel * RL) for rel in range(4)]
        dctx, go_all = gather_matmul(0, core, places, [gos[-1], gp[-1], gx[-1], gxp[-1]], wo2, "nt", (), 1, [me ^ rel for rel in range(4)],
                                     RL, RE, HN, bufs=bufs)
        dctx = dctx.reshape(T, HN)
        go_all = go_all.reshape(T, D)

        dwo_own = dwo_proj(ctx, go_all, 512)
        dwo_peer = to_core(dwo_own)
        grads = attn_bwd(base, qkv, KL, HL, dctx, ctx, lse, cos, sin)
        dqkv = grads[:3]
        dqkv_pr = [to_core(g) for g in grads[3:]]
        dqkv_p = [to_core(g) for g in dqkv]
        ga_part = ga_rows(base, dqkv, dqkv_pr, (w_own, w_oth), tokens, 512)
        ga_peer = to_tp(ga_part)

        pairs = [g for pair in zip(dqkv, dqkv_p) for g in pair]
        dwq, dwk, dwv, dwo = dw_proj(base, a_all, pairs, (dwo_own, dwo_peer), 256)
        dwo = dwo.reshape(w_o.shape)

        grad_h, dgr = norm_call(pre_kernel, ga_part, ga_peer, hidden, d_out, g_pre, 0, None, False)
        dg = jnp.stack([jnp.sum(dgr, axis=0), jnp.sum(sum(dgp), axis=0)])
        dg = dg + to_core(dg)
        dg = dg + to_x(dg)
        return y_blk, grad_h, dg[0], dwq, dwk, dwv, dwo, dg[1]


    row_spec = P('cp', None)
    head_spec = P(None, 'tp', None)
    out_head_spec = P('tp', None, None)
    return jax.shard_map(device_fn, mesh=mesh, in_specs=(row_spec, P(), head_spec, head_spec, head_spec, out_head_spec, P(), row_spec), out_specs=(row_spec, row_spec, P(), head_spec, head_spec, head_spec, out_head_spec, P()), check_vma=False)
```
